256 devices in a mesh: grp: 4 (over x_hi, core), inf: 64 (over y, z, x_lo).
Axes of the slice: x: 4 (x_hi: 2, x_lo: 2; x = x_hi * 2 + x_lo), y: 4, z: 8, core: 2. Of those that a mesh axis runs over, the one named last changes fastest.
Arguments:
- range_one: float32 [1408], replicated, may hold values from 0.05 to 1
- range_two: float32 [1408], replicated, may hold values from 0.05 to 1
- flop_weight: int32 [1024], P('grp'), may hold values from 0 to 24, as said below
- board_mask: int32 [1024, 1408], P('grp', 'inf'), may hold values 0 or 1
- runout: int32 [1024, 4, 2], P('grp'), may hold values from 0 to 51
- strength: int32 [1024, 4, 1408], P('grp', None, 'inf'), may hold values from 0 to 1073741823
Outputs:
- turn_reach: float32 [512, 6, 1408], P(('grp', 'inf'))
- preflop_reach: float32 [1408], P('inf')
The draws below stay inside these ranges and needn't reach their ends.
Inputs may be any that keep to these rules, and one draw needn't show every extreme that they name: `flop_weight`: slots 256 g to 256 g + 255 belong to group g; in each group the slots with nonzero weight come first; nonzero weights are 4, 12 or 24; exactly 512 slots in all have nonzero weight, every group has at least half of 128 of them, and the busiest group has exactly 256.
All inputs are finite; a program needn't handle non-finite values. No bound on the sum of `board_mask` on one device may be relied on, other than what follows from the above.
Results may differ from the reference program's by a relative error of at most 0.0003.
Values may be sent and summed in bfloat16 or wider, within the bound.
No kernel may reach another device: no remote copies, remote signals or barrier semaphores. Data moves between devices by JAX's collectives and lax.ppermute only.
A program may use at most 64 MiB of HBM per device.

```python
from functools import partial
import jax
import jax.numpy as jnp
import numpy as np
from jax import lax

HANDS = 1326
H = 1408
ITERS = 4
FLOP_GRP = 128
CAP = 256
FLOPS = 512
SLOTS = 1024
N_GRP = 4


def draw_flop_weight(key, part):
    shift_key = jax.random.fold_in(key, 11)
    first_key = jax.random.fold_in(key, 12)
    second_key = jax.random.fold_in(key, 14)
    kind_key = jax.random.fold_in(key, 13)
    shift = jax.random.randint(shift_key, (), 0, 4)
    first_extra = jax.random.randint(first_key, (), 0, FLOP_GRP // 4 + 1)
    second_extra = jax.random.randint(second_key, (), 0, FLOP_GRP // 4 + 1)
    base_counts = jnp.stack([jnp.asarray(CAP, jnp.int32), FLOP_GRP // 2 + first_extra, FLOP_GRP // 2 + second_extra, FLOP_GRP - first_extra - second_extra]).astype(jnp.int32)
    group_ids = jnp.arange(4)
    counts = base_counts[(group_ids - shift) % 4]
    slot_ids = jnp.arange(SLOTS)
    slot_group = slot_ids // CAP
    slot_place = slot_ids % CAP
    is_live = slot_place < counts[slot_group]
    kind_ids = jax.random.randint(kind_key, (SLOTS,), 0, 3)
    multiplicity = jnp.where(kind_ids == 0, 4, jnp.where(kind_ids == 1, 12, 24))
    return jnp.where(is_live, multiplicity, 0).astype(jnp.int32)


def set_ends(entries, rng, smallest, largest):
    spot = [jax.random.randint(jax.random.fold_in(rng, axis), (), 0, length) for axis, length in enumerate(entries.shape)]
    widest = entries.shape.index(max(entries.shape))
    next_to = spot[:widest] + [(spot[widest] + 1) % entries.shape[widest]] + spot[widest + 1:]
    return entries.at[tuple(spot)].set(smallest).at[tuple(next_to)].set(largest)


def setup_inputs(seed: int = 0) -> dict:
    splits = jax.random.split(jax.random.key(seed), 7)
    range_one = jnp.clip(jax.random.uniform(splits[0], (H,), jnp.float32, 0.05, 1.0), 0.05, 1.0)
    range_two = jnp.clip(jax.random.uniform(splits[1], (H,), jnp.float32, 0.05, 1.0), 0.05, 1.0)
    flop_weight = draw_flop_weight(jax.random.fold_in(splits[6], 71), 0)
    board_mask = set_ends((jax.random.randint(splits[3], (SLOTS, H), 0, 9) < 8).astype(jnp.int32), jax.random.fold_in(splits[3], 1), 0, 1)
    runout = set_ends(jax.random.randint(splits[4], (SLOTS, ITERS, 2), 0, 52), jax.random.fold_in(splits[4], 1), 0, 51).astype(jnp.int32)
    strength = set_ends(jax.random.randint(splits[5], (SLOTS, ITERS, H), 0, 1073741824), jax.random.fold_in(splits[5], 1), 0, 1073741823).astype(jnp.int32)
    return {"range_one": range_one, "range_two": range_two, "flop_weight": flop_weight, "board_mask": board_mask, "runout": runout, "strength": strength}


EPSILON = 0.01
FOLD_VALUE = -0.1


def hand_cards(slot_total, real_total):
    low_list = []
    high_list = []
    for first_card in range(52):
        for second_card in range(first_card + 1, 52):
            low_list.append(first_card)
            high_list.append(second_card)
    low_table = np.full(slot_total, 52, np.int32)
    high_table = np.full(slot_total, 53, np.int32)
    used_count = min(slot_total, real_total)
    low_table[:used_count] = np.array(low_list[:used_count], np.int32)
    high_table[:used_count] = np.array(high_list[:used_count], np.int32)
    return low_table, high_table


def action_share(first_regret, second_regret):
    return (first_regret + EPSILON) / (first_regret + second_regret + 2.0 * EPSILON)


def slot_values(low_card, high_card, member):
    key_row, reach_columns = member
    compat = (low_card[:, None] != low_card[None, :]) & (low_card[:, None] != high_card[None, :])
    compat = compat & (high_card[:, None] != low_card[None, :]) & (high_card[:, None] != high_card[None, :])
    both_live = compat & (key_row[:, None] >= 0) & (key_row[None, :] >= 0)
    weight_mat = both_live.astype(jnp.bfloat16)
    sign_mat = jnp.sign(key_row[:, None] - key_row[None, :]).astype(jnp.bfloat16) * weight_mat
    sign_sum = jnp.dot(reach_columns, sign_mat.T, preferred_element_type=jnp.float32)
    summed_weight_total = jnp.dot(reach_columns, weight_mat.T, preferred_element_type=jnp.float32)
    return sign_sum, summed_weight_total


def reference(range_one, range_two, flop_weight, board_mask, runout, strength):
    low_table, high_table = hand_cards(H, HANDS)
    low_card = jnp.asarray(low_table)
    high_card = jnp.asarray(high_table)
    slot_all = jnp.arange(SLOTS).astype(jnp.int32)
    slot_group = slot_all // CAP
    slot_place = slot_all % CAP
    order_key = jnp.where(flop_weight > 0, slot_place * N_GRP + slot_group, CAP * N_GRP + slot_all).astype(jnp.int32)
    live_slots = jnp.argsort(order_key)[:FLOPS].astype(jnp.int32)
    flop_share = flop_weight[live_slots].astype(jnp.float32) / (12.0 * FLOPS)
    board_rows = board_mask[live_slots]
    run_cards = runout[live_slots]
    key_rows = strength[live_slots]
    slot_ids = jnp.arange(H)
    flop_live = ((board_rows == 1) & (slot_ids < HANDS)[None, :]).astype(jnp.float32)
    payoff_value_scale = 1.0 / HANDS
    player_two_total = range_two[None, :] * flop_live
    zero_flop = jnp.zeros((FLOPS, H), jnp.float32)
    root_check = root_bet = facing_call_fold = fc_call = zero_flop
    ac_check = ac_bet = fb_fold = fb_call = zero_flop
    pre_fold = jnp.zeros((H,), jnp.float32)
    pre_cont = jnp.zeros((H,), jnp.float32)
    turn_sum = jnp.zeros((FLOPS, 6, H), jnp.float32)
    pre_sum = jnp.zeros((H,), jnp.float32)
    for counter in range(ITERS):
        share_pre = action_share(pre_cont, pre_fold)
        one_range = range_one * share_pre
        player_one_total = one_range[None, :] * flop_live
        share_root = action_share(root_check, root_bet)
        facing_call_share = action_share(facing_call_fold, fc_call)
        share_ac = action_share(ac_check, ac_bet)
        share_fb = action_share(fb_fold, fb_call)
        player_one_check_share = player_one_total * share_root
        player_one_check_bet_fold = player_one_check_share * facing_call_share
        player_two_check_check = player_two_total * share_ac
        player_two_bet_fold = player_two_total * share_fb
        reach_columns = jnp.stack([player_two_total, player_two_check_check, player_two_bet_fold, player_one_total, player_one_check_share, player_one_check_bet_fold], axis=1).astype(jnp.bfloat16)
        turn_card = run_cards[:, counter, 0:1]
        river_card = run_cards[:, counter, 1:2]
        blocked = (low_card[None, :] == turn_card) | (low_card[None, :] == river_card)
        blocked = blocked | (high_card[None, :] == turn_card) | (high_card[None, :] == river_card)
        is_alive = (flop_live > 0) & jnp.logical_not(blocked)
        key_now = jnp.where(is_alive, key_rows[:, counter, :], -1).astype(jnp.int32)
        sign_sum, summed_weight_total = lax.map(partial(slot_values, low_card, high_card), (key_now, reach_columns))
        v_cc = 0.5 * payoff_value_scale * sign_sum[:, 1, :]
        check_bet_fold_value = -0.5 * payoff_value_scale * (summed_weight_total[:, 0, :] - summed_weight_total[:, 1, :])
        check_bet_call_value = 1.5 * payoff_value_scale * (sign_sum[:, 0, :] - sign_sum[:, 1, :])
        v_bf = 0.5 * payoff_value_scale * summed_weight_total[:, 2, :]
        v_bc = 1.5 * payoff_value_scale * (sign_sum[:, 0, :] - sign_sum[:, 2, :])
        w_cc = 0.5 * payoff_value_scale * sign_sum[:, 4, :]
        check_bet_fold_weight = 0.5 * payoff_value_scale * summed_weight_total[:, 5, :]
        check_bet_call_weight = 1.5 * payoff_value_scale * (sign_sum[:, 4, :] - sign_sum[:, 5, :])
        w_bf = -0.5 * payoff_value_scale * (summed_weight_total[:, 3, :] - summed_weight_total[:, 4, :])
        w_bc = 1.5 * payoff_value_scale * (sign_sum[:, 3, :] - sign_sum[:, 4, :])
        facing_call_utility = facing_call_share * check_bet_fold_value + (1.0 - facing_call_share) * check_bet_call_value
        v_check = v_cc + facing_call_utility
        v_bet = v_bf + v_bc
        u_root = share_root * v_check + (1.0 - share_root) * v_bet
        strategy_bet_share = check_bet_fold_weight + check_bet_call_weight
        u_ac = share_ac * w_cc + (1.0 - share_ac) * strategy_bet_share
        u_fb = share_fb * w_bf + (1.0 - share_fb) * w_bc
        facing_call_fold = jnp.maximum(facing_call_fold + check_bet_fold_value - facing_call_utility, 0.0)
        fc_call = jnp.maximum(fc_call + check_bet_call_value - facing_call_utility, 0.0)
        root_check = jnp.maximum(root_check + v_check - u_root, 0.0)
        root_bet = jnp.maximum(root_bet + v_bet - u_root, 0.0)
        ac_check = jnp.maximum(ac_check + w_cc - u_ac, 0.0)
        ac_bet = jnp.maximum(ac_bet + strategy_bet_share - u_ac, 0.0)
        fb_fold = jnp.maximum(fb_fold + w_bf - u_fb, 0.0)
        fb_call = jnp.maximum(fb_call + w_bc - u_fb, 0.0)
        cont_value = jnp.sum(flop_share[:, None] * u_root, axis=0)
        u_pre = share_pre * cont_value + (1.0 - share_pre) * FOLD_VALUE
        pre_cont = jnp.maximum(pre_cont + cont_value - u_pre, 0.0)
        pre_fold = jnp.maximum(pre_fold + FOLD_VALUE - u_pre, 0.0)
        iter_weight = float(counter + 1)
        turn_row_block = jnp.stack([player_one_check_share, player_one_total - player_one_check_share, player_one_check_share - player_one_check_bet_fold, player_two_check_check, player_two_total - player_two_bet_fold, player_two_total - player_two_check_check], axis=1)
        turn_sum = turn_sum + iter_weight * turn_row_block
        pre_sum = pre_sum + iter_weight * one_range
    total_weight = ITERS * (ITERS + 1) / 2.0
    return turn_sum / total_weight, pre_sum / total_weight
```

```python
import math

import jax
import jax.numpy as jnp
import numpy as np
from jax import lax
from jax.experimental import pallas as pl
from jax.experimental.pallas import tpu as pltpu
from jax.sharding import Mesh
from jax.sharding import PartitionSpec as P

HANDS = 1326
H = 1408
ITERS = 4
FLOP_GRP = 128
GRP = ("grp_0", "grp_1")
INF = ("inf_0", "inf_1", "inf_2")
GRP_INF = ("grp_0", "grp_1", "inf_0", "inf_1", "inf_2")


EPSILON = 0.01
FOLD_VALUE = -0.1


def sent_to_all(x, axis):
    copies = jnp.broadcast_to(x, (lax.axis_size(axis), *x.shape))
    return lax.all_to_all(copies, axis, split_axis=0, concat_axis=0, tiled=True)


def in_order(parts, dim):
    parts = jnp.moveaxis(parts, 0, dim)
    dims = parts.shape
    return parts.reshape(*dims[:dim], dims[dim] * dims[dim + 1], *dims[dim + 2 :])


def gathered_copies(x, axis, dim):
    parts = sent_to_all(x, axis)
    return in_order(parts, dim)


def sent_together(arrays, axis, split_dim, concat_dim, along):
    widths = [math.prod(a.shape[along:]) for a in arrays]
    both = jnp.concatenate(
        [a.reshape(*a.shape[:along], w) for a, w in zip(arrays, widths)], axis=along
    )
    filled = lax.all_to_all(both, axis, split_axis=split_dim, concat_axis=concat_dim, tiled=True)
    parts = jnp.split(filled, [sum(widths[:k]) for k in range(1, len(widths))], axis=along)
    return tuple(
        (b.reshape(*filled.shape[:along], *a.shape[along:]) for a, b in zip(arrays, parts))
    )


def side_by_side(arrays, axis, split_dim, concat_dim, along):
    widths = [a.shape[along] for a in arrays]
    both = jnp.concatenate(arrays, axis=along)
    filled = lax.all_to_all(both, axis, split_axis=split_dim, concat_axis=concat_dim, tiled=True)
    return tuple(jnp.split(filled, [sum(widths[:k]) for k in range(1, len(widths))], axis=along))


def hand_cards(slot_total, real_total):
    low_list = []
    high_list = []
    for first_card in range(52):
        for second_card in range(first_card + 1, 52):
            low_list.append(first_card)
            high_list.append(second_card)
    low_table = np.full(slot_total, 52, np.int32)
    high_table = np.full(slot_total, 53, np.int32)
    used_count = min(slot_total, real_total)
    low_table[:used_count] = np.array(low_list[:used_count], np.int32)
    high_table[:used_count] = np.array(high_list[:used_count], np.int32)
    return (low_table, high_table)


def action_share(first_regret, second_regret):
    return (first_regret + EPSILON) / (first_regret + second_regret + 2.0 * EPSILON)


def slot_route(counts, group_id, per_group, groups, capacity):
    group_ids = jnp.arange(groups)
    own_count = jnp.sum(jnp.where(group_ids == group_id, counts, 0), dtype=jnp.int32)
    own_rows = jnp.arange(capacity)
    earlier = (group_ids < group_id).astype(jnp.int32)
    place = jnp.sum(
        jnp.minimum(counts[None, :], own_rows[:, None] + earlier[None, :]), axis=1, dtype=jnp.int32
    )
    target = group_ids[:, None] * per_group + jnp.arange(per_group)[None, :]
    match = (place[None, None, :] == target[:, :, None]) & (own_rows < own_count)[None, None, :]
    is_valid = jnp.any(match, axis=2)
    source = jnp.sum(jnp.where(match, own_rows[None, None, :], 0), axis=2, dtype=jnp.int32).reshape(
        -1
    )
    return (source, is_valid)


def place_rows(member, route_pair):
    source, is_valid = route_pair
    groups, per_group = is_valid.shape
    taken_rows = jnp.take(member, source, axis=0).reshape((groups, per_group) + member.shape[1:])
    keep_mask = is_valid.reshape((groups, per_group) + (1,) * (member.ndim - 1))
    return jnp.where(keep_mask, taken_rows, jnp.zeros_like(taken_rows))


def add_sources(member):
    return jnp.sum(member, axis=0, dtype=member.dtype)


SCALE = 1.0 / HANDS
BLOCK = 128
FIRST_SUM = ("grp_0", "inf_0", "inf_2")


def compat_kernel(low_ref, high_ref, out_ref):
    low_row = low_ref[...]
    high_row = high_ref[...]
    for first in range(0, H, BLOCK):
        low_col = jnp.broadcast_to(low_ref[:, first : first + BLOCK], (BLOCK, BLOCK)).T
        high_col = jnp.broadcast_to(high_ref[:, first : first + BLOCK], (BLOCK, BLOCK)).T
        for start in range(0, H, BLOCK):
            low_here = low_row[:, start : start + BLOCK]
            high_here = high_row[:, start : start + BLOCK]
            apart = (low_col != low_here) & (low_col != high_here)
            apart = apart & (high_col != low_here) & (high_col != high_here)
            out_ref[first : first + BLOCK, start : start + BLOCK] = jnp.where(
                apart, 1.0, 0.0
            ).astype(jnp.bfloat16)


def compat_matrix(low, high):
    return pl.pallas_call(
        compat_kernel,
        out_shape=jax.ShapeDtypeStruct((H, H), jnp.bfloat16),
        name="compat",
    )(low.reshape(1, H), high.reshape(1, H))


def pair_sums(key_ref, counter, columns, compat_ref, col_ref, lhs_ref, sign_ref, sums_ref, weight_ref):
    alive = (key_ref[counter] >= 0).astype(jnp.float32)
    col_ref[...] = jnp.zeros((16, H), jnp.float32)
    for k, column in columns.items():
        col_ref[2 * k : 2 * k + 2, :] = column * alive
    lhs_ref[...] = col_ref[...].astype(jnp.bfloat16)
    weight_ref[...] = jnp.dot(lhs_ref[...], compat_ref[...], preferred_element_type=jnp.float32)
    row_flop = lax.broadcasted_iota(jnp.int32, (16, H), 0) & 1

    def one_flop(flop, carry):
        key_row = key_ref[counter, flop : flop + 1, :]
        for first in range(0, H, BLOCK):
            key_col = jnp.broadcast_to(key_row[:, first : first + BLOCK], (BLOCK, BLOCK)).T
            for start in range(0, H, BLOCK):
                key_here = key_row[:, start : start + BLOCK]
                sign = jnp.where(
                    key_here > key_col, 1.0, jnp.where(key_here < key_col, -1.0, 0.0)
                ).astype(jnp.bfloat16)
                sign_ref[first : first + BLOCK, start : start + BLOCK] = (
                    sign * compat_ref[first : first + BLOCK, start : start + BLOCK]
                )
        total = jnp.dot(lhs_ref[...], sign_ref[...], preferred_element_type=jnp.float32)
        sums_ref[...] = jnp.where(row_flop == flop, total, sums_ref[...])
        return carry

    for flop in range(2):
        one_flop(flop, 0)
    sign_sum = {k: sums_ref[2 * k : 2 * k + 2, :] * alive for k in columns}
    weight_sum = {k: weight_ref[2 * k : 2 * k + 2, :] * alive for k in columns}
    return sign_sum, weight_sum


def two_values(sign_sum, weight_sum, share_root, share_fc):
    v_cc = 0.5 * SCALE * sign_sum[1]
    v_cbf = -0.5 * SCALE * (weight_sum[0] - weight_sum[1])
    v_cbc = 1.5 * SCALE * (sign_sum[0] - sign_sum[1])
    v_bf = 0.5 * SCALE * weight_sum[2]
    v_bc = 1.5 * SCALE * (sign_sum[0] - sign_sum[2])
    u_fc = share_fc * v_cbf + (1.0 - share_fc) * v_cbc
    v_check = v_cc + u_fc
    v_bet = v_bf + v_bc
    u_root = share_root * v_check + (1.0 - share_root) * v_bet
    return v_cbf, v_cbc, u_fc, v_check, v_bet, u_root


def one_values(sign_sum, weight_sum, share_ac, share_fb):
    w_cc = 0.5 * SCALE * sign_sum[4]
    w_cbf = 0.5 * SCALE * weight_sum[5]
    w_cbc = 1.5 * SCALE * (sign_sum[4] - sign_sum[5])
    w_bf = -0.5 * SCALE * (weight_sum[3] - weight_sum[4])
    w_bc = 1.5 * SCALE * (sign_sum[3] - sign_sum[4])
    x_bet = w_cbf + w_cbc
    u_ac = share_ac * w_cc + (1.0 - share_ac) * x_bet
    u_fb = share_fb * w_bf + (1.0 - share_fb) * w_bc
    return w_cc, x_bet, u_ac, w_bf, w_bc, u_fb


def two_regrets(regrets, values):
    root_check, root_bet, fc_fold, fc_call = regrets
    v_cbf, v_cbc, u_fc, v_check, v_bet, u_root = values
    return (
        jnp.maximum(root_check + v_check - u_root, 0.0),
        jnp.maximum(root_bet + v_bet - u_root, 0.0),
        jnp.maximum(fc_fold + v_cbf - u_fc, 0.0),
        jnp.maximum(fc_call + v_cbc - u_fc, 0.0),
    )


def one_regrets(regrets, values):
    ac_check, ac_bet, fb_fold, fb_call = regrets
    w_cc, x_bet, u_ac, w_bf, w_bc, u_fb = values
    return (
        jnp.maximum(ac_check + w_cc - u_ac, 0.0),
        jnp.maximum(ac_bet + x_bet - u_ac, 0.0),
        jnp.maximum(fb_fold + w_bf - u_fb, 0.0),
        jnp.maximum(fb_call + w_bc - u_fb, 0.0),
    )


def pre_step(pre_cont, pre_fold, cont_value):
    share_pre = action_share(pre_cont, pre_fold)
    u_pre = share_pre * cont_value + (1.0 - share_pre) * FOLD_VALUE
    return (
        jnp.maximum(pre_cont + cont_value - u_pre, 0.0),
        jnp.maximum(pre_fold + FOLD_VALUE - u_pre, 0.0),
    )


def one_columns(one_all, share_root, share_fc):
    one_check = one_all * share_root
    return {3: one_all, 4: one_check, 5: one_check * share_fc}


def two_columns(two_all, share_ac, share_fb):
    return {0: two_all, 1: two_all * share_ac, 2: two_all * share_fb}


def one_rows(columns):
    return columns[4], columns[3] - columns[4], columns[4] - columns[5]


def two_rows(columns):
    return columns[1], columns[0] - columns[2], columns[0] - columns[1]


def flop_value(share, u_root):
    part = share * u_root
    return part[0:1, :] + part[1:2, :]


def first_kernel(
    key_ref, live_ref, one_ref, two_ref, share_ref, compat_ref,
    cont_ref, root_check_ref, root_bet_ref, fc_fold_ref, fc_call_ref,
    ac_check_ref, ac_bet_ref, fb_fold_ref, fb_call_ref, share_root_ref, share_fc_ref, turn_ref,
    col_ref, lhs_ref, sign_ref, sums_ref, weight_ref,
):
    scratch = (compat_ref, col_ref, lhs_ref, sign_ref, sums_ref, weight_ref)
    live = live_ref[...]
    share = share_ref[...]
    zero = jnp.zeros((2, H), jnp.float32)
    zero_row = jnp.zeros((1, H), jnp.float32)
    two_all = two_ref[...] * live
    start = action_share(zero, zero)
    one_all = one_ref[...] * action_share(zero_row, zero_row) * live
    one_cols = one_columns(one_all, start, start)
    two_cols = two_columns(two_all, start, start)
    sign_sum, weight_sum = pair_sums(key_ref, 0, {**two_cols, **one_cols}, *scratch)
    values = two_values(sign_sum, weight_sum, start, start)
    cont_ref[0:1, :] = flop_value(share, values[5])
    regrets = two_regrets((zero, zero, zero, zero), values)
    others = one_regrets((zero, zero, zero, zero), one_values(sign_sum, weight_sum, start, start))
    turns = [*one_rows(one_cols), *two_rows(two_cols)]

    share_root = action_share(regrets[0], regrets[1])
    share_fc = action_share(regrets[2], regrets[3])
    two_cols = two_columns(
        two_all, action_share(others[0], others[1]), action_share(others[2], others[3])
    )
    sign_sum, weight_sum = pair_sums(key_ref, 1, two_cols, *scratch)
    values = two_values(sign_sum, weight_sum, share_root, share_fc)
    cont_ref[1:2, :] = flop_value(share, values[5])
    regrets = two_regrets(regrets, values)
    for k, row in enumerate(two_rows(two_cols)):
        turns[3 + k] = turns[3 + k] + 2.0 * row
    root_check_ref[...], root_bet_ref[...], fc_fold_ref[...], fc_call_ref[...] = regrets
    ac_check_ref[...], ac_bet_ref[...], fb_fold_ref[...], fb_call_ref[...] = others
    share_root_ref[...] = share_root
    share_fc_ref[...] = share_fc
    for k in range(6):
        turn_ref[k] = turns[k]


def second_kernel(
    key_ref, live_ref, one_ref, two_ref, share_ref, compat_ref, sums_in_ref,
    root_check_ref, root_bet_ref, fc_fold_ref, fc_call_ref,
    ac_check_ref, ac_bet_ref, fb_fold_ref, fb_call_ref, share_root_ref, share_fc_ref, turn_ref,
    cont_ref, out_root_ref, out_fc_ref, out_turn_ref, out_pre_ref,
    col_ref, lhs_ref, sign_ref, sums_ref, weight_ref,
):
    scratch = (compat_ref, col_ref, lhs_ref, sign_ref, sums_ref, weight_ref)
    live = live_ref[...]
    zero_row = jnp.zeros((1, H), jnp.float32)
    two_all = two_ref[...] * live
    one_range = one_ref[...]
    turns = [turn_ref[k] for k in range(6)]
    pre_sum = one_range * action_share(zero_row, zero_row)
    pre_cont, pre_fold = pre_step(zero_row, zero_row, sums_in_ref[0:1, :])
    one_now = one_range * action_share(pre_cont, pre_fold)
    pre_sum = pre_sum + 2.0 * one_now
    one_cols = one_columns(one_now * live, share_root_ref[...], share_fc_ref[...])
    for k, row in enumerate(one_rows(one_cols)):
        turns[k] = turns[k] + 2.0 * row
    others = (ac_check_ref[...], ac_bet_ref[...], fb_fold_ref[...], fb_call_ref[...])
    share_ac = action_share(others[0], others[1])
    share_fb = action_share(others[2], others[3])
    sign_sum, weight_sum = pair_sums(key_ref, 1, one_cols, *scratch)
    others = one_regrets(others, one_values(sign_sum, weight_sum, share_ac, share_fb))

    pre_cont, pre_fold = pre_step(pre_cont, pre_fold, sums_in_ref[1:2, :])
    one_now = one_range * action_share(pre_cont, pre_fold)
    pre_sum = pre_sum + 3.0 * one_now
    regrets = (root_check_ref[...], root_bet_ref[...], fc_fold_ref[...], fc_call_ref[...])
    share_root = action_share(regrets[0], regrets[1])
    share_fc = action_share(regrets[2], regrets[3])
    share_ac = action_share(others[0], others[1])
    share_fb = action_share(others[2], others[3])
    one_cols = one_columns(one_now * live, share_root, share_fc)
    two_cols = two_columns(two_all, share_ac, share_fb)
    for k, row in enumerate((*one_rows(one_cols), *two_rows(two_cols))):
        turns[k] = turns[k] + 3.0 * row
    sign_sum, weight_sum = pair_sums(key_ref, 2, {**two_cols, **one_cols}, *scratch)
    values = two_values(sign_sum, weight_sum, share_root, share_fc)
    cont_ref[...] = flop_value(share_ref[...], values[5])
    regrets = two_regrets(regrets, values)
    others = one_regrets(others, one_values(sign_sum, weight_sum, share_ac, share_fb))
    two_cols = two_columns(
        two_all, action_share(others[0], others[1]), action_share(others[2], others[3])
    )
    for k, row in enumerate(two_rows(two_cols)):
        turns[3 + k] = turns[3 + k] + 4.0 * row
    out_root_ref[...] = action_share(regrets[0], regrets[1])
    out_fc_ref[...] = action_share(regrets[2], regrets[3])
    for k in range(6):
        out_turn_ref[k] = turns[k]
    out_pre_ref[0:1, :] = pre_cont
    out_pre_ref[1:2, :] = pre_fold
    out_pre_ref[2:3, :] = pre_sum


def pair_scratch():
    return [
        pltpu.VMEM((16, H), jnp.float32),
        pltpu.VMEM((16, H), jnp.bfloat16),
        pltpu.VMEM((H, H), jnp.bfloat16),
        pltpu.VMEM((16, H), jnp.float32),
        pltpu.VMEM((16, H), jnp.float32),
    ]


def rows_of(*shapes):
    return [jax.ShapeDtypeStruct(shape, jnp.float32) for shape in shapes]


def solve(key_now, live, range_one, range_two, flop_share, compat, whole_sum):
    one_row = range_one.reshape(1, H)
    shared = (key_now, live, one_row, range_two.reshape(1, H), flop_share[:, None], compat)
    pair = (2, H)
    first = pl.pallas_call(
        first_kernel,
        out_shape=rows_of(*([pair] * 11), (6, 2, H)),
        scratch_shapes=pair_scratch(),
        name="first",
    )(*shared)
    second = pl.pallas_call(
        second_kernel,
        out_shape=rows_of((1, H), pair, pair, (6, 2, H), (3, H)),
        scratch_shapes=pair_scratch(),
        name="second",
    )(*shared, whole_sum(first[0]), *first[1:])
    cont_value, share_root, share_fc, turns, pre = second
    pre_cont, pre_fold = pre_step(pre[0:1], pre[1:2], whole_sum(cont_value))
    one_range = one_row * action_share(pre_cont, pre_fold)
    columns = one_columns(one_range * live, share_root, share_fc)
    last = jnp.concatenate([jnp.stack(one_rows(columns)) * 4.0, jnp.zeros((3, 2, H))])
    return jnp.swapaxes(turns + last, 0, 1), (pre[2:3] + 4.0 * one_range).reshape(H)


def spread_sum(x, axis):
    rows, width = x.shape
    return jnp.sum(sent_to_all(x.reshape(1, rows * width), axis), axis=0).reshape(rows, width)


def whole_sum(x):
    x = x + lax.ppermute(x, "grp_1", [(0, 1), (1, 0)])
    return spread_sum(spread_sum(x, FIRST_SUM), "inf_1")


def on_device(range_one, range_two, flop_weight, board_mask, runout, strength):
    groups = lax.axis_size(GRP)
    shards = lax.axis_size(INF)
    shard_id = lax.axis_index(INF)
    group_id = lax.axis_index(GRP)
    low_table, high_table = hand_cards(H, HANDS)
    low_all = jnp.asarray(low_table)
    high_all = jnp.asarray(high_table)
    capacity = strength.shape[0]
    hand_block = strength.shape[2]
    flop_total = 12.0 * FLOP_GRP * groups
    live_count = jnp.sum((flop_weight > 0).astype(jnp.int32), dtype=jnp.int32)
    counts = gathered_copies(live_count[None], GRP, 0)
    route_pair = slot_route(counts, group_id, FLOP_GRP, groups, capacity)
    arrived = sent_together(
        (
            place_rows(flop_weight, route_pair),
            place_rows(board_mask, route_pair),
            place_rows(runout, route_pair),
            place_rows(strength, route_pair),
        ),
        GRP,
        0,
        0,
        2,
    )
    weight = add_sources(arrived[0])
    board_rows = add_sources(arrived[1])
    run_cards = add_sources(arrived[2])
    key_rows = add_sources(arrived[3])
    local_count = key_rows.shape[0] // shards
    flop_keys, flop_board = side_by_side((key_rows, board_rows[:, None, :]), INF, 0, 2, 1)
    first_slot = shard_id * local_count
    runs_here = lax.dynamic_slice_in_dim(run_cards, first_slot, local_count, 0)
    weight_here = lax.dynamic_slice_in_dim(weight, first_slot, local_count, 0)

    flop_live = (flop_board[:, 0, :] == 1) & (jnp.arange(H) < HANDS)[None, :]
    keys = []
    for counter in range(ITERS - 1):
        turn_card = runs_here[:, counter, 0:1]
        river_card = runs_here[:, counter, 1:2]
        blocked = (low_all[None, :] == turn_card) | (low_all[None, :] == river_card)
        blocked = blocked | (high_all[None, :] == turn_card) | (high_all[None, :] == river_card)
        keys.append(jnp.where(flop_live & ~blocked, flop_keys[:, counter, :], -1))
    turn_sum, pre_sum = solve(
        jnp.stack(keys),
        flop_live.astype(jnp.float32),
        range_one,
        range_two,
        weight_here.astype(jnp.float32) / flop_total,
        compat_matrix(low_all, high_all),
        whole_sum,
    )
    pre_block = lax.dynamic_slice_in_dim(pre_sum, shard_id * hand_block, hand_block)
    total_weight = ITERS * (ITERS + 1) / 2.0
    turn_final = turn_sum / total_weight
    return (turn_final, pre_block / total_weight)


def solution(mesh):
    split = Mesh(mesh.devices.reshape(2, 2, 4, 8, 2), ("grp_0", "grp_1", "inf_0", "inf_1", "inf_2"))
    return jax.shard_map(
        on_device,
        mesh=split,
        in_specs=(P(), P(), P(GRP), P(GRP, INF), P(GRP, None, None), P(GRP, None, INF)),
        out_specs=(P(GRP_INF, None, None), P(INF)),
        check_vma=False,
    )
```

```python
import jax
import jax.numpy as jnp
import numpy as np
from jax import lax
from jax.experimental import pallas as pl
from jax.experimental.pallas import tpu as pltpu
from jax.sharding import Mesh
from jax.sharding import PartitionSpec as P

HANDS = 1326
H = 1408
ITERS = 4
FLOP_GRP = 128
GRP = ("grp_0", "grp_1")
INF = ("inf_0", "inf_1", "inf_2")
GRP_INF = ("grp_0", "grp_1", "inf_0", "inf_1", "inf_2")


EPSILON = 0.01
FOLD_VALUE = -0.1


def sent_to_all(x, axis):
    copies = jnp.broadcast_to(x, (lax.axis_size(axis), *x.shape))
    return lax.all_to_all(copies, axis, split_axis=0, concat_axis=0, tiled=True)


def hand_cards(slot_total, real_total):
    low_list = []
    high_list = []
    for first_card in range(52):
        for second_card in range(first_card + 1, 52):
            low_list.append(first_card)
            high_list.append(second_card)
    low_table = np.full(slot_total, 52, np.int32)
    high_table = np.full(slot_total, 53, np.int32)
    used_count = min(slot_total, real_total)
    low_table[:used_count] = np.array(low_list[:used_count], np.int32)
    high_table[:used_count] = np.array(high_list[:used_count], np.int32)
    return (low_table, high_table)


def action_share(first_regret, second_regret):
    return (first_regret + EPSILON) / (first_regret + second_regret + 2.0 * EPSILON)


SCALE = 1.0 / HANDS
FLOP_TOTAL = 12.0 * FLOP_GRP * 4
LINE = 128
PART = 256
BLOCK = 128
WIDE = 256
DEEP = 256
PADDED = 1536
FIRST_SUM = ("grp_1", "inf_0", "inf_2")
SECOND_SUM = ("grp_0", "inf_1")


def compat_kernel(low_ref, high_ref, out_ref):
    def rows(step, carry):
        first = pl.multiple_of(step * BLOCK, BLOCK)
        low_col = jnp.broadcast_to(low_ref[:, pl.ds(first, BLOCK)], (BLOCK, BLOCK)).T
        high_col = jnp.broadcast_to(high_ref[:, pl.ds(first, BLOCK)], (BLOCK, BLOCK)).T
        for start in range(0, PADDED, BLOCK):
            low_here = low_ref[:, start : start + BLOCK]
            high_here = high_ref[:, start : start + BLOCK]
            apart = (low_col != low_here) & (low_col != high_here)
            apart = apart & (high_col != low_here) & (high_col != high_here)
            out_ref[pl.ds(first, BLOCK), start : start + BLOCK] = jnp.where(
                apart, 1.0, 0.0
            ).astype(jnp.bfloat16)
        return carry

    lax.fori_loop(0, H // BLOCK, rows, 0)


def compat_matrix(low, high):
    return pl.pallas_call(
        compat_kernel,
        out_shape=jax.ShapeDtypeStruct((H, PADDED), jnp.bfloat16),
        name="compat",
    )(low, high)


def pair_sums(key_ref, counter, columns, compat_ref, lhs_ref, low_ref, sums_ref, col_ref):
    alive = (key_ref[counter, :, :H] >= 0).astype(jnp.float32)
    lhs_ref[...] = jnp.zeros((16, H), jnp.float32)
    for k, column in columns.items():
        lhs_ref[2 * k : 2 * k + 2, :] = column * alive
    low_ref[...] = lhs_ref[...].astype(jnp.bfloat16)

    def key_column(step, carry):
        first = pl.multiple_of(step * BLOCK, BLOCK)
        for flop in range(2):
            keys = key_ref[counter, flop : flop + 1, pl.ds(first, BLOCK)]
            col_ref[flop, pl.ds(first, BLOCK), :] = jnp.broadcast_to(keys, (BLOCK, BLOCK)).T
        return carry

    lax.fori_loop(0, H // BLOCK, key_column, 0)

    def mine(step, carry):
        start = pl.multiple_of(step * WIDE, WIDE)
        weight_total = jnp.zeros((16, WIDE), jnp.float32)
        totals = [jnp.zeros((16, WIDE), jnp.float32) for flop in range(2)]
        rows = [key_ref[counter, flop : flop + 1, pl.ds(start, WIDE)] for flop in range(2)]
        for first in range(0, H, DEEP):
            depth = min(DEEP, H - first)
            lhs = low_ref[:, first : first + depth]
            most = compat_ref[first : first + depth, pl.ds(start, WIDE)]
            least = -most
            weight_total = weight_total + jnp.dot(lhs, most, preferred_element_type=jnp.float32)
            for flop in range(2):
                parts = []
                key_col = col_ref[flop, first : first + depth, :]
                for lane in range(0, WIDE, BLOCK):
                    gap = rows[flop][:, lane : lane + BLOCK] - key_col
                    parts.append(gap.astype(jnp.float32).astype(jnp.bfloat16))
                sign = jnp.concatenate(parts, axis=1) if len(parts) > 1 else parts[0]
                sign = jnp.minimum(jnp.maximum(sign, least), most)
                totals[flop] = totals[flop] + jnp.dot(
                    lhs, sign, preferred_element_type=jnp.float32
                )
        row_flop = lax.broadcasted_iota(jnp.int32, (16, WIDE), 0) & 1
        sums_ref[0, :, pl.ds(start, WIDE)] = jnp.where(row_flop == 0, totals[0], totals[1])
        sums_ref[1, :, pl.ds(start, WIDE)] = weight_total
        return carry

    lax.fori_loop(0, PADDED // WIDE, mine, 0)
    sign_sum = {k: sums_ref[0, 2 * k : 2 * k + 2, :H] * alive for k in columns}
    weight_sum = {k: sums_ref[1, 2 * k : 2 * k + 2, :H] * alive for k in columns}
    return sign_sum, weight_sum


def two_values(sign_sum, weight_sum, share_root, share_fc):
    v_cc = 0.5 * SCALE * sign_sum[1]
    v_cbf = -0.5 * SCALE * (weight_sum[0] - weight_sum[1])
    v_cbc = 1.5 * SCALE * (sign_sum[0] - sign_sum[1])
    v_bf = 0.5 * SCALE * weight_sum[2]
    v_bc = 1.5 * SCALE * (sign_sum[0] - sign_sum[2])
    u_fc = share_fc * v_cbf + (1.0 - share_fc) * v_cbc
    v_check = v_cc + u_fc
    v_bet = v_bf + v_bc
    u_root = share_root * v_check + (1.0 - share_root) * v_bet
    return v_cbf, v_cbc, u_fc, v_check, v_bet, u_root


def one_values(sign_sum, weight_sum, share_ac, share_fb):
    w_cc = 0.5 * SCALE * sign_sum[4]
    w_cbf = 0.5 * SCALE * weight_sum[5]
    w_cbc = 1.5 * SCALE * (sign_sum[4] - sign_sum[5])
    w_bf = -0.5 * SCALE * (weight_sum[3] - weight_sum[4])
    w_bc = 1.5 * SCALE * (sign_sum[3] - sign_sum[4])
    x_bet = w_cbf + w_cbc
    u_ac = share_ac * w_cc + (1.0 - share_ac) * x_bet
    u_fb = share_fb * w_bf + (1.0 - share_fb) * w_bc
    return w_cc, x_bet, u_ac, w_bf, w_bc, u_fb


def two_regrets(regrets, values):
    root_check, root_bet, fc_fold, fc_call = regrets
    v_cbf, v_cbc, u_fc, v_check, v_bet, u_root = values
    return (
        jnp.maximum(root_check + v_check - u_root, 0.0),
        jnp.maximum(root_bet + v_bet - u_root, 0.0),
        jnp.maximum(fc_fold + v_cbf - u_fc, 0.0),
        jnp.maximum(fc_call + v_cbc - u_fc, 0.0),
    )


def one_regrets(regrets, values):
    ac_check, ac_bet, fb_fold, fb_call = regrets
    w_cc, x_bet, u_ac, w_bf, w_bc, u_fb = values
    return (
        jnp.maximum(ac_check + w_cc - u_ac, 0.0),
        jnp.maximum(ac_bet + x_bet - u_ac, 0.0),
        jnp.maximum(fb_fold + w_bf - u_fb, 0.0),
        jnp.maximum(fb_call + w_bc - u_fb, 0.0),
    )


def pre_step(pre_cont, pre_fold, cont_value):
    share_pre = action_share(pre_cont, pre_fold)
    u_pre = share_pre * cont_value + (1.0 - share_pre) * FOLD_VALUE
    return (
        jnp.maximum(pre_cont + cont_value - u_pre, 0.0),
        jnp.maximum(pre_fold + FOLD_VALUE - u_pre, 0.0),
    )


def one_columns(one_all, share_root, share_fc):
    one_check = one_all * share_root
    return {3: one_all, 4: one_check, 5: one_check * share_fc}


def two_columns(two_all, share_ac, share_fb):
    return {0: two_all, 1: two_all * share_ac, 2: two_all * share_fb}


def one_rows(columns):
    return columns[4], columns[3] - columns[4], columns[4] - columns[5]


def two_rows(columns):
    return columns[1], columns[0] - columns[2], columns[0] - columns[1]


def flop_value(share, u_root):
    part = share * u_root
    return part[0:1, :] + part[1:2, :]


def add_parts(parts_ref, start):
    total = parts_ref[0, :, start : start + H]
    for k in range(1, parts_ref.shape[0]):
        total = total + parts_ref[k, :, start : start + H]
    return total


def spread(copies_ref, start, value):
    for k in range(copies_ref.shape[0]):
        copies_ref[k, :, start : start + H] = value


def read_flops(arrived_ref, low_ref, high_ref, key_ref, live_ref, share_ref):
    used = key_ref.shape[0]
    shards = arrived_ref.shape[0]
    hand_block = H // shards
    for shard in range(shards):
        line = arrived_ref[shard] - 1
        for flop in range(2):
            for counter in range(used):
                first = LINE * flop + hand_block * counter
                key_ref[
                    counter, flop : flop + 1, hand_block * shard : hand_block * (shard + 1)
                ] = line[:, first : first + hand_block]
    live_ref[...] = (key_ref[0, :, :H] >= 0).astype(jnp.float32)
    low = low_ref[...]
    high = high_ref[...]
    for flop in range(2):
        first = LINE * flop + hand_block * used
        extra = arrived_ref[0, :, first : first + 1 + 2 * used]
        share_ref[flop : flop + 1, :] = extra[:, 0:1].astype(jnp.float32) / FLOP_TOTAL
        for counter in range(used):
            turn = extra[:, 1 + 2 * counter : 2 + 2 * counter]
            river = extra[:, 2 + 2 * counter : 3 + 2 * counter]
            blocked = (low == turn) | (low == river) | (high == turn) | (high == river)
            blocked = blocked | (lax.broadcasted_iota(jnp.int32, (1, PADDED), 1) >= H)
            row = key_ref[counter, flop : flop + 1, :]
            key_ref[counter, flop : flop + 1, :] = jnp.where(blocked, -1, row)


def first_kernel(
    arrived_ref, low_ref, high_ref, one_ref, two_ref, compat_ref,
    key_ref, live_ref, share_ref, cont_ref,
    root_check_ref, root_bet_ref, fc_fold_ref, fc_call_ref,
    ac_check_ref, ac_bet_ref, fb_fold_ref, fb_call_ref, share_root_ref, share_fc_ref, turn_ref,
    lhs_ref, low_part_ref, sums_ref, col_ref,
):
    scratch = (compat_ref, lhs_ref, low_part_ref, sums_ref, col_ref)
    read_flops(arrived_ref, low_ref, high_ref, key_ref, live_ref, share_ref)
    live = live_ref[...]
    share = share_ref[...]
    zero = jnp.zeros((2, H), jnp.float32)
    zero_row = jnp.zeros((1, H), jnp.float32)
    two_all = two_ref[...] * live
    start = action_share(zero, zero)
    one_all = one_ref[...] * action_share(zero_row, zero_row) * live
    one_cols = one_columns(one_all, start, start)
    two_cols = two_columns(two_all, start, start)
    sign_sum, weight_sum = pair_sums(key_ref, 0, {**two_cols, **one_cols}, *scratch)
    values = two_values(sign_sum, weight_sum, start, start)
    spread(cont_ref, 0, flop_value(share, values[5]))
    regrets = two_regrets((zero, zero, zero, zero), values)
    others = one_regrets((zero, zero, zero, zero), one_values(sign_sum, weight_sum, start, start))
    turns = [*one_rows(one_cols), *two_rows(two_cols)]

    share_root = action_share(regrets[0], regrets[1])
    share_fc = action_share(regrets[2], regrets[3])
    two_cols = two_columns(
        two_all, action_share(others[0], others[1]), action_share(others[2], others[3])
    )
    sign_sum, weight_sum = pair_sums(key_ref, 1, two_cols, *scratch)
    values = two_values(sign_sum, weight_sum, share_root, share_fc)
    spread(cont_ref, H, flop_value(share, values[5]))
    regrets = two_regrets(regrets, values)
    for k, row in enumerate(two_rows(two_cols)):
        turns[3 + k] = turns[3 + k] + 2.0 * row
    root_check_ref[...], root_bet_ref[...], fc_fold_ref[...], fc_call_ref[...] = regrets
    ac_check_ref[...], ac_bet_ref[...], fb_fold_ref[...], fb_call_ref[...] = others
    share_root_ref[...] = share_root
    share_fc_ref[...] = share_fc
    for k in range(6):
        turn_ref[k] = turns[k]


def second_kernel(
    key_ref, live_ref, one_ref, two_ref, share_ref, compat_ref, sums_in_ref,
    root_check_ref, root_bet_ref, fc_fold_ref, fc_call_ref,
    ac_check_ref, ac_bet_ref, fb_fold_ref, fb_call_ref, share_root_ref, share_fc_ref, turn_ref,
    cont_ref, out_root_ref, out_fc_ref, out_turn_ref, out_pre_ref,
    lhs_ref, low_ref, sums_ref, col_ref,
):
    scratch = (compat_ref, lhs_ref, low_ref, sums_ref, col_ref)
    live = live_ref[...]
    zero_row = jnp.zeros((1, H), jnp.float32)
    two_all = two_ref[...] * live
    one_range = one_ref[...]
    turns = [turn_ref[k] for k in range(6)]
    pre_sum = one_range * action_share(zero_row, zero_row)
    pre_cont, pre_fold = pre_step(zero_row, zero_row, add_parts(sums_in_ref, 0))
    one_now = one_range * action_share(pre_cont, pre_fold)
    pre_sum = pre_sum + 2.0 * one_now
    one_cols = one_columns(one_now * live, share_root_ref[...], share_fc_ref[...])
    for k, row in enumerate(one_rows(one_cols)):
        turns[k] = turns[k] + 2.0 * row
    others = (ac_check_ref[...], ac_bet_ref[...], fb_fold_ref[...], fb_call_ref[...])
    share_ac = action_share(others[0], others[1])
    share_fb = action_share(others[2], others[3])
    sign_sum, weight_sum = pair_sums(key_ref, 1, one_cols, *scratch)
    others = one_regrets(others, one_values(sign_sum, weight_sum, share_ac, share_fb))

    pre_cont, pre_fold = pre_step(pre_cont, pre_fold, add_parts(sums_in_ref, H))
    one_now = one_range * action_share(pre_cont, pre_fold)
    pre_sum = pre_sum + 3.0 * one_now
    regrets = (root_check_ref[...], root_bet_ref[...], fc_fold_ref[...], fc_call_ref[...])
    share_root = action_share(regrets[0], regrets[1])
    share_fc = action_share(regrets[2], regrets[3])
    share_ac = action_share(others[0], others[1])
    share_fb = action_share(others[2], others[3])
    one_cols = one_columns(one_now * live, share_root, share_fc)
    two_cols = two_columns(two_all, share_ac, share_fb)
    for k, row in enumerate((*one_rows(one_cols), *two_rows(two_cols))):
        turns[k] = turns[k] + 3.0 * row
    sign_sum, weight_sum = pair_sums(key_ref, 2, {**two_cols, **one_cols}, *scratch)
    values = two_values(sign_sum, weight_sum, share_root, share_fc)
    spread(cont_ref, 0, flop_value(share_ref[...], values[5]))
    regrets = two_regrets(regrets, values)
    others = one_regrets(others, one_values(sign_sum, weight_sum, share_ac, share_fb))
    two_cols = two_columns(
        two_all, action_share(others[0], others[1]), action_share(others[2], others[3])
    )
    for k, row in enumerate(two_rows(two_cols)):
        turns[3 + k] = turns[3 + k] + 4.0 * row
    out_root_ref[...] = action_share(regrets[0], regrets[1])
    out_fc_ref[...] = action_share(regrets[2], regrets[3])
    for k in range(6):
        out_turn_ref[k] = turns[k]
    out_pre_ref[0:1, :] = pre_cont
    out_pre_ref[1:2, :] = pre_fold
    out_pre_ref[2:3, :] = pre_sum


def pair_scratch():
    return [
        pltpu.VMEM((16, H), jnp.float32),
        pltpu.VMEM((16, H), jnp.bfloat16),
        pltpu.VMEM((2, 16, PADDED), jnp.float32),
        pltpu.VMEM((2, H, BLOCK), jnp.int32),
    ]


def rows_of(*shapes):
    return [jax.ShapeDtypeStruct(shape, jnp.float32) for shape in shapes]


def last_kernel(
    live_ref, one_ref, sums_in_ref, share_root_ref, share_fc_ref, turn_ref, pre_ref,
    out_ref, pre_out_ref,
):
    total_weight = ITERS * (ITERS + 1) / 2.0
    pre_cont, pre_fold = pre_step(pre_ref[0:1, :], pre_ref[1:2, :], add_parts(sums_in_ref, 0))
    one_now = one_ref[...] * action_share(pre_cont, pre_fold)
    columns = one_columns(one_now * live_ref[...], share_root_ref[...], share_fc_ref[...])
    for k, row in enumerate(one_rows(columns)):
        out_ref[k] = (turn_ref[k] + 4.0 * row) / total_weight
    for k in range(3, 6):
        out_ref[k] = turn_ref[k] / total_weight
    pre_out_ref[...] = (pre_ref[2:3, :] + 4.0 * one_now) / total_weight


def solve(arrived, range_one, range_two, low, high, compat):
    one_row = range_one.reshape(1, H)
    two_row = range_two.reshape(1, H)
    pair = (2, H)
    first_count = lax.axis_size(FIRST_SUM)
    key_now, live, share, cont, *state = pl.pallas_call(
        first_kernel,
        out_shape=[
            jax.ShapeDtypeStruct((ITERS - 1, 2, PADDED), jnp.int32),
            *rows_of(pair, (2, 1), (first_count, 1, 2 * H), *([pair] * 10), (6, 2, H)),
        ],
        scratch_shapes=pair_scratch(),
        name="first",
    )(arrived, low, high, one_row, two_row, compat)
    parts = whole_parts(cont)
    cont, share_root, share_fc, turns, pre = pl.pallas_call(
        second_kernel,
        out_shape=rows_of((first_count, 1, H), pair, pair, (6, 2, H), (3, H)),
        scratch_shapes=pair_scratch(),
        name="second",
    )(key_now, live, one_row, two_row, share, compat, parts, *state)
    parts = whole_parts(cont)
    turns, pre = pl.pallas_call(
        last_kernel,
        out_shape=rows_of((6, 2, H), (1, H)),
        name="last",
    )(live, one_row, parts, share_root, share_fc, turns, pre)
    return jnp.swapaxes(turns, 0, 1), pre.reshape(H)


def exchanged(copies, axis):
    return lax.all_to_all(copies, axis, split_axis=0, concat_axis=0, tiled=True)


def whole_parts(copies):
    part = jnp.sum(exchanged(copies, FIRST_SUM), axis=0)
    return sent_to_all(part, SECOND_SUM)


ROWS = 80


def pack_kernel(first_hand_ref, strength_ref, board_ref, weight_ref, cards_ref, out_ref):
    groups, rows, capacity = out_ref.shape
    hand_block = strength_ref.shape[0]
    used = ITERS - 1
    hand = first_hand_ref[0, 0] + lax.broadcasted_iota(jnp.int32, (hand_block, capacity), 0)
    flop_live = (board_ref[...] == 1) & (hand < HANDS)
    extra = used * hand_block
    for group in range(groups):
        for counter in range(used):
            out_ref[group, hand_block * counter : hand_block * (counter + 1), :] = jnp.where(
                flop_live, strength_ref[:, counter, :] + 1, 0
            )
        out_ref[group, extra : extra + 1, :] = weight_ref[...]
        for counter in range(used):
            row = extra + 1 + 2 * counter
            out_ref[group, row : row + 2, :] = cards_ref[counter]
        blank = extra + 1 + 2 * used
        out_ref[group, blank:, :] = jnp.zeros((rows - blank, capacity), jnp.int32)


def packed(first_hand, strength, board_mask, flop_weight, runout, groups):
    capacity = strength.shape[0]
    return pl.pallas_call(
        pack_kernel,
        out_shape=jax.ShapeDtypeStruct((groups, ROWS, capacity), jnp.int32),
        in_specs=[
            pl.BlockSpec(memory_space=pltpu.SMEM),
            *([pl.BlockSpec(memory_space=pltpu.VMEM)] * 4),
        ],
        name="pack",
    )(
        first_hand.astype(jnp.int32).reshape(1, 1),
        jnp.transpose(strength, (2, 1, 0)),
        board_mask.T,
        flop_weight.reshape(1, capacity),
        jnp.transpose(runout, (1, 2, 0)),
    )


def route_kernel(group_ref, slots_ref, out_ref):
    groups, rows, capacity = slots_ref.shape
    pairs = out_ref.shape[0]
    weight_row = (ITERS - 1) * (H // pairs)
    row = lax.broadcasted_iota(jnp.int32, (1, capacity), 1)
    counts = [
        jnp.sum((slots_ref[g, weight_row : weight_row + 1, :] > 0).astype(jnp.int32))
        for g in range(groups)
    ]
    totals = [[jnp.zeros((pairs, LINE), jnp.float32) for part in range(4)] for odd in range(2)]
    pair = lax.broadcasted_iota(jnp.int32, (pairs, capacity), 0)
    blank = jnp.zeros((LINE - rows, capacity), jnp.int32)
    for g in range(groups):
        place = -2 * pairs * group_ref[0, 0] + jnp.zeros((1, capacity), jnp.int32)
        for other in range(groups):
            place = place + jnp.minimum(counts[other], row + int(other < g))
        place = jnp.where(row < counts[g], place, -1)
        values = jnp.concatenate([slots_ref[g], blank])
        picks = [
            (place == 2 * pair + odd).astype(jnp.float32).astype(jnp.bfloat16) for odd in range(2)
        ]
        for part in range(4):
            digits = (values >> (8 * part)) & (PART - 1)
            digits = digits.astype(jnp.float32).astype(jnp.bfloat16)
            for odd in range(2):
                found = lax.dot_general(
                    picks[odd], digits, (((1,), (1,)), ((), ())), preferred_element_type=jnp.float32
                )
                totals[odd][part] = totals[odd][part] + found
    for odd in range(2):
        whole = jnp.zeros((pairs, LINE), jnp.int32)
        for part in range(4):
            whole = whole + (totals[odd][part].astype(jnp.int32) << (8 * part))
        out_ref[:, 0, LINE * odd : LINE * (odd + 1)] = whole


def route(slots, group_id, pairs):
    return pl.pallas_call(
        route_kernel,
        out_shape=jax.ShapeDtypeStruct((pairs, 1, 2 * LINE), jnp.int32),
        in_specs=[pl.BlockSpec(memory_space=pltpu.SMEM), pl.BlockSpec(memory_space=pltpu.VMEM)],
        name="route",
    )(group_id.astype(jnp.int32).reshape(1, 1), slots)


def on_device(range_one, range_two, flop_weight, board_mask, runout, strength):
    groups = lax.axis_size(GRP)
    shards = lax.axis_size(INF)
    shard_id = lax.axis_index(INF)
    hand_block = strength.shape[2]
    first_hand = shard_id * hand_block
    low, high = (jnp.asarray(table).reshape(1, PADDED) for table in hand_cards(PADDED, HANDS))
    slots = exchanged(
        packed(first_hand, strength, board_mask, flop_weight, runout, groups), GRP
    )
    arrived = exchanged(route(slots, lax.axis_index(GRP), shards), INF)
    turn_reach, pre_reach = solve(
        arrived, range_one, range_two, low, high, compat_matrix(low, high)
    )
    return turn_reach, lax.dynamic_slice_in_dim(pre_reach, first_hand, hand_block)


def solution(mesh):
    split = Mesh(mesh.devices.reshape(2, 2, 4, 8, 2), ("grp_0", "grp_1", "inf_0", "inf_1", "inf_2"))
    return jax.shard_map(
        on_device,
        mesh=split,
        in_specs=(P(), P(), P(GRP), P(GRP, INF), P(GRP, None, None), P(GRP, None, INF)),
        out_specs=(P(GRP_INF, None, None), P(INF)),
        check_vma=False,
    )
```

```python
import jax
import jax.numpy as jnp
import numpy as np
from jax import lax
from jax.experimental import pallas as pl
from jax.experimental.pallas import tpu as pltpu
from jax.sharding import Mesh
from jax.sharding import PartitionSpec as P

HANDS = 1326
H = 1408
ITERS = 4
FLOP_GRP = 128
GRP = ("grp_0", "grp_1")
INF = ("inf_0", "inf_1", "inf_2")
GRP_INF = ("grp_0", "grp_1", "inf_0", "inf_1", "inf_2")


EPSILON = 0.01
FOLD_VALUE = -0.1


def sent_to_all(x, axis):
    copies = jnp.broadcast_to(x, (lax.axis_size(axis), *x.shape))
    return lax.all_to_all(copies, axis, split_axis=0, concat_axis=0, tiled=True)


def hand_cards(slot_total, real_total):
    low_list = []
    high_list = []
    for first_card in range(52):
        for second_card in range(first_card + 1, 52):
            low_list.append(first_card)
            high_list.append(second_card)
    low_table = np.full(slot_total, 52, np.int32)
    high_table = np.full(slot_total, 53, np.int32)
    used_count = min(slot_total, real_total)
    low_table[:used_count] = np.array(low_list[:used_count], np.int32)
    high_table[:used_count] = np.array(high_list[:used_count], np.int32)
    return (low_table, high_table)


def action_share(first_regret, second_regret):
    return (first_regret + EPSILON) / (first_regret + second_regret + 2.0 * EPSILON)


SCALE = 1.0 / HANDS
FLOP_TOTAL = 12.0 * FLOP_GRP * 4
LINE = 128
PART = 256
BLOCK = 128
WIDE = 1408
DEEP = 128
PADDED = 1408
FIRST_SUM = ("grp_1", "inf_0", "inf_2")
SECOND_SUM = ("grp_0", "inf_1")


def compat_kernel(low_ref, high_ref, out_ref):
    def rows(step, carry):
        first = pl.multiple_of(step * BLOCK, BLOCK)
        low_col = jnp.broadcast_to(low_ref[:, pl.ds(first, BLOCK)], (BLOCK, BLOCK)).T
        high_col = jnp.broadcast_to(high_ref[:, pl.ds(first, BLOCK)], (BLOCK, BLOCK)).T
        for start in range(0, PADDED, BLOCK):
            low_here = low_ref[:, start : start + BLOCK]
            high_here = high_ref[:, start : start + BLOCK]
            apart = (low_col != low_here) & (low_col != high_here)
            apart = apart & (high_col != low_here) & (high_col != high_here)
            out_ref[pl.ds(first, BLOCK), start : start + BLOCK] = jnp.where(
                apart, 1.0, 0.0
            ).astype(jnp.bfloat16)
        return carry

    lax.fori_loop(0, H // BLOCK, rows, 0)


def compat_matrix(low, high):
    return pl.pallas_call(
        compat_kernel,
        out_shape=jax.ShapeDtypeStruct((H, PADDED), jnp.bfloat16),
        name="compat",
        compiler_params=pltpu.CompilerParams(vmem_limit_bytes=12 << 20),
    )(low, high)


def pair_sums(key_ref, counter, columns, compat_ref, lhs_ref, low_ref, sums_ref, col_ref, fetch=None):
    alive = (key_ref[counter, :, :H] >= 0).astype(jnp.float32)
    lhs_ref[...] = jnp.zeros((16, H), jnp.float32)
    for k, column in columns.items():
        lhs_ref[2 * k : 2 * k + 2, :] = column * alive
    low_ref[...] = lhs_ref[...].astype(jnp.bfloat16)

    def key_column(step, carry):
        first = pl.multiple_of(step * BLOCK, BLOCK)
        for flop in range(2):
            keys = key_ref[counter, flop : flop + 1, pl.ds(first, BLOCK)]
            col_ref[flop, pl.ds(first, BLOCK), :] = jnp.broadcast_to(keys, (BLOCK, BLOCK)).T
        return carry

    lax.fori_loop(0, H // BLOCK, key_column, 0)
    if fetch is not None:
        fetch.wait()

    def mine(step, carry):
        start = pl.multiple_of(step * WIDE, WIDE)
        weight_total = jnp.zeros((16, WIDE), jnp.float32)
        totals = [jnp.zeros((16, WIDE), jnp.float32) for flop in range(2)]
        rows = [key_ref[counter, flop : flop + 1, pl.ds(start, WIDE)] for flop in range(2)]
        for first in range(0, H, DEEP):
            depth = min(DEEP, H - first)
            lhs = low_ref[:, first : first + depth]
            most = compat_ref[first : first + depth, pl.ds(start, WIDE)]
            weight_total = weight_total + jnp.dot(lhs, most, preferred_element_type=jnp.float32)
            for flop in range(2):
                parts = []
                key_col = col_ref[flop, first : first + depth, :]
                for lane in range(0, WIDE, BLOCK):
                    gap = rows[flop][:, lane : lane + BLOCK] - key_col
                    parts.append(gap.astype(jnp.float32).astype(jnp.bfloat16))
                sign = jnp.concatenate(parts, axis=1) if len(parts) > 1 else parts[0]
                one = jnp.bfloat16(1)
                sign = jnp.minimum(jnp.maximum(sign, -one), one) * most
                totals[flop] = totals[flop] + jnp.dot(
                    lhs, sign, preferred_element_type=jnp.float32
                )
        row_flop = lax.broadcasted_iota(jnp.int32, (16, WIDE), 0) & 1
        sums_ref[0, :, pl.ds(start, WIDE)] = jnp.where(row_flop == 0, totals[0], totals[1])
        sums_ref[1, :, pl.ds(start, WIDE)] = weight_total
        return carry

    lax.fori_loop(0, PADDED // WIDE, mine, 0)
    sign_sum = {k: sums_ref[0, 2 * k : 2 * k + 2, :H] * alive for k in columns}
    weight_sum = {k: sums_ref[1, 2 * k : 2 * k + 2, :H] * alive for k in columns}
    return sign_sum, weight_sum


def two_values(sign_sum, weight_sum, share_root, share_fc):
    v_cc = 0.5 * SCALE * sign_sum[1]
    v_cbf = -0.5 * SCALE * (weight_sum[0] - weight_sum[1])
    v_cbc = 1.5 * SCALE * (sign_sum[0] - sign_sum[1])
    v_bf = 0.5 * SCALE * weight_sum[2]
    v_bc = 1.5 * SCALE * (sign_sum[0] - sign_sum[2])
    u_fc = share_fc * v_cbf + (1.0 - share_fc) * v_cbc
    v_check = v_cc + u_fc
    v_bet = v_bf + v_bc
    u_root = share_root * v_check + (1.0 - share_root) * v_bet
    return v_cbf, v_cbc, u_fc, v_check, v_bet, u_root


def one_values(sign_sum, weight_sum, share_ac, share_fb):
    w_cc = 0.5 * SCALE * sign_sum[4]
    w_cbf = 0.5 * SCALE * weight_sum[5]
    w_cbc = 1.5 * SCALE * (sign_sum[4] - sign_sum[5])
    w_bf = -0.5 * SCALE * (weight_sum[3] - weight_sum[4])
    w_bc = 1.5 * SCALE * (sign_sum[3] - sign_sum[4])
    x_bet = w_cbf + w_cbc
    u_ac = share_ac * w_cc + (1.0 - share_ac) * x_bet
    u_fb = share_fb * w_bf + (1.0 - share_fb) * w_bc
    return w_cc, x_bet, u_ac, w_bf, w_bc, u_fb


def two_regrets(regrets, values):
    root_check, root_bet, fc_fold, fc_call = regrets
    v_cbf, v_cbc, u_fc, v_check, v_bet, u_root = values
    return (
        jnp.maximum(root_check + v_check - u_root, 0.0),
        jnp.maximum(root_bet + v_bet - u_root, 0.0),
        jnp.maximum(fc_fold + v_cbf - u_fc, 0.0),
        jnp.maximum(fc_call + v_cbc - u_fc, 0.0),
    )


def one_regrets(regrets, values):
    ac_check, ac_bet, fb_fold, fb_call = regrets
    w_cc, x_bet, u_ac, w_bf, w_bc, u_fb = values
    return (
        jnp.maximum(ac_check + w_cc - u_ac, 0.0),
        jnp.maximum(ac_bet + x_bet - u_ac, 0.0),
        jnp.maximum(fb_fold + w_bf - u_fb, 0.0),
        jnp.maximum(fb_call + w_bc - u_fb, 0.0),
    )


def pre_step(pre_cont, pre_fold, cont_value):
    share_pre = action_share(pre_cont, pre_fold)
    u_pre = share_pre * cont_value + (1.0 - share_pre) * FOLD_VALUE
    return (
        jnp.maximum(pre_cont + cont_value - u_pre, 0.0),
        jnp.maximum(pre_fold + FOLD_VALUE - u_pre, 0.0),
    )


def one_columns(one_all, share_root, share_fc):
    one_check = one_all * share_root
    return {3: one_all, 4: one_check, 5: one_check * share_fc}


def two_columns(two_all, share_ac, share_fb):
    return {0: two_all, 1: two_all * share_ac, 2: two_all * share_fb}


def one_rows(columns):
    return columns[4], columns[3] - columns[4], columns[4] - columns[5]


def two_rows(columns):
    return columns[1], columns[0] - columns[2], columns[0] - columns[1]


def flop_value(share, u_root):
    part = share * u_root
    return part[0:1, :] + part[1:2, :]


def add_parts(parts_ref, start):
    total = parts_ref[0, :, start : start + H]
    for k in range(1, parts_ref.shape[0]):
        total = total + parts_ref[k, :, start : start + H]
    return total


def spread(copies_ref, start, value):
    for k in range(copies_ref.shape[0]):
        copies_ref[k, :, start : start + H] = value


def read_flops(arrived_ref, low_ref, high_ref, key_ref, live_ref, share_ref):
    used = key_ref.shape[0]
    shards = arrived_ref.shape[0]
    hand_block = H // shards
    for shard in range(shards):
        line = arrived_ref[shard] - 1
        for flop in range(2):
            for counter in range(used):
                first = LINE * flop + hand_block * counter
                key_ref[
                    counter, flop : flop + 1, hand_block * shard : hand_block * (shard + 1)
                ] = line[:, first : first + hand_block]
    live_ref[...] = (key_ref[0, :, :H] >= 0).astype(jnp.float32)
    low = low_ref[...]
    high = high_ref[...]
    for flop in range(2):
        first = LINE * flop + hand_block * used
        extra = arrived_ref[0, :, first : first + 1 + 2 * used]
        share_ref[flop : flop + 1, :] = extra[:, 0:1].astype(jnp.float32) / FLOP_TOTAL
        for counter in range(used):
            turn = extra[:, 1 + 2 * counter : 2 + 2 * counter]
            river = extra[:, 2 + 2 * counter : 3 + 2 * counter]
            blocked = (low == turn) | (low == river) | (high == turn) | (high == river)
            blocked = blocked | (lax.broadcasted_iota(jnp.int32, (1, PADDED), 1) >= H)
            row = key_ref[counter, flop : flop + 1, :]
            key_ref[counter, flop : flop + 1, :] = jnp.where(blocked, -1, row)


def first_kernel(
    arrived_ref, low_ref, high_ref, one_ref, two_ref, compat_hbm_ref,
    key_ref, live_ref, share_ref, cont_ref,
    root_check_ref, root_bet_ref, fc_fold_ref, fc_call_ref,
    ac_check_ref, ac_bet_ref, fb_fold_ref, fb_call_ref, share_root_ref, share_fc_ref, turn_ref,
    lhs_ref, low_part_ref, sums_ref, col_ref, compat_ref, compat_sem,
):
    fetch = pltpu.make_async_copy(compat_hbm_ref, compat_ref, compat_sem)
    fetch.start()
    scratch = (compat_ref, lhs_ref, low_part_ref, sums_ref, col_ref)
    read_flops(arrived_ref, low_ref, high_ref, key_ref, live_ref, share_ref)
    live = live_ref[...]
    share = share_ref[...]
    zero = jnp.zeros((2, H), jnp.float32)
    zero_row = jnp.zeros((1, H), jnp.float32)
    two_all = two_ref[...] * live
    start = action_share(zero, zero)
    one_all = one_ref[...] * action_share(zero_row, zero_row) * live
    one_cols = one_columns(one_all, start, start)
    two_cols = two_columns(two_all, start, start)
    sign_sum, weight_sum = pair_sums(key_ref, 0, {**two_cols, **one_cols}, *scratch, fetch)
    values = two_values(sign_sum, weight_sum, start, start)
    spread(cont_ref, 0, flop_value(share, values[5]))
    regrets = two_regrets((zero, zero, zero, zero), values)
    others = one_regrets((zero, zero, zero, zero), one_values(sign_sum, weight_sum, start, start))
    turns = [*one_rows(one_cols), *two_rows(two_cols)]

    share_root = action_share(regrets[0], regrets[1])
    share_fc = action_share(regrets[2], regrets[3])
    two_cols = two_columns(
        two_all, action_share(others[0], others[1]), action_share(others[2], others[3])
    )
    sign_sum, weight_sum = pair_sums(key_ref, 1, two_cols, *scratch)
    values = two_values(sign_sum, weight_sum, share_root, share_fc)
    spread(cont_ref, H, flop_value(share, values[5]))
    regrets = two_regrets(regrets, values)
    for k, row in enumerate(two_rows(two_cols)):
        turns[3 + k] = turns[3 + k] + 2.0 * row
    root_check_ref[...], root_bet_ref[...], fc_fold_ref[...], fc_call_ref[...] = regrets
    ac_check_ref[...], ac_bet_ref[...], fb_fold_ref[...], fb_call_ref[...] = others
    share_root_ref[...] = share_root
    share_fc_ref[...] = share_fc
    for k in range(6):
        turn_ref[k] = turns[k]


def second_kernel(
    key_ref, live_ref, one_ref, two_ref, share_ref, compat_hbm_ref, sums_in_ref,
    root_check_ref, root_bet_ref, fc_fold_ref, fc_call_ref,
    ac_check_ref, ac_bet_ref, fb_fold_ref, fb_call_ref, share_root_ref, share_fc_ref, turn_ref,
    cont_ref, out_root_ref, out_fc_ref, out_turn_ref, out_pre_ref,
    lhs_ref, low_ref, sums_ref, col_ref, compat_ref, compat_sem,
):
    fetch = pltpu.make_async_copy(compat_hbm_ref, compat_ref, compat_sem)
    fetch.start()
    scratch = (compat_ref, lhs_ref, low_ref, sums_ref, col_ref)
    live = live_ref[...]
    zero_row = jnp.zeros((1, H), jnp.float32)
    two_all = two_ref[...] * live
    one_range = one_ref[...]
    turns = [turn_ref[k] for k in range(6)]
    pre_sum = one_range * action_share(zero_row, zero_row)
    pre_cont, pre_fold = pre_step(zero_row, zero_row, add_parts(sums_in_ref, 0))
    one_now = one_range * action_share(pre_cont, pre_fold)
    pre_sum = pre_sum + 2.0 * one_now
    one_cols = one_columns(one_now * live, share_root_ref[...], share_fc_ref[...])
    for k, row in enumerate(one_rows(one_cols)):
        turns[k] = turns[k] + 2.0 * row
    others = (ac_check_ref[...], ac_bet_ref[...], fb_fold_ref[...], fb_call_ref[...])
    share_ac = action_share(others[0], others[1])
    share_fb = action_share(others[2], others[3])
    sign_sum, weight_sum = pair_sums(key_ref, 1, one_cols, *scratch, fetch)
    others = one_regrets(others, one_values(sign_sum, weight_sum, share_ac, share_fb))

    pre_cont, pre_fold = pre_step(pre_cont, pre_fold, add_parts(sums_in_ref, H))
    one_now = one_range * action_share(pre_cont, pre_fold)
    pre_sum = pre_sum + 3.0 * one_now
    regrets = (root_check_ref[...], root_bet_ref[...], fc_fold_ref[...], fc_call_ref[...])
    share_root = action_share(regrets[0], regrets[1])
    share_fc = action_share(regrets[2], regrets[3])
    share_ac = action_share(others[0], others[1])
    share_fb = action_share(others[2], others[3])
    one_cols = one_columns(one_now * live, share_root, share_fc)
    two_cols = two_columns(two_all, share_ac, share_fb)
    for k, row in enumerate((*one_rows(one_cols), *two_rows(two_cols))):
        turns[k] = turns[k] + 3.0 * row
    sign_sum, weight_sum = pair_sums(key_ref, 2, {**two_cols, **one_cols}, *scratch)
    values = two_values(sign_sum, weight_sum, share_root, share_fc)
    spread(cont_ref, 0, flop_value(share_ref[...], values[5]))
    regrets = two_regrets(regrets, values)
    others = one_regrets(others, one_values(sign_sum, weight_sum, share_ac, share_fb))
    two_cols = two_columns(
        two_all, action_share(others[0], others[1]), action_share(others[2], others[3])
    )
    for k, row in enumerate(two_rows(two_cols)):
        turns[3 + k] = turns[3 + k] + 4.0 * row
    out_root_ref[...] = action_share(regrets[0], regrets[1])
    out_fc_ref[...] = action_share(regrets[2], regrets[3])
    for k in range(6):
        out_turn_ref[k] = turns[k]
    out_pre_ref[0:1, :] = pre_cont
    out_pre_ref[1:2, :] = pre_fold
    out_pre_ref[2:3, :] = pre_sum


def pair_scratch():
    return [
        pltpu.VMEM((16, H), jnp.float32),
        pltpu.VMEM((16, H), jnp.bfloat16),
        pltpu.VMEM((2, 16, PADDED), jnp.float32),
        pltpu.VMEM((2, H, BLOCK), jnp.int32),
        pltpu.VMEM((H, PADDED), jnp.bfloat16),
        pltpu.SemaphoreType.DMA,
    ]


def in_vmem(count):
    return [pl.BlockSpec(memory_space=pltpu.VMEM)] * count


def in_hbm():
    return pl.BlockSpec(memory_space=pltpu.HBM)


def rows_of(*shapes):
    return [jax.ShapeDtypeStruct(shape, jnp.float32) for shape in shapes]


def last_kernel(
    live_ref, one_ref, sums_in_ref, share_root_ref, share_fc_ref, turn_ref, pre_ref,
    out_ref, pre_out_ref,
):
    total_weight = ITERS * (ITERS + 1) / 2.0
    pre_cont, pre_fold = pre_step(pre_ref[0:1, :], pre_ref[1:2, :], add_parts(sums_in_ref, 0))
    one_now = one_ref[...] * action_share(pre_cont, pre_fold)
    columns = one_columns(one_now * live_ref[...], share_root_ref[...], share_fc_ref[...])
    for k, row in enumerate(one_rows(columns)):
        out_ref[k] = (turn_ref[k] + 4.0 * row) / total_weight
    for k in range(3, 6):
        out_ref[k] = turn_ref[k] / total_weight
    pre_out_ref[...] = (pre_ref[2:3, :] + 4.0 * one_now) / total_weight


def solve(arrived, range_one, range_two, low, high, compat):
    one_row = range_one.reshape(1, H)
    two_row = range_two.reshape(1, H)
    pair = (2, H)
    first_count = lax.axis_size(FIRST_SUM)
    key_now, live, share, cont, *state = pl.pallas_call(
        first_kernel,
        out_shape=[
            jax.ShapeDtypeStruct((ITERS - 1, 2, PADDED), jnp.int32),
            *rows_of(pair, (2, 1), (first_count, 1, 2 * H), *([pair] * 10), (6, 2, H)),
        ],
        in_specs=[*in_vmem(5), in_hbm()],
        scratch_shapes=pair_scratch(),
        name="first",
        compiler_params=pltpu.CompilerParams(vmem_limit_bytes=20 << 20),
    )(arrived, low, high, one_row, two_row, compat)
    parts = whole_parts(cont)
    cont, share_root, share_fc, turns, pre = pl.pallas_call(
        second_kernel,
        out_shape=rows_of((first_count, 1, H), pair, pair, (6, 2, H), (3, H)),
        in_specs=[*in_vmem(5), in_hbm(), *in_vmem(12)],
        scratch_shapes=pair_scratch(),
        name="second",
        compiler_params=pltpu.CompilerParams(vmem_limit_bytes=20 << 20),
    )(key_now, live, one_row, two_row, share, compat, parts, *state)
    parts = whole_parts(cont)
    turns, pre = pl.pallas_call(
        last_kernel,
        out_shape=rows_of((6, 2, H), (1, H)),
        name="last",
        compiler_params=pltpu.CompilerParams(vmem_limit_bytes=8 << 20),
    )(live, one_row, parts, share_root, share_fc, turns, pre)
    return jnp.swapaxes(turns, 0, 1), pre.reshape(H)


def exchanged(copies, axis):
    return lax.all_to_all(copies, axis, split_axis=0, concat_axis=0, tiled=True)


def whole_parts(copies):
    part = jnp.sum(exchanged(copies, FIRST_SUM), axis=0)
    return sent_to_all(part, SECOND_SUM)


ROWS = 80


def pack_kernel(first_hand_ref, strength_ref, board_ref, weight_ref, cards_ref, out_ref):
    groups, rows, capacity = out_ref.shape
    hand_block = strength_ref.shape[0]
    used = ITERS - 1
    hand = first_hand_ref[0, 0] + lax.broadcasted_iota(jnp.int32, (hand_block, capacity), 0)
    flop_live = (board_ref[...] == 1) & (hand < HANDS)
    extra = used * hand_block
    for group in range(groups):
        for counter in range(used):
            out_ref[group, hand_block * counter : hand_block * (counter + 1), :] = jnp.where(
                flop_live, strength_ref[:, counter, :] + 1, 0
            )
        out_ref[group, extra : extra + 1, :] = weight_ref[...]
        for counter in range(used):
            row = extra + 1 + 2 * counter
            out_ref[group, row : row + 2, :] = cards_ref[counter]
        blank = extra + 1 + 2 * used
        out_ref[group, blank:, :] = jnp.zeros((rows - blank, capacity), jnp.int32)


def packed(first_hand, strength, board_mask, flop_weight, runout, groups):
    capacity = strength.shape[0]
    return pl.pallas_call(
        pack_kernel,
        out_shape=jax.ShapeDtypeStruct((groups, ROWS, capacity), jnp.int32),
        in_specs=[
            pl.BlockSpec(memory_space=pltpu.SMEM),
            *([pl.BlockSpec(memory_space=pltpu.VMEM)] * 4),
        ],
        name="pack",
    )(
        first_hand.astype(jnp.int32).reshape(1, 1),
        jnp.transpose(strength, (2, 1, 0)),
        board_mask.T,
        flop_weight.reshape(1, capacity),
        jnp.transpose(runout, (1, 2, 0)),
    )


def route_kernel(group_ref, slots_ref, out_ref):
    groups, rows, capacity = slots_ref.shape
    pairs = out_ref.shape[0]
    weight_row = (ITERS - 1) * (H // pairs)
    row = lax.broadcasted_iota(jnp.int32, (1, capacity), 1)
    counts = [
        jnp.sum((slots_ref[g, weight_row : weight_row + 1, :] > 0).astype(jnp.int32))
        for g in range(groups)
    ]
    totals = [[jnp.zeros((pairs, LINE), jnp.float32) for part in range(4)] for odd in range(2)]
    pair = lax.broadcasted_iota(jnp.int32, (pairs, capacity), 0)
    blank = jnp.zeros((LINE - rows, capacity), jnp.int32)
    for g in range(groups):
        place = -2 * pairs * group_ref[0, 0] + jnp.zeros((1, capacity), jnp.int32)
        for other in range(groups):
            place = place + jnp.minimum(counts[other], row + int(other < g))
        place = jnp.where(row < counts[g], place, -1)
        values = jnp.concatenate([slots_ref[g], blank])
        picks = [
            (place == 2 * pair + odd).astype(jnp.float32).astype(jnp.bfloat16) for odd in range(2)
        ]
        for part in range(4):
            digits = (values >> (8 * part)) & (PART - 1)
            digits = digits.astype(jnp.float32).astype(jnp.bfloat16)
            for odd in range(2):
                found = lax.dot_general(
                    picks[odd], digits, (((1,), (1,)), ((), ())), preferred_element_type=jnp.float32
                )
                totals[odd][part] = totals[odd][part] + found
    for odd in range(2):
        whole = jnp.zeros((pairs, LINE), jnp.int32)
        for part in range(4):
            whole = whole + (totals[odd][part].astype(jnp.int32) << (8 * part))
        out_ref[:, 0, LINE * odd : LINE * (odd + 1)] = whole


def route(slots, group_id, pairs):
    return pl.pallas_call(
        route_kernel,
        out_shape=jax.ShapeDtypeStruct((pairs, 1, 2 * LINE), jnp.int32),
        in_specs=[pl.BlockSpec(memory_space=pltpu.SMEM), pl.BlockSpec(memory_space=pltpu.VMEM)],
        name="route",
        compiler_params=pltpu.CompilerParams(vmem_limit_bytes=12 << 20),
    )(group_id.astype(jnp.int32).reshape(1, 1), slots)


def on_device(range_one, range_two, flop_weight, board_mask, runout, strength):
    groups = lax.axis_size(GRP)
    shards = lax.axis_size(INF)
    shard_id = lax.axis_index(INF)
    hand_block = strength.shape[2]
    first_hand = shard_id * hand_block
    low, high = (jnp.asarray(table).reshape(1, PADDED) for table in hand_cards(PADDED, HANDS))
    slots = exchanged(
        packed(first_hand, strength, board_mask, flop_weight, runout, groups), GRP
    )
    arrived = exchanged(route(slots, lax.axis_index(GRP), shards), INF)
    turn_reach, pre_reach = solve(
        arrived,
        range_one,
        range_two,
        low,
        high,
        pltpu.with_memory_space_constraint(compat_matrix(low, high), pltpu.HBM),
    )
    return turn_reach, lax.dynamic_slice_in_dim(pre_reach, first_hand, hand_block)


def solution(mesh):
    split = Mesh(mesh.devices.reshape(2, 2, 4, 8, 2), ("grp_0", "grp_1", "inf_0", "inf_1", "inf_2"))
    return jax.shard_map(
        on_device,
        mesh=split,
        in_specs=(P(), P(), P(GRP), P(GRP, INF), P(GRP, None, None), P(GRP, None, INF)),
        out_specs=(P(GRP_INF, None, None), P(INF)),
        check_vma=False,
    )
```

```python
import jax
import jax.numpy as jnp
import numpy as np
from jax import lax
from jax.experimental import pallas as pl
from jax.experimental.pallas import tpu as pltpu
from jax.sharding import Mesh
from jax.sharding import PartitionSpec as P

HANDS = 1326
H = 1408
ITERS = 4
FLOP_GRP = 128
GRP = ("grp_0", "grp_1")
INF = ("inf_0", "inf_1", "inf_2")
GRP_INF = ("grp_0", "grp_1", "inf_0", "inf_1", "inf_2")


EPSILON = 0.01
FOLD_VALUE = -0.1


def sent_to_all(x, axis):
    copies = jnp.broadcast_to(x, (lax.axis_size(axis), *x.shape))
    return lax.all_to_all(copies, axis, split_axis=0, concat_axis=0, tiled=True)


def hand_cards(slot_total, real_total):
    low_list = []
    high_list = []
    for first_card in range(52):
        for second_card in range(first_card + 1, 52):
            low_list.append(first_card)
            high_list.append(second_card)
    low_table = np.full(slot_total, 52, np.int32)
    high_table = np.full(slot_total, 53, np.int32)
    used_count = min(slot_total, real_total)
    low_table[:used_count] = np.array(low_list[:used_count], np.int32)
    high_table[:used_count] = np.array(high_list[:used_count], np.int32)
    return (low_table, high_table)


def action_share(first_regret, second_regret):
    return (first_regret + EPSILON) / (first_regret + second_regret + 2.0 * EPSILON)


SCALE = 1.0 / HANDS
FLOP_TOTAL = 12.0 * FLOP_GRP * 4
LINE = 128
PART = 256
BLOCK = 128
WIDE = 1408
DEEP = 128
PADDED = 1408
FIRST_SUM = ("grp_1", "inf_0", "inf_2")
SECOND_SUM = ("grp_0", "inf_1")


def compat_kernel(low_ref, high_ref, out_ref):
    def rows(step, carry):
        first = pl.multiple_of(step * BLOCK, BLOCK)
        low_col = jnp.broadcast_to(low_ref[:, pl.ds(first, BLOCK)], (BLOCK, BLOCK)).T
        high_col = jnp.broadcast_to(high_ref[:, pl.ds(first, BLOCK)], (BLOCK, BLOCK)).T
        for start in range(0, PADDED, BLOCK):
            low_here = low_ref[:, start : start + BLOCK]
            high_here = high_ref[:, start : start + BLOCK]
            apart = (low_col != low_here) & (low_col != high_here)
            apart = apart & (high_col != low_here) & (high_col != high_here)
            out_ref[pl.ds(first, BLOCK), start : start + BLOCK] = jnp.where(
                apart, 1.0, 0.0
            ).astype(jnp.bfloat16)
        return carry

    lax.fori_loop(0, H // BLOCK, rows, 0)


def compat_matrix(low, high):
    return pl.pallas_call(
        compat_kernel,
        out_shape=jax.ShapeDtypeStruct((H, PADDED), jnp.bfloat16),
        name="compat",
        compiler_params=pltpu.CompilerParams(vmem_limit_bytes=12 << 20),
    )(low, high)


def pair_sums(key_ref, counter, columns, compat_ref, lhs_ref, low_ref, sums_ref, col_ref, fetch=None):
    alive = (key_ref[counter, :, :H] >= 0).astype(jnp.float32)
    lhs_ref[...] = jnp.zeros((16, H), jnp.float32)
    for k, column in columns.items():
        lhs_ref[2 * k : 2 * k + 2, :] = column * alive
    low_ref[...] = lhs_ref[...].astype(jnp.bfloat16)

    def key_column(step, carry):
        first = pl.multiple_of(step * BLOCK, BLOCK)
        for flop in range(2):
            keys = key_ref[counter, flop : flop + 1, pl.ds(first, BLOCK)]
            col_ref[flop, pl.ds(first, BLOCK), :] = jnp.broadcast_to(keys, (BLOCK, BLOCK)).T
        return carry

    lax.fori_loop(0, H // BLOCK, key_column, 0)
    if fetch is not None:
        fetch.wait()

    def mine(step, carry):
        start = pl.multiple_of(step * WIDE, WIDE)
        weight_total = jnp.zeros((16, WIDE), jnp.float32)
        totals = [jnp.zeros((16, WIDE), jnp.float32) for flop in range(2)]
        rows = [key_ref[counter, flop : flop + 1, pl.ds(start, WIDE)] for flop in range(2)]
        for first in range(0, H, DEEP):
            depth = min(DEEP, H - first)
            lhs = low_ref[:, first : first + depth]
            most = compat_ref[first : first + depth, pl.ds(start, WIDE)]
            weight_total = weight_total + jnp.dot(lhs, most, preferred_element_type=jnp.float32)
            for flop in range(2):
                parts = []
                key_col = col_ref[flop, first : first + depth, :]
                for lane in range(0, WIDE, BLOCK):
                    gap = rows[flop][:, lane : lane + BLOCK] - key_col
                    parts.append(gap.astype(jnp.float32).astype(jnp.bfloat16))
                sign = jnp.concatenate(parts, axis=1) if len(parts) > 1 else parts[0]
                one = jnp.bfloat16(1)
                sign = jnp.minimum(jnp.maximum(sign, -one), one) * most
                totals[flop] = totals[flop] + jnp.dot(
                    lhs, sign, preferred_element_type=jnp.float32
                )
        row_flop = lax.broadcasted_iota(jnp.int32, (16, WIDE), 0) & 1
        sums_ref[0, :, pl.ds(start, WIDE)] = jnp.where(row_flop == 0, totals[0], totals[1])
        sums_ref[1, :, pl.ds(start, WIDE)] = weight_total
        return carry

    lax.fori_loop(0, PADDED // WIDE, mine, 0)
    sign_sum = {k: sums_ref[0, 2 * k : 2 * k + 2, :H] * alive for k in columns}
    weight_sum = {k: sums_ref[1, 2 * k : 2 * k + 2, :H] * alive for k in columns}
    return sign_sum, weight_sum


def two_values(sign_sum, weight_sum, share_root, share_fc):
    v_cc = 0.5 * SCALE * sign_sum[1]
    v_cbf = -0.5 * SCALE * (weight_sum[0] - weight_sum[1])
    v_cbc = 1.5 * SCALE * (sign_sum[0] - sign_sum[1])
    v_bf = 0.5 * SCALE * weight_sum[2]
    v_bc = 1.5 * SCALE * (sign_sum[0] - sign_sum[2])
    u_fc = share_fc * v_cbf + (1.0 - share_fc) * v_cbc
    v_check = v_cc + u_fc
    v_bet = v_bf + v_bc
    u_root = share_root * v_check + (1.0 - share_root) * v_bet
    return v_cbf, v_cbc, u_fc, v_check, v_bet, u_root


def one_values(sign_sum, weight_sum, share_ac, share_fb):
    w_cc = 0.5 * SCALE * sign_sum[4]
    w_cbf = 0.5 * SCALE * weight_sum[5]
    w_cbc = 1.5 * SCALE * (sign_sum[4] - sign_sum[5])
    w_bf = -0.5 * SCALE * (weight_sum[3] - weight_sum[4])
    w_bc = 1.5 * SCALE * (sign_sum[3] - sign_sum[4])
    x_bet = w_cbf + w_cbc
    u_ac = share_ac * w_cc + (1.0 - share_ac) * x_bet
    u_fb = share_fb * w_bf + (1.0 - share_fb) * w_bc
    return w_cc, x_bet, u_ac, w_bf, w_bc, u_fb


def two_regrets(regrets, values):
    root_check, root_bet, fc_fold, fc_call = regrets
    v_cbf, v_cbc, u_fc, v_check, v_bet, u_root = values
    return (
        jnp.maximum(root_check + v_check - u_root, 0.0),
        jnp.maximum(root_bet + v_bet - u_root, 0.0),
        jnp.maximum(fc_fold + v_cbf - u_fc, 0.0),
        jnp.maximum(fc_call + v_cbc - u_fc, 0.0),
    )


def one_regrets(regrets, values):
    ac_check, ac_bet, fb_fold, fb_call = regrets
    w_cc, x_bet, u_ac, w_bf, w_bc, u_fb = values
    return (
        jnp.maximum(ac_check + w_cc - u_ac, 0.0),
        jnp.maximum(ac_bet + x_bet - u_ac, 0.0),
        jnp.maximum(fb_fold + w_bf - u_fb, 0.0),
        jnp.maximum(fb_call + w_bc - u_fb, 0.0),
    )


def pre_step(pre_cont, pre_fold, cont_value):
    share_pre = action_share(pre_cont, pre_fold)
    u_pre = share_pre * cont_value + (1.0 - share_pre) * FOLD_VALUE
    return (
        jnp.maximum(pre_cont + cont_value - u_pre, 0.0),
        jnp.maximum(pre_fold + FOLD_VALUE - u_pre, 0.0),
    )


def one_columns(one_all, share_root, share_fc):
    one_check = one_all * share_root
    return {3: one_all, 4: one_check, 5: one_check * share_fc}


def two_columns(two_all, share_ac, share_fb):
    return {0: two_all, 1: two_all * share_ac, 2: two_all * share_fb}


def one_rows(columns):
    return columns[4], columns[3] - columns[4], columns[4] - columns[5]


def two_rows(columns):
    return columns[1], columns[0] - columns[2], columns[0] - columns[1]


def flop_value(share, u_root):
    part = share * u_root
    return part[0:1, :] + part[1:2, :]


def add_parts(parts_ref, start):
    total = parts_ref[0, :, start : start + H]
    for k in range(1, parts_ref.shape[0]):
        total = total + parts_ref[k, :, start : start + H]
    return total


def spread(copies_ref, start, value):
    for k in range(copies_ref.shape[0]):
        copies_ref[k, :, start : start + H] = value


def read_flops(arrived_ref, low_ref, high_ref, key_ref, live_ref, share_ref):
    used = key_ref.shape[0]
    shards = arrived_ref.shape[0]
    hand_block = H // shards
    for shard in range(shards):
        line = arrived_ref[shard] - 1
        for flop in range(2):
            for counter in range(used):
                first = LINE * flop + hand_block * counter
                key_ref[
                    counter, flop : flop + 1, hand_block * shard : hand_block * (shard + 1)
                ] = line[:, first : first + hand_block]
    live_ref[...] = (key_ref[0, :, :H] >= 0).astype(jnp.float32)
    low = low_ref[...]
    high = high_ref[...]
    for flop in range(2):
        first = LINE * flop + hand_block * used
        extra = arrived_ref[0, :, first : first + 1 + 2 * used]
        share_ref[flop : flop + 1, :] = extra[:, 0:1].astype(jnp.float32) / FLOP_TOTAL
        for counter in range(used):
            turn = extra[:, 1 + 2 * counter : 2 + 2 * counter]
            river = extra[:, 2 + 2 * counter : 3 + 2 * counter]
            blocked = (low == turn) | (low == river) | (high == turn) | (high == river)
            blocked = blocked | (lax.broadcasted_iota(jnp.int32, (1, PADDED), 1) >= H)
            row = key_ref[counter, flop : flop + 1, :]
            key_ref[counter, flop : flop + 1, :] = jnp.where(blocked, -1, row)


def first_kernel(
    arrived_ref, low_ref, high_ref, one_ref, two_ref, compat_hbm_ref,
    key_ref, live_ref, share_ref, cont_ref,
    root_check_ref, root_bet_ref, fc_fold_ref, fc_call_ref,
    ac_check_ref, ac_bet_ref, fb_fold_ref, fb_call_ref, share_root_ref, share_fc_ref, turn_ref,
    lhs_ref, low_part_ref, sums_ref, col_ref, compat_ref, compat_sem,
):
    fetch = pltpu.make_async_copy(compat_hbm_ref, compat_ref, compat_sem)
    fetch.start()
    scratch = (compat_ref, lhs_ref, low_part_ref, sums_ref, col_ref)
    read_flops(arrived_ref, low_ref, high_ref, key_ref, live_ref, share_ref)
    live = live_ref[...]
    share = share_ref[...]
    zero = jnp.zeros((2, H), jnp.float32)
    zero_row = jnp.zeros((1, H), jnp.float32)
    two_all = two_ref[...] * live
    start = action_share(zero, zero)
    one_all = one_ref[...] * action_share(zero_row, zero_row) * live
    one_cols = one_columns(one_all, start, start)
    two_cols = two_columns(two_all, start, start)
    sign_sum, weight_sum = pair_sums(key_ref, 0, {**two_cols, **one_cols}, *scratch, fetch)
    values = two_values(sign_sum, weight_sum, start, start)
    spread(cont_ref, 0, flop_value(share, values[5]))
    regrets = two_regrets((zero, zero, zero, zero), values)
    others = one_regrets((zero, zero, zero, zero), one_values(sign_sum, weight_sum, start, start))
    turns = [*one_rows(one_cols), *two_rows(two_cols)]

    share_root = action_share(regrets[0], regrets[1])
    share_fc = action_share(regrets[2], regrets[3])
    two_cols = two_columns(
        two_all, action_share(others[0], others[1]), action_share(others[2], others[3])
    )
    sign_sum, weight_sum = pair_sums(key_ref, 1, two_cols, *scratch)
    values = two_values(sign_sum, weight_sum, share_root, share_fc)
    spread(cont_ref, H, flop_value(share, values[5]))
    regrets = two_regrets(regrets, values)
    for k, row in enumerate(two_rows(two_cols)):
        turns[3 + k] = turns[3 + k] + 2.0 * row
    root_check_ref[...], root_bet_ref[...], fc_fold_ref[...], fc_call_ref[...] = regrets
    ac_check_ref[...], ac_bet_ref[...], fb_fold_ref[...], fb_call_ref[...] = others
    share_root_ref[...] = share_root
    share_fc_ref[...] = share_fc
    for k in range(6):
        turn_ref[k] = turns[k]


def second_kernel(
    key_ref, live_ref, one_ref, two_ref, share_ref, compat_hbm_ref, sums_in_ref,
    root_check_ref, root_bet_ref, fc_fold_ref, fc_call_ref,
    ac_check_ref, ac_bet_ref, fb_fold_ref, fb_call_ref, share_root_ref, share_fc_ref, turn_ref,
    cont_ref, out_root_ref, out_fc_ref, out_turn_ref, out_pre_ref,
    lhs_ref, low_ref, sums_ref, col_ref, compat_ref, compat_sem,
):
    fetch = pltpu.make_async_copy(compat_hbm_ref, compat_ref, compat_sem)
    fetch.start()
    scratch = (compat_ref, lhs_ref, low_ref, sums_ref, col_ref)
    live = live_ref[...]
    zero_row = jnp.zeros((1, H), jnp.float32)
    two_all = two_ref[...] * live
    one_range = one_ref[...]
    turns = [turn_ref[k] for k in range(6)]
    pre_sum = one_range * action_share(zero_row, zero_row)
    pre_cont, pre_fold = pre_step(zero_row, zero_row, add_parts(sums_in_ref, 0))
    one_now = one_range * action_share(pre_cont, pre_fold)
    pre_sum = pre_sum + 2.0 * one_now
    one_cols = one_columns(one_now * live, share_root_ref[...], share_fc_ref[...])
    for k, row in enumerate(one_rows(one_cols)):
        turns[k] = turns[k] + 2.0 * row
    others = (ac_check_ref[...], ac_bet_ref[...], fb_fold_ref[...], fb_call_ref[...])
    share_ac = action_share(others[0], others[1])
    share_fb = action_share(others[2], others[3])
    sign_sum, weight_sum = pair_sums(key_ref, 1, one_cols, *scratch, fetch)
    others = one_regrets(others, one_values(sign_sum, weight_sum, share_ac, share_fb))

    pre_cont, pre_fold = pre_step(pre_cont, pre_fold, add_parts(sums_in_ref, H))
    one_now = one_range * action_share(pre_cont, pre_fold)
    pre_sum = pre_sum + 3.0 * one_now
    regrets = (root_check_ref[...], root_bet_ref[...], fc_fold_ref[...], fc_call_ref[...])
    share_root = action_share(regrets[0], regrets[1])
    share_fc = action_share(regrets[2], regrets[3])
    share_ac = action_share(others[0], others[1])
    share_fb = action_share(others[2], others[3])
    one_cols = one_columns(one_now * live, share_root, share_fc)
    two_cols = two_columns(two_all, share_ac, share_fb)
    for k, row in enumerate((*one_rows(one_cols), *two_rows(two_cols))):
        turns[k] = turns[k] + 3.0 * row
    sign_sum, weight_sum = pair_sums(key_ref, 2, {**two_cols, **one_cols}, *scratch)
    values = two_values(sign_sum, weight_sum, share_root, share_fc)
    spread(cont_ref, 0, flop_value(share_ref[...], values[5]))
    regrets = two_regrets(regrets, values)
    others = one_regrets(others, one_values(sign_sum, weight_sum, share_ac, share_fb))
    two_cols = two_columns(
        two_all, action_share(others[0], others[1]), action_share(others[2], others[3])
    )
    for k, row in enumerate(two_rows(two_cols)):
        turns[3 + k] = turns[3 + k] + 4.0 * row
    out_root_ref[...] = action_share(regrets[0], regrets[1])
    out_fc_ref[...] = action_share(regrets[2], regrets[3])
    for k in range(6):
        out_turn_ref[k] = turns[k]
    out_pre_ref[0:1, :] = pre_cont
    out_pre_ref[1:2, :] = pre_fold
    out_pre_ref[2:3, :] = pre_sum


def pair_scratch():
    return [
        pltpu.VMEM((16, H), jnp.float32),
        pltpu.VMEM((16, H), jnp.bfloat16),
        pltpu.VMEM((2, 16, PADDED), jnp.float32),
        pltpu.VMEM((2, H, BLOCK), jnp.int32),
        pltpu.VMEM((H, PADDED), jnp.bfloat16),
        pltpu.SemaphoreType.DMA,
    ]


def in_vmem(count):
    return [pl.BlockSpec(memory_space=pltpu.VMEM)] * count


def in_hbm():
    return pl.BlockSpec(memory_space=pltpu.HBM)


def rows_of(*shapes):
    return [jax.ShapeDtypeStruct(shape, jnp.float32) for shape in shapes]


def last_kernel(
    live_ref, one_ref, sums_in_ref, share_root_ref, share_fc_ref, turn_ref, pre_ref,
    out_ref, pre_out_ref,
):
    total_weight = ITERS * (ITERS + 1) / 2.0
    pre_cont, pre_fold = pre_step(pre_ref[0:1, :], pre_ref[1:2, :], add_parts(sums_in_ref, 0))
    one_now = one_ref[...] * action_share(pre_cont, pre_fold)
    columns = one_columns(one_now * live_ref[...], share_root_ref[...], share_fc_ref[...])
    for k, row in enumerate(one_rows(columns)):
        out_ref[k] = (turn_ref[k] + 4.0 * row) / total_weight
    for k in range(3, 6):
        out_ref[k] = turn_ref[k] / total_weight
    pre_out_ref[...] = (pre_ref[2:3, :] + 4.0 * one_now) / total_weight


def solve(arrived, range_one, range_two, low, high, compat):
    one_row = range_one.reshape(1, H)
    two_row = range_two.reshape(1, H)
    pair = (2, H)
    first_count = lax.axis_size(FIRST_SUM)
    key_now, live, share, cont, *state = pl.pallas_call(
        first_kernel,
        out_shape=[
            jax.ShapeDtypeStruct((ITERS - 1, 2, PADDED), jnp.int32),
            *rows_of(pair, (2, 1), (first_count, 1, 2 * H), *([pair] * 10), (6, 2, H)),
        ],
        in_specs=[*in_vmem(5), in_hbm()],
        scratch_shapes=pair_scratch(),
        name="first",
        compiler_params=pltpu.CompilerParams(vmem_limit_bytes=20 << 20),
    )(arrived, low, high, one_row, two_row, compat)
    parts = whole_parts(cont)
    cont, share_root, share_fc, turns, pre = pl.pallas_call(
        second_kernel,
        out_shape=rows_of((first_count, 1, H), pair, pair, (6, 2, H), (3, H)),
        in_specs=[*in_vmem(5), in_hbm(), *in_vmem(12)],
        scratch_shapes=pair_scratch(),
        name="second",
        compiler_params=pltpu.CompilerParams(vmem_limit_bytes=20 << 20),
    )(key_now, live, one_row, two_row, share, compat, parts, *state)
    parts = whole_parts(cont)
    turns, pre = pl.pallas_call(
        last_kernel,
        out_shape=rows_of((6, 2, H), (1, H)),
        name="last",
        compiler_params=pltpu.CompilerParams(vmem_limit_bytes=8 << 20),
    )(live, one_row, parts, share_root, share_fc, turns, pre)
    return jnp.swapaxes(turns, 0, 1), pre.reshape(H)


def exchanged(copies, axis):
    return lax.all_to_all(copies, axis, split_axis=0, concat_axis=0, tiled=True)


def whole_parts(copies):
    part = jnp.sum(exchanged(copies, FIRST_SUM), axis=0)
    return sent_to_all(part, SECOND_SUM)


ROWS = 80
FIRST_ROWS = (0, 0, FLOP_GRP // 2, FLOP_GRP)


def pack_kernel(first_hand_ref, strength_ref, board_ref, weight_ref, cards_ref, out_ref):
    groups, rows, width = out_ref.shape
    hand_block, _, capacity = strength_ref.shape
    used = ITERS - 1
    hand = first_hand_ref[0, 0] + lax.broadcasted_iota(jnp.int32, (hand_block, capacity), 0)
    flop_live = (board_ref[...] == 1) & (hand < HANDS)
    keys = [jnp.where(flop_live, strength_ref[:, counter, :] + 1, 0) for counter in range(used)]
    weights = weight_ref[...]
    cards = [cards_ref[counter] for counter in range(used)]
    count = jnp.zeros((1, width), jnp.int32) + jnp.sum((weights > 0).astype(jnp.int32))
    extra = used * hand_block
    for group, first in enumerate(FIRST_ROWS):
        for counter in range(used):
            out_ref[group, hand_block * counter : hand_block * (counter + 1), :] = keys[counter][
                :, first : first + width
            ]
        out_ref[group, extra : extra + 1, :] = weights[:, first : first + width]
        for counter in range(used):
            row = extra + 1 + 2 * counter
            out_ref[group, row : row + 2, :] = cards[counter][:, first : first + width]
        blank = extra + 1 + 2 * used
        out_ref[group, blank : blank + 1, :] = count
        out_ref[group, blank + 1 :, :] = jnp.zeros((rows - blank - 1, width), jnp.int32)


def packed(first_hand, strength, board_mask, flop_weight, runout, groups):
    capacity = strength.shape[0]
    return pl.pallas_call(
        pack_kernel,
        out_shape=jax.ShapeDtypeStruct((groups, ROWS, FLOP_GRP), jnp.int32),
        in_specs=[
            pl.BlockSpec(memory_space=pltpu.SMEM),
            *([pl.BlockSpec(memory_space=pltpu.VMEM)] * 4),
        ],
        name="pack",
    )(
        first_hand.astype(jnp.int32).reshape(1, 1),
        jnp.transpose(strength, (2, 1, 0)),
        board_mask.T,
        flop_weight.reshape(1, capacity),
        jnp.transpose(runout, (1, 2, 0)),
    )


def route_kernel(group_ref, slots_ref, out_ref):
    groups, rows, width = slots_ref.shape
    pairs = out_ref.shape[0]
    count_row = (ITERS - 1) * (H // pairs + 2) + 1
    group = group_ref[0, 0]
    first = jnp.where(group == 3, FIRST_ROWS[3], jnp.where(group == 2, FIRST_ROWS[2], 0))
    row = first + lax.broadcasted_iota(jnp.int32, (1, width), 1)
    counts = [slots_ref[g, count_row : count_row + 1, :] for g in range(groups)]
    totals = [[jnp.zeros((pairs, LINE), jnp.float32) for part in range(4)] for odd in range(2)]
    pair = lax.broadcasted_iota(jnp.int32, (pairs, width), 0)
    blank = jnp.zeros((LINE - rows, width), jnp.int32)
    for g in range(groups):
        place = -2 * pairs * group + jnp.zeros((1, width), jnp.int32)
        for other in range(groups):
            place = place + jnp.minimum(counts[other], row + int(other < g))
        place = jnp.where(row < counts[g], place, -1)
        values = jnp.concatenate([slots_ref[g], blank])
        picks = [
            (place == 2 * pair + odd).astype(jnp.float32).astype(jnp.bfloat16) for odd in range(2)
        ]
        for part in range(4):
            digits = (values >> (8 * part)) & (PART - 1)
            digits = digits.astype(jnp.float32).astype(jnp.bfloat16)
            for odd in range(2):
                found = lax.dot_general(
                    picks[odd], digits, (((1,), (1,)), ((), ())), preferred_element_type=jnp.float32
                )
                totals[odd][part] = totals[odd][part] + found
    for odd in range(2):
        whole = jnp.zeros((pairs, LINE), jnp.int32)
        for part in range(4):
            whole = whole + (totals[odd][part].astype(jnp.int32) << (8 * part))
        out_ref[:, 0, LINE * odd : LINE * (odd + 1)] = whole


def route(slots, group_id, pairs):
    return pl.pallas_call(
        route_kernel,
        out_shape=jax.ShapeDtypeStruct((pairs, 1, 2 * LINE), jnp.int32),
        in_specs=[pl.BlockSpec(memory_space=pltpu.SMEM), pl.BlockSpec(memory_space=pltpu.VMEM)],
        name="route",
        compiler_params=pltpu.CompilerParams(vmem_limit_bytes=12 << 20),
    )(group_id.astype(jnp.int32).reshape(1, 1), slots)


def on_device(range_one, range_two, flop_weight, board_mask, runout, strength):
    groups = lax.axis_size(GRP)
    shards = lax.axis_size(INF)
    shard_id = lax.axis_index(INF)
    hand_block = strength.shape[2]
    first_hand = shard_id * hand_block
    low, high = (jnp.asarray(table).reshape(1, PADDED) for table in hand_cards(PADDED, HANDS))
    slots = exchanged(
        packed(first_hand, strength, board_mask, flop_weight, runout, groups), GRP
    )
    arrived = exchanged(route(slots, lax.axis_index(GRP), shards), INF)
    turn_reach, pre_reach = solve(
        arrived,
        range_one,
        range_two,
        low,
        high,
        pltpu.with_memory_space_constraint(compat_matrix(low, high), pltpu.HBM),
    )
    return turn_reach, lax.dynamic_slice(
        pre_reach, (first_hand,), (hand_block,), allow_negative_indices=False
    )


def solution(mesh):
    split = Mesh(mesh.devices.reshape(2, 2, 4, 8, 2), ("grp_0", "grp_1", "inf_0", "inf_1", "inf_2"))
    return jax.shard_map(
        on_device,
        mesh=split,
        in_specs=(P(), P(), P(GRP), P(GRP, INF), P(GRP, None, None), P(GRP, None, INF)),
        out_specs=(P(GRP_INF, None, None), P(INF)),
        check_vma=False,
    )
```

```python
import jax
import jax.numpy as jnp
import numpy as np
from jax import lax
from jax.experimental import pallas as pl
from jax.experimental.pallas import tpu as pltpu
from jax.sharding import Mesh
from jax.sharding import PartitionSpec as P

HANDS = 1326
H = 1408
ITERS = 4
FLOP_GRP = 128
GRP = ("grp_0", "grp_1")
INF = ("inf_0", "inf_1", "inf_2")
GRP_INF = ("grp_0", "grp_1", "inf_0", "inf_1", "inf_2")


EPSILON = 0.01
FOLD_VALUE = -0.1


def sent_to_all(x, axis):
    copies = jnp.broadcast_to(x, (lax.axis_size(axis), *x.shape))
    return lax.all_to_all(copies, axis, split_axis=0, concat_axis=0, tiled=True)


def hand_cards(slot_total, real_total):
    low_list = []
    high_list = []
    for first_card in range(52):
        for second_card in range(first_card + 1, 52):
            low_list.append(first_card)
            high_list.append(second_card)
    low_table = np.full(slot_total, 52, np.int32)
    high_table = np.full(slot_total, 53, np.int32)
    used_count = min(slot_total, real_total)
    low_table[:used_count] = np.array(low_list[:used_count], np.int32)
    high_table[:used_count] = np.array(high_list[:used_count], np.int32)
    return (low_table, high_table)


def action_share(first_regret, second_regret):
    return (first_regret + EPSILON) / (first_regret + second_regret + 2.0 * EPSILON)


SCALE = 1.0 / HANDS
FLOP_TOTAL = 12.0 * FLOP_GRP * 4
LINE = 128
PART = 256
BLOCK = 128
WIDE = 1408
DEEP = 128
PADDED = 1408
FIRST_SUM = ("grp_1", "inf_0", "inf_2")
SECOND_SUM = ("grp_0", "inf_1")


def compat_kernel(cards_ref, out_ref):
    low_ref = cards_ref.at[0:1]
    high_ref = cards_ref.at[1:2]

    def rows(step, carry):
        first = pl.multiple_of(step * BLOCK, BLOCK)
        low_col = jnp.broadcast_to(low_ref[:, pl.ds(first, BLOCK)], (BLOCK, BLOCK)).T
        high_col = jnp.broadcast_to(high_ref[:, pl.ds(first, BLOCK)], (BLOCK, BLOCK)).T
        for start in range(0, PADDED, BLOCK):
            low_here = low_ref[:, start : start + BLOCK]
            high_here = high_ref[:, start : start + BLOCK]
            apart = (low_col != low_here) & (low_col != high_here)
            apart = apart & (high_col != low_here) & (high_col != high_here)
            out_ref[pl.ds(first, BLOCK), start : start + BLOCK] = jnp.where(
                apart, 1.0, 0.0
            ).astype(jnp.bfloat16)
        return carry

    lax.fori_loop(0, H // BLOCK, rows, 0)


def compat_matrix(cards):
    return pl.pallas_call(
        compat_kernel,
        out_shape=jax.ShapeDtypeStruct((H, PADDED), jnp.bfloat16),
        name="compat",
        compiler_params=pltpu.CompilerParams(vmem_limit_bytes=12 << 20),
    )(cards)


def pair_sums(key_ref, counter, columns, compat_ref, lhs_ref, low_ref, sums_ref, col_ref, fetch=None):
    alive = (key_ref[counter, :, :H] >= 0).astype(jnp.float32)
    lhs_ref[...] = jnp.zeros((16, H), jnp.float32)
    for k, column in columns.items():
        lhs_ref[2 * k : 2 * k + 2, :] = column * alive
    low_ref[...] = lhs_ref[...].astype(jnp.bfloat16)

    def key_column(step, carry):
        first = pl.multiple_of(step * BLOCK, BLOCK)
        for flop in range(2):
            keys = key_ref[counter, flop : flop + 1, pl.ds(first, BLOCK)]
            col_ref[flop, pl.ds(first, BLOCK), :] = jnp.broadcast_to(keys, (BLOCK, BLOCK)).T
        return carry

    lax.fori_loop(0, H // BLOCK, key_column, 0)
    if fetch is not None:
        fetch.wait()

    def mine(step, carry):
        start = pl.multiple_of(step * WIDE, WIDE)
        weight_total = jnp.zeros((16, WIDE), jnp.float32)
        totals = [jnp.zeros((16, WIDE), jnp.float32) for flop in range(2)]
        rows = [key_ref[counter, flop : flop + 1, pl.ds(start, WIDE)] for flop in range(2)]
        for first in range(0, H, DEEP):
            depth = min(DEEP, H - first)
            lhs = low_ref[:, first : first + depth]
            most = compat_ref[first : first + depth, pl.ds(start, WIDE)]
            weight_total = weight_total + jnp.dot(lhs, most, preferred_element_type=jnp.float32)
            for flop in range(2):
                parts = []
                key_col = col_ref[flop, first : first + depth, :]
                for lane in range(0, WIDE, BLOCK):
                    gap = rows[flop][:, lane : lane + BLOCK] - key_col
                    parts.append(gap.astype(jnp.float32).astype(jnp.bfloat16))
                sign = jnp.concatenate(parts, axis=1) if len(parts) > 1 else parts[0]
                one = jnp.bfloat16(1)
                sign = jnp.minimum(jnp.maximum(sign, -one), one) * most
                totals[flop] = totals[flop] + jnp.dot(
                    lhs, sign, preferred_element_type=jnp.float32
                )
        row_flop = lax.broadcasted_iota(jnp.int32, (16, WIDE), 0) & 1
        sums_ref[0, :, pl.ds(start, WIDE)] = jnp.where(row_flop == 0, totals[0], totals[1])
        sums_ref[1, :, pl.ds(start, WIDE)] = weight_total
        return carry

    lax.fori_loop(0, PADDED // WIDE, mine, 0)
    sign_sum = {k: sums_ref[0, 2 * k : 2 * k + 2, :H] * alive for k in columns}
    weight_sum = {k: sums_ref[1, 2 * k : 2 * k + 2, :H] * alive for k in columns}
    return sign_sum, weight_sum


def two_values(sign_sum, weight_sum, share_root, share_fc):
    v_cc = 0.5 * SCALE * sign_sum[1]
    v_cbf = -0.5 * SCALE * (weight_sum[0] - weight_sum[1])
    v_cbc = 1.5 * SCALE * (sign_sum[0] - sign_sum[1])
    v_bf = 0.5 * SCALE * weight_sum[2]
    v_bc = 1.5 * SCALE * (sign_sum[0] - sign_sum[2])
    u_fc = share_fc * v_cbf + (1.0 - share_fc) * v_cbc
    v_check = v_cc + u_fc
    v_bet = v_bf + v_bc
    u_root = share_root * v_check + (1.0 - share_root) * v_bet
    return v_cbf, v_cbc, u_fc, v_check, v_bet, u_root


def one_values(sign_sum, weight_sum, share_ac, share_fb):
    w_cc = 0.5 * SCALE * sign_sum[4]
    w_cbf = 0.5 * SCALE * weight_sum[5]
    w_cbc = 1.5 * SCALE * (sign_sum[4] - sign_sum[5])
    w_bf = -0.5 * SCALE * (weight_sum[3] - weight_sum[4])
    w_bc = 1.5 * SCALE * (sign_sum[3] - sign_sum[4])
    x_bet = w_cbf + w_cbc
    u_ac = share_ac * w_cc + (1.0 - share_ac) * x_bet
    u_fb = share_fb * w_bf + (1.0 - share_fb) * w_bc
    return w_cc, x_bet, u_ac, w_bf, w_bc, u_fb


def two_regrets(regrets, values):
    root_check, root_bet, fc_fold, fc_call = regrets
    v_cbf, v_cbc, u_fc, v_check, v_bet, u_root = values
    return (
        jnp.maximum(root_check + v_check - u_root, 0.0),
        jnp.maximum(root_bet + v_bet - u_root, 0.0),
        jnp.maximum(fc_fold + v_cbf - u_fc, 0.0),
        jnp.maximum(fc_call + v_cbc - u_fc, 0.0),
    )


def one_regrets(regrets, values):
    ac_check, ac_bet, fb_fold, fb_call = regrets
    w_cc, x_bet, u_ac, w_bf, w_bc, u_fb = values
    return (
        jnp.maximum(ac_check + w_cc - u_ac, 0.0),
        jnp.maximum(ac_bet + x_bet - u_ac, 0.0),
        jnp.maximum(fb_fold + w_bf - u_fb, 0.0),
        jnp.maximum(fb_call + w_bc - u_fb, 0.0),
    )


def pre_step(pre_cont, pre_fold, cont_value):
    share_pre = action_share(pre_cont, pre_fold)
    u_pre = share_pre * cont_value + (1.0 - share_pre) * FOLD_VALUE
    return (
        jnp.maximum(pre_cont + cont_value - u_pre, 0.0),
        jnp.maximum(pre_fold + FOLD_VALUE - u_pre, 0.0),
    )


def one_columns(one_all, share_root, share_fc):
    one_check = one_all * share_root
    return {3: one_all, 4: one_check, 5: one_check * share_fc}


def two_columns(two_all, share_ac, share_fb):
    return {0: two_all, 1: two_all * share_ac, 2: two_all * share_fb}


def one_rows(columns):
    return columns[4], columns[3] - columns[4], columns[4] - columns[5]


def two_rows(columns):
    return columns[1], columns[0] - columns[2], columns[0] - columns[1]


def flop_value(share, u_root):
    part = share * u_root
    return part[0:1, :] + part[1:2, :]


def add_parts(parts_ref):
    total = parts_ref[0]
    for k in range(1, parts_ref.shape[0]):
        total = total + parts_ref[k]
    return total


def spread(copies_ref, value, part=0, parts=1):
    count = copies_ref.shape[0] // parts
    for k in range(count * part, count * (part + 1)):
        copies_ref[k] = value


def read_flops(arrived_ref, cards_ref, key_ref, live_ref, share_ref):
    used = key_ref.shape[0]
    shards = arrived_ref.shape[0]
    hand_block = H // shards
    for shard in range(shards):
        line = arrived_ref[shard] - 1
        for flop in range(2):
            for counter in range(used):
                first = LINE * flop + hand_block * counter
                key_ref[
                    counter, flop : flop + 1, hand_block * shard : hand_block * (shard + 1)
                ] = line[:, first : first + hand_block]
    live_ref[...] = (key_ref[0, :, :H] >= 0).astype(jnp.float32)
    low = cards_ref[0:1, :]
    high = cards_ref[1:2, :]
    for flop in range(2):
        first = LINE * flop + hand_block * used
        extra = arrived_ref[0, :, first : first + 1 + 2 * used]
        share_ref[flop : flop + 1, :] = extra[:, 0:1].astype(jnp.float32) / FLOP_TOTAL
        for counter in range(used):
            turn = extra[:, 1 + 2 * counter : 2 + 2 * counter]
            river = extra[:, 2 + 2 * counter : 3 + 2 * counter]
            blocked = (low == turn) | (low == river) | (high == turn) | (high == river)
            blocked = blocked | (lax.broadcasted_iota(jnp.int32, (1, PADDED), 1) >= H)
            row = key_ref[counter, flop : flop + 1, :]
            key_ref[counter, flop : flop + 1, :] = jnp.where(blocked, -1, row)


def first_kernel(
    arrived_ref, cards_ref, one_ref, two_ref, compat_hbm_ref,
    key_ref, live_ref, share_ref, cont_ref,
    root_check_ref, root_bet_ref, fc_fold_ref, fc_call_ref,
    ac_check_ref, ac_bet_ref, fb_fold_ref, fb_call_ref, share_root_ref, share_fc_ref, turn_ref,
    lhs_ref, low_part_ref, sums_ref, col_ref, compat_ref, compat_sem,
):
    fetch = pltpu.make_async_copy(compat_hbm_ref, compat_ref, compat_sem)
    fetch.start()
    scratch = (compat_ref, lhs_ref, low_part_ref, sums_ref, col_ref)
    read_flops(arrived_ref, cards_ref, key_ref, live_ref, share_ref)
    live = live_ref[...]
    share = share_ref[...]
    zero = jnp.zeros((2, H), jnp.float32)
    zero_row = jnp.zeros((1, H), jnp.float32)
    two_all = two_ref[...] * live
    start = action_share(zero, zero)
    one_all = one_ref[...] * action_share(zero_row, zero_row) * live
    one_cols = one_columns(one_all, start, start)
    two_cols = two_columns(two_all, start, start)
    sign_sum, weight_sum = pair_sums(key_ref, 0, {**two_cols, **one_cols}, *scratch, fetch)
    values = two_values(sign_sum, weight_sum, start, start)
    spread(cont_ref, flop_value(share, values[5]), 0, 2)
    regrets = two_regrets((zero, zero, zero, zero), values)
    others = one_regrets((zero, zero, zero, zero), one_values(sign_sum, weight_sum, start, start))
    turns = [*one_rows(one_cols), *two_rows(two_cols)]

    share_root = action_share(regrets[0], regrets[1])
    share_fc = action_share(regrets[2], regrets[3])
    two_cols = two_columns(
        two_all, action_share(others[0], others[1]), action_share(others[2], others[3])
    )
    sign_sum, weight_sum = pair_sums(key_ref, 1, two_cols, *scratch)
    values = two_values(sign_sum, weight_sum, share_root, share_fc)
    spread(cont_ref, flop_value(share, values[5]), 1, 2)
    regrets = two_regrets(regrets, values)
    for k, row in enumerate(two_rows(two_cols)):
        turns[3 + k] = turns[3 + k] + 2.0 * row
    root_check_ref[...], root_bet_ref[...], fc_fold_ref[...], fc_call_ref[...] = regrets
    ac_check_ref[...], ac_bet_ref[...], fb_fold_ref[...], fb_call_ref[...] = others
    share_root_ref[...] = share_root
    share_fc_ref[...] = share_fc
    for k in range(6):
        turn_ref[k] = turns[k]


def second_kernel(
    key_ref, live_ref, one_ref, two_ref, share_ref, compat_hbm_ref,
    core_ref, own_sum_ref, other_sum_ref,
    root_check_ref, root_bet_ref, fc_fold_ref, fc_call_ref,
    ac_check_ref, ac_bet_ref, fb_fold_ref, fb_call_ref, share_root_ref, share_fc_ref, turn_ref,
    cont_ref, out_root_ref, out_fc_ref, out_turn_ref, out_pre_ref,
    lhs_ref, low_ref, sums_ref, col_ref, compat_ref, compat_sem,
):
    fetch = pltpu.make_async_copy(compat_hbm_ref, compat_ref, compat_sem)
    fetch.start()
    scratch = (compat_ref, lhs_ref, low_ref, sums_ref, col_ref)
    first_core = core_ref[0, 0] == 0
    own_sum = own_sum_ref[...]
    other_sum = other_sum_ref[...]
    live = live_ref[...]
    zero_row = jnp.zeros((1, H), jnp.float32)
    two_all = two_ref[...] * live
    one_range = one_ref[...]
    turns = [turn_ref[k] for k in range(6)]
    pre_sum = one_range * action_share(zero_row, zero_row)
    pre_cont, pre_fold = pre_step(zero_row, zero_row, jnp.where(first_core, own_sum, other_sum))
    one_now = one_range * action_share(pre_cont, pre_fold)
    pre_sum = pre_sum + 2.0 * one_now
    one_cols = one_columns(one_now * live, share_root_ref[...], share_fc_ref[...])
    for k, row in enumerate(one_rows(one_cols)):
        turns[k] = turns[k] + 2.0 * row
    others = (ac_check_ref[...], ac_bet_ref[...], fb_fold_ref[...], fb_call_ref[...])
    share_ac = action_share(others[0], others[1])
    share_fb = action_share(others[2], others[3])
    sign_sum, weight_sum = pair_sums(key_ref, 1, one_cols, *scratch, fetch)
    others = one_regrets(others, one_values(sign_sum, weight_sum, share_ac, share_fb))

    pre_cont, pre_fold = pre_step(pre_cont, pre_fold, jnp.where(first_core, other_sum, own_sum))
    one_now = one_range * action_share(pre_cont, pre_fold)
    pre_sum = pre_sum + 3.0 * one_now
    regrets = (root_check_ref[...], root_bet_ref[...], fc_fold_ref[...], fc_call_ref[...])
    share_root = action_share(regrets[0], regrets[1])
    share_fc = action_share(regrets[2], regrets[3])
    share_ac = action_share(others[0], others[1])
    share_fb = action_share(others[2], others[3])
    one_cols = one_columns(one_now * live, share_root, share_fc)
    two_cols = two_columns(two_all, share_ac, share_fb)
    for k, row in enumerate((*one_rows(one_cols), *two_rows(two_cols))):
        turns[k] = turns[k] + 3.0 * row
    sign_sum, weight_sum = pair_sums(key_ref, 2, {**two_cols, **one_cols}, *scratch)
    values = two_values(sign_sum, weight_sum, share_root, share_fc)
    spread(cont_ref, flop_value(share_ref[...], values[5]))
    regrets = two_regrets(regrets, values)
    others = one_regrets(others, one_values(sign_sum, weight_sum, share_ac, share_fb))
    two_cols = two_columns(
        two_all, action_share(others[0], others[1]), action_share(others[2], others[3])
    )
    for k, row in enumerate(two_rows(two_cols)):
        turns[3 + k] = turns[3 + k] + 4.0 * row
    out_root_ref[...] = action_share(regrets[0], regrets[1])
    out_fc_ref[...] = action_share(regrets[2], regrets[3])
    for k in range(6):
        out_turn_ref[k] = turns[k]
    out_pre_ref[0:1, :] = pre_cont
    out_pre_ref[1:2, :] = pre_fold
    out_pre_ref[2:3, :] = pre_sum


def pair_scratch():
    return [
        pltpu.VMEM((16, H), jnp.float32),
        pltpu.VMEM((16, H), jnp.bfloat16),
        pltpu.VMEM((2, 16, PADDED), jnp.float32),
        pltpu.VMEM((2, H, BLOCK), jnp.int32),
        pltpu.VMEM((H, PADDED), jnp.bfloat16),
        pltpu.SemaphoreType.DMA,
    ]


def in_vmem(count):
    return [pl.BlockSpec(memory_space=pltpu.VMEM)] * count


def in_hbm():
    return pl.BlockSpec(memory_space=pltpu.HBM)


def rows_of(*shapes):
    return [jax.ShapeDtypeStruct(shape, jnp.float32) for shape in shapes]


def last_kernel(
    live_ref, one_ref, sums_in_ref, share_root_ref, share_fc_ref, turn_ref, pre_ref,
    out_ref, pre_out_ref,
):
    total_weight = ITERS * (ITERS + 1) / 2.0
    pre_cont, pre_fold = pre_step(pre_ref[0:1, :], pre_ref[1:2, :], add_parts(sums_in_ref))
    one_now = one_ref[...] * action_share(pre_cont, pre_fold)
    columns = one_columns(one_now * live_ref[...], share_root_ref[...], share_fc_ref[...])
    for k, row in enumerate(one_rows(columns)):
        out_ref[k] = (turn_ref[k] + 4.0 * row) / total_weight
    for k in range(3, 6):
        out_ref[k] = turn_ref[k] / total_weight
    pre_out_ref[...] = (pre_ref[2:3, :] + 4.0 * one_now) / total_weight


def solve(arrived, range_one, range_two, cards, compat):
    one_row = range_one.reshape(1, H)
    two_row = range_two.reshape(1, H)
    pair = (2, H)
    first_count = lax.axis_size(FIRST_SUM)
    key_now, live, share, cont, *state = pl.pallas_call(
        first_kernel,
        out_shape=[
            jax.ShapeDtypeStruct((ITERS - 1, 2, PADDED), jnp.int32),
            *rows_of(pair, (2, 1), (first_count, 1, H), *([pair] * 10), (6, 2, H)),
        ],
        in_specs=[*in_vmem(4), in_hbm()],
        scratch_shapes=pair_scratch(),
        name="first",
        compiler_params=pltpu.CompilerParams(vmem_limit_bytes=20 << 20),
    )(arrived, cards, one_row, two_row, compat)
    own_sum = jnp.sum(whole_parts(cont), axis=0)
    other_sum = lax.ppermute(own_sum, "grp_1", [(0, 1), (1, 0)])
    core = lax.axis_index("grp_1").astype(jnp.int32).reshape(1, 1)
    cont, share_root, share_fc, turns, pre = pl.pallas_call(
        second_kernel,
        out_shape=rows_of((first_count, 1, H), pair, pair, (6, 2, H), (3, H)),
        in_specs=[
            *in_vmem(5), in_hbm(), pl.BlockSpec(memory_space=pltpu.SMEM), *in_vmem(13)
        ],
        scratch_shapes=pair_scratch(),
        name="second",
        compiler_params=pltpu.CompilerParams(vmem_limit_bytes=20 << 20),
    )(key_now, live, one_row, two_row, share, compat, core, own_sum, other_sum, *state)
    parts = whole_parts(cont)
    turns, pre = pl.pallas_call(
        last_kernel,
        out_shape=rows_of((6, 2, H), (1, H)),
        name="last",
        compiler_params=pltpu.CompilerParams(vmem_limit_bytes=8 << 20),
    )(live, one_row, parts, share_root, share_fc, turns, pre)
    return jnp.swapaxes(turns, 0, 1), pre.reshape(H)


def exchanged(copies, axis):
    return lax.all_to_all(copies, axis, split_axis=0, concat_axis=0, tiled=True)


def whole_parts(copies):
    part = jnp.sum(exchanged(copies, FIRST_SUM), axis=0)
    return sent_to_all(part, SECOND_SUM)


ROWS = 80
FIRST_ROWS = (0, 0, FLOP_GRP // 2, FLOP_GRP)


def pack_kernel(first_hand_ref, strength_ref, board_ref, weight_ref, cards_ref, out_ref):
    groups, rows, width = out_ref.shape
    hand_block, _, capacity = strength_ref.shape
    used = ITERS - 1
    hand = first_hand_ref[0, 0] + lax.broadcasted_iota(jnp.int32, (hand_block, capacity), 0)
    flop_live = (board_ref[...] == 1) & (hand < HANDS)
    keys = [jnp.where(flop_live, strength_ref[:, counter, :] + 1, 0) for counter in range(used)]
    weights = weight_ref[...]
    cards = [cards_ref[counter] for counter in range(used)]
    count = jnp.zeros((1, width), jnp.int32) + jnp.sum((weights > 0).astype(jnp.int32))
    extra = used * hand_block
    for group, first in enumerate(FIRST_ROWS):
        for counter in range(used):
            out_ref[group, hand_block * counter : hand_block * (counter + 1), :] = keys[counter][
                :, first : first + width
            ]
        out_ref[group, extra : extra + 1, :] = weights[:, first : first + width]
        for counter in range(used):
            row = extra + 1 + 2 * counter
            out_ref[group, row : row + 2, :] = cards[counter][:, first : first + width]
        blank = extra + 1 + 2 * used
        out_ref[group, blank : blank + 1, :] = count
        out_ref[group, blank + 1 :, :] = jnp.zeros((rows - blank - 1, width), jnp.int32)


def packed(first_hand, strength, board_mask, flop_weight, runout, groups):
    capacity = strength.shape[0]
    return pl.pallas_call(
        pack_kernel,
        out_shape=jax.ShapeDtypeStruct((groups, ROWS, FLOP_GRP), jnp.int32),
        in_specs=[
            pl.BlockSpec(memory_space=pltpu.SMEM),
            *([pl.BlockSpec(memory_space=pltpu.VMEM)] * 4),
        ],
        name="pack",
    )(
        first_hand.astype(jnp.int32).reshape(1, 1),
        jnp.transpose(strength, (2, 1, 0)),
        board_mask.T,
        flop_weight.reshape(1, capacity),
        jnp.transpose(runout, (1, 2, 0)),
    )


def route_kernel(group_ref, slots_ref, out_ref):
    groups, rows, width = slots_ref.shape
    pairs = out_ref.shape[0]
    count_row = (ITERS - 1) * (H // pairs + 2) + 1
    group = group_ref[0, 0]
    first = jnp.where(group == 3, FIRST_ROWS[3], jnp.where(group == 2, FIRST_ROWS[2], 0))
    row = first + lax.broadcasted_iota(jnp.int32, (1, width), 1)
    counts = [slots_ref[g, count_row : count_row + 1, :] for g in range(groups)]
    totals = [[jnp.zeros((pairs, LINE), jnp.float32) for part in range(4)] for odd in range(2)]
    pair = lax.broadcasted_iota(jnp.int32, (pairs, width), 0)
    blank = jnp.zeros((LINE - rows, width), jnp.int32)
    for g in range(groups):
        place = -2 * pairs * group + jnp.zeros((1, width), jnp.int32)
        for other in range(groups):
            place = place + jnp.minimum(counts[other], row + int(other < g))
        place = jnp.where(row < counts[g], place, -1)
        values = jnp.concatenate([slots_ref[g], blank])
        picks = [
            (place == 2 * pair + odd).astype(jnp.float32).astype(jnp.bfloat16) for odd in range(2)
        ]
        for part in range(4):
            digits = (values >> (8 * part)) & (PART - 1)
            digits = digits.astype(jnp.float32).astype(jnp.bfloat16)
            for odd in range(2):
                found = lax.dot_general(
                    picks[odd], digits, (((1,), (1,)), ((), ())), preferred_element_type=jnp.float32
                )
                totals[odd][part] = totals[odd][part] + found
    for odd in range(2):
        whole = jnp.zeros((pairs, LINE), jnp.int32)
        for part in range(4):
            whole = whole + (totals[odd][part].astype(jnp.int32) << (8 * part))
        out_ref[:, 0, LINE * odd : LINE * (odd + 1)] = whole


def route(slots, group_id, pairs):
    return pl.pallas_call(
        route_kernel,
        out_shape=jax.ShapeDtypeStruct((pairs, 1, 2 * LINE), jnp.int32),
        in_specs=[pl.BlockSpec(memory_space=pltpu.SMEM), pl.BlockSpec(memory_space=pltpu.VMEM)],
        name="route",
        compiler_params=pltpu.CompilerParams(vmem_limit_bytes=12 << 20),
    )(group_id.astype(jnp.int32).reshape(1, 1), slots)


def on_device(range_one, range_two, flop_weight, board_mask, runout, strength):
    groups = lax.axis_size(GRP)
    shards = lax.axis_size(INF)
    shard_id = lax.axis_index(INF)
    hand_block = strength.shape[2]
    first_hand = shard_id * hand_block
    cards = jnp.asarray(np.stack(hand_cards(PADDED, HANDS)))
    slots = exchanged(
        packed(first_hand, strength, board_mask, flop_weight, runout, groups), GRP
    )
    slots, compat = lax.optimization_barrier((slots, compat_matrix(cards)))
    routed = route(slots, lax.axis_index(GRP), shards)
    routed, compat = lax.optimization_barrier((routed, compat))
    arrived = exchanged(routed, INF)
    compat = pltpu.with_memory_space_constraint(compat, pltpu.HBM)
    turn_reach, pre_reach = solve(arrived, range_one, range_two, cards, compat)
    return turn_reach, lax.dynamic_slice(
        pre_reach, (first_hand,), (hand_block,), allow_negative_indices=False
    )


def solution(mesh):
    split = Mesh(mesh.devices.reshape(2, 2, 4, 8, 2), ("grp_0", "grp_1", "inf_0", "inf_1", "inf_2"))
    return jax.shard_map(
        on_device,
        mesh=split,
        in_specs=(P(), P(), P(GRP), P(GRP, INF), P(GRP, None, None), P(GRP, None, INF)),
        out_specs=(P(GRP_INF, None, None), P(INF)),
        check_vma=False,
    )
```

```python
import jax
import jax.numpy as jnp
import numpy as np
from jax import lax
from jax.experimental import pallas as pl
from jax.experimental.pallas import tpu as pltpu
from jax.sharding import Mesh
from jax.sharding import PartitionSpec as P

HANDS = 1326
H = 1408
ITERS = 4
FLOP_GRP = 128
GRP = ("grp_0", "grp_1")
INF = ("inf_0", "inf_1", "inf_2")
GRP_INF = ("grp_0", "grp_1", "inf_0", "inf_1", "inf_2")


EPSILON = 0.01
FOLD_VALUE = -0.1


def sent_to_all(x, axis):
    copies = jnp.broadcast_to(x, (lax.axis_size(axis), *x.shape))
    return lax.all_to_all(copies, axis, split_axis=0, concat_axis=0, tiled=True)


def hand_cards(slot_total, real_total):
    low_list = []
    high_list = []
    for first_card in range(52):
        for second_card in range(first_card + 1, 52):
            low_list.append(first_card)
            high_list.append(second_card)
    low_table = np.full(slot_total, 52, np.int32)
    high_table = np.full(slot_total, 53, np.int32)
    used_count = min(slot_total, real_total)
    low_table[:used_count] = np.array(low_list[:used_count], np.int32)
    high_table[:used_count] = np.array(high_list[:used_count], np.int32)
    return (low_table, high_table)


def action_share(first_regret, second_regret):
    return (first_regret + EPSILON) / (first_regret + second_regret + 2.0 * EPSILON)


SCALE = 1.0 / HANDS
FLOP_TOTAL = 12.0 * FLOP_GRP * 4
LINE = 128
PART = 256
BLOCK = 128
WIDE = 1408
DEEP = 128
PADDED = 1408
FIRST_SUM = ("grp_1", "inf_0", "inf_2")
SECOND_SUM = ("grp_0", "inf_1")


def compat_kernel(cards_ref, out_ref, rows_ref, sems):
    low_ref = cards_ref.at[0:1]
    high_ref = cards_ref.at[1:2]

    def sent(step):
        first = pl.multiple_of(step * BLOCK, BLOCK)
        return pltpu.make_async_copy(
            rows_ref.at[step], out_ref.at[pl.ds(first, BLOCK)], sems.at[step]
        )

    def rows(step, carry):
        first = pl.multiple_of(step * BLOCK, BLOCK)
        low_col = jnp.broadcast_to(low_ref[:, pl.ds(first, BLOCK)], (BLOCK, BLOCK)).T
        high_col = jnp.broadcast_to(high_ref[:, pl.ds(first, BLOCK)], (BLOCK, BLOCK)).T
        for start in range(0, PADDED, BLOCK):
            low_here = low_ref[:, start : start + BLOCK]
            high_here = high_ref[:, start : start + BLOCK]
            apart = (low_col != low_here) & (low_col != high_here)
            apart = apart & (high_col != low_here) & (high_col != high_here)
            rows_ref[step, :, start : start + BLOCK] = jnp.where(apart, 1.0, 0.0).astype(
                jnp.bfloat16
            )
        sent(step).start()
        return carry

    lax.fori_loop(0, H // BLOCK, rows, 0)
    for step in range(H // BLOCK):
        sent(step).wait()


def compat_matrix(cards):
    return pl.pallas_call(
        compat_kernel,
        out_shape=pltpu.HBM((H, PADDED), jnp.bfloat16),
        out_specs=pl.BlockSpec(memory_space=pltpu.HBM),
        scratch_shapes=[
            pltpu.VMEM((H // BLOCK, BLOCK, PADDED), jnp.bfloat16),
            pltpu.SemaphoreType.DMA((H // BLOCK,)),
        ],
        name="compat",
        compiler_params=pltpu.CompilerParams(vmem_limit_bytes=12 << 20),
    )(cards)


def pair_sums(key_ref, counter, columns, compat_ref, lhs_ref, low_ref, sums_ref, col_ref, fetch=None):
    alive = (key_ref[counter, :, :H] >= 0).astype(jnp.float32)
    lhs_ref[...] = jnp.zeros((16, H), jnp.float32)
    for k, column in columns.items():
        lhs_ref[2 * k : 2 * k + 2, :] = column * alive
    low_ref[...] = lhs_ref[...].astype(jnp.bfloat16)

    def key_column(step, carry):
        first = pl.multiple_of(step * BLOCK, BLOCK)
        for flop in range(2):
            keys = key_ref[counter, flop : flop + 1, pl.ds(first, BLOCK)]
            col_ref[flop, pl.ds(first, BLOCK), :] = jnp.broadcast_to(keys, (BLOCK, BLOCK)).T
        return carry

    lax.fori_loop(0, H // BLOCK, key_column, 0)
    if fetch is not None:
        fetch.wait()

    def mine(step, carry):
        start = pl.multiple_of(step * WIDE, WIDE)
        weight_total = jnp.zeros((16, WIDE), jnp.float32)
        totals = [jnp.zeros((16, WIDE), jnp.float32) for flop in range(2)]
        rows = [key_ref[counter, flop : flop + 1, pl.ds(start, WIDE)] for flop in range(2)]
        for first in range(0, H, DEEP):
            depth = min(DEEP, H - first)
            lhs = low_ref[:, first : first + depth]
            most = compat_ref[first : first + depth, pl.ds(start, WIDE)]
            weight_total = weight_total + jnp.dot(lhs, most, preferred_element_type=jnp.float32)
            for flop in range(2):
                parts = []
                key_col = col_ref[flop, first : first + depth, :]
                for lane in range(0, WIDE, BLOCK):
                    gap = rows[flop][:, lane : lane + BLOCK] - key_col
                    parts.append(gap.astype(jnp.float32).astype(jnp.bfloat16))
                sign = jnp.concatenate(parts, axis=1) if len(parts) > 1 else parts[0]
                one = jnp.bfloat16(1)
                sign = jnp.minimum(jnp.maximum(sign, -one), one) * most
                totals[flop] = totals[flop] + jnp.dot(
                    lhs, sign, preferred_element_type=jnp.float32
                )
        row_flop = lax.broadcasted_iota(jnp.int32, (16, WIDE), 0) & 1
        sums_ref[0, :, pl.ds(start, WIDE)] = jnp.where(row_flop == 0, totals[0], totals[1])
        sums_ref[1, :, pl.ds(start, WIDE)] = weight_total
        return carry

    lax.fori_loop(0, PADDED // WIDE, mine, 0)
    sign_sum = {k: sums_ref[0, 2 * k : 2 * k + 2, :H] * alive for k in columns}
    weight_sum = {k: sums_ref[1, 2 * k : 2 * k + 2, :H] * alive for k in columns}
    return sign_sum, weight_sum


def two_values(sign_sum, weight_sum, share_root, share_fc):
    v_cc = 0.5 * SCALE * sign_sum[1]
    v_cbf = -0.5 * SCALE * (weight_sum[0] - weight_sum[1])
    v_cbc = 1.5 * SCALE * (sign_sum[0] - sign_sum[1])
    v_bf = 0.5 * SCALE * weight_sum[2]
    v_bc = 1.5 * SCALE * (sign_sum[0] - sign_sum[2])
    u_fc = share_fc * v_cbf + (1.0 - share_fc) * v_cbc
    v_check = v_cc + u_fc
    v_bet = v_bf + v_bc
    u_root = share_root * v_check + (1.0 - share_root) * v_bet
    return v_cbf, v_cbc, u_fc, v_check, v_bet, u_root


def one_values(sign_sum, weight_sum, share_ac, share_fb):
    w_cc = 0.5 * SCALE * sign_sum[4]
    w_cbf = 0.5 * SCALE * weight_sum[5]
    w_cbc = 1.5 * SCALE * (sign_sum[4] - sign_sum[5])
    w_bf = -0.5 * SCALE * (weight_sum[3] - weight_sum[4])
    w_bc = 1.5 * SCALE * (sign_sum[3] - sign_sum[4])
    x_bet = w_cbf + w_cbc
    u_ac = share_ac * w_cc + (1.0 - share_ac) * x_bet
    u_fb = share_fb * w_bf + (1.0 - share_fb) * w_bc
    return w_cc, x_bet, u_ac, w_bf, w_bc, u_fb


def two_regrets(regrets, values):
    root_check, root_bet, fc_fold, fc_call = regrets
    v_cbf, v_cbc, u_fc, v_check, v_bet, u_root = values
    return (
        jnp.maximum(root_check + v_check - u_root, 0.0),
        jnp.maximum(root_bet + v_bet - u_root, 0.0),
        jnp.maximum(fc_fold + v_cbf - u_fc, 0.0),
        jnp.maximum(fc_call + v_cbc - u_fc, 0.0),
    )


def one_regrets(regrets, values):
    ac_check, ac_bet, fb_fold, fb_call = regrets
    w_cc, x_bet, u_ac, w_bf, w_bc, u_fb = values
    return (
        jnp.maximum(ac_check + w_cc - u_ac, 0.0),
        jnp.maximum(ac_bet + x_bet - u_ac, 0.0),
        jnp.maximum(fb_fold + w_bf - u_fb, 0.0),
        jnp.maximum(fb_call + w_bc - u_fb, 0.0),
    )


def pre_step(pre_cont, pre_fold, cont_value):
    share_pre = action_share(pre_cont, pre_fold)
    u_pre = share_pre * cont_value + (1.0 - share_pre) * FOLD_VALUE
    return (
        jnp.maximum(pre_cont + cont_value - u_pre, 0.0),
        jnp.maximum(pre_fold + FOLD_VALUE - u_pre, 0.0),
    )


def one_columns(one_all, share_root, share_fc):
    one_check = one_all * share_root
    return {3: one_all, 4: one_check, 5: one_check * share_fc}


def two_columns(two_all, share_ac, share_fb):
    return {0: two_all, 1: two_all * share_ac, 2: two_all * share_fb}


def one_rows(columns):
    return columns[4], columns[3] - columns[4], columns[4] - columns[5]


def two_rows(columns):
    return columns[1], columns[0] - columns[2], columns[0] - columns[1]


def flop_value(share, u_root):
    part = share * u_root
    return part[0:1, :] + part[1:2, :]


def add_parts(parts_ref):
    total = parts_ref[0]
    for k in range(1, parts_ref.shape[0]):
        total = total + parts_ref[k]
    return total


def spread(copies_ref, value, part=0, parts=1):
    count = copies_ref.shape[0] // parts
    for k in range(count * part, count * (part + 1)):
        copies_ref[k] = value


def read_flops(arrived_ref, cards_ref, key_ref, live_ref, share_ref):
    used = key_ref.shape[0]
    shards = arrived_ref.shape[0]
    hand_block = H // shards
    for shard in range(shards):
        line = arrived_ref[shard] - 1
        for flop in range(2):
            for counter in range(used):
                first = LINE * flop + hand_block * counter
                key_ref[
                    counter, flop : flop + 1, hand_block * shard : hand_block * (shard + 1)
                ] = line[:, first : first + hand_block]
    live_ref[...] = (key_ref[0, :, :H] >= 0).astype(jnp.float32)
    low = cards_ref[0:1, :]
    high = cards_ref[1:2, :]
    for flop in range(2):
        first = LINE * flop + hand_block * used
        extra = arrived_ref[0, :, first : first + 1 + 2 * used]
        share_ref[flop : flop + 1, :] = extra[:, 0:1].astype(jnp.float32) / FLOP_TOTAL
        for counter in range(used):
            turn = extra[:, 1 + 2 * counter : 2 + 2 * counter]
            river = extra[:, 2 + 2 * counter : 3 + 2 * counter]
            blocked = (low == turn) | (low == river) | (high == turn) | (high == river)
            blocked = blocked | (lax.broadcasted_iota(jnp.int32, (1, PADDED), 1) >= H)
            row = key_ref[counter, flop : flop + 1, :]
            key_ref[counter, flop : flop + 1, :] = jnp.where(blocked, -1, row)


def first_kernel(
    arrived_ref, cards_ref, one_ref, two_ref, compat_hbm_ref,
    key_ref, live_ref, share_ref, cont_ref,
    root_check_ref, root_bet_ref, fc_fold_ref, fc_call_ref,
    ac_check_ref, ac_bet_ref, fb_fold_ref, fb_call_ref, share_root_ref, share_fc_ref, turn_ref,
    lhs_ref, low_part_ref, sums_ref, col_ref, compat_ref, compat_sem,
):
    fetch = pltpu.make_async_copy(compat_hbm_ref, compat_ref, compat_sem)
    fetch.start()
    scratch = (compat_ref, lhs_ref, low_part_ref, sums_ref, col_ref)
    read_flops(arrived_ref, cards_ref, key_ref, live_ref, share_ref)
    live = live_ref[...]
    share = share_ref[...]
    zero = jnp.zeros((2, H), jnp.float32)
    zero_row = jnp.zeros((1, H), jnp.float32)
    two_all = two_ref[...] * live
    start = action_share(zero, zero)
    one_all = one_ref[...] * action_share(zero_row, zero_row) * live
    one_cols = one_columns(one_all, start, start)
    two_cols = two_columns(two_all, start, start)
    sign_sum, weight_sum = pair_sums(key_ref, 0, {**two_cols, **one_cols}, *scratch, fetch)
    values = two_values(sign_sum, weight_sum, start, start)
    spread(cont_ref, flop_value(share, values[5]), 0, 2)
    regrets = two_regrets((zero, zero, zero, zero), values)
    others = one_regrets((zero, zero, zero, zero), one_values(sign_sum, weight_sum, start, start))
    turns = [*one_rows(one_cols), *two_rows(two_cols)]

    share_root = action_share(regrets[0], regrets[1])
    share_fc = action_share(regrets[2], regrets[3])
    two_cols = two_columns(
        two_all, action_share(others[0], others[1]), action_share(others[2], others[3])
    )
    sign_sum, weight_sum = pair_sums(key_ref, 1, two_cols, *scratch)
    values = two_values(sign_sum, weight_sum, share_root, share_fc)
    spread(cont_ref, flop_value(share, values[5]), 1, 2)
    regrets = two_regrets(regrets, values)
    for k, row in enumerate(two_rows(two_cols)):
        turns[3 + k] = turns[3 + k] + 2.0 * row
    root_check_ref[...], root_bet_ref[...], fc_fold_ref[...], fc_call_ref[...] = regrets
    ac_check_ref[...], ac_bet_ref[...], fb_fold_ref[...], fb_call_ref[...] = others
    share_root_ref[...] = share_root
    share_fc_ref[...] = share_fc
    for k in range(6):
        turn_ref[k] = turns[k]


def second_kernel(
    key_ref, live_ref, one_ref, two_ref, share_ref, compat_hbm_ref,
    core_ref, own_sum_ref, other_sum_ref,
    root_check_ref, root_bet_ref, fc_fold_ref, fc_call_ref,
    ac_check_ref, ac_bet_ref, fb_fold_ref, fb_call_ref, share_root_ref, share_fc_ref, turn_ref,
    cont_ref, out_root_ref, out_fc_ref, out_turn_ref, out_pre_ref,
    lhs_ref, low_ref, sums_ref, col_ref, compat_ref, compat_sem,
):
    fetch = pltpu.make_async_copy(compat_hbm_ref, compat_ref, compat_sem)
    fetch.start()
    scratch = (compat_ref, lhs_ref, low_ref, sums_ref, col_ref)
    first_core = core_ref[0, 0] == 0
    own_sum = own_sum_ref[...]
    other_sum = other_sum_ref[...]
    live = live_ref[...]
    zero_row = jnp.zeros((1, H), jnp.float32)
    two_all = two_ref[...] * live
    one_range = one_ref[...]
    turns = [turn_ref[k] for k in range(6)]
    pre_sum = one_range * action_share(zero_row, zero_row)
    pre_cont, pre_fold = pre_step(zero_row, zero_row, jnp.where(first_core, own_sum, other_sum))
    one_now = one_range * action_share(pre_cont, pre_fold)
    pre_sum = pre_sum + 2.0 * one_now
    one_cols = one_columns(one_now * live, share_root_ref[...], share_fc_ref[...])
    for k, row in enumerate(one_rows(one_cols)):
        turns[k] = turns[k] + 2.0 * row
    others = (ac_check_ref[...], ac_bet_ref[...], fb_fold_ref[...], fb_call_ref[...])
    share_ac = action_share(others[0], others[1])
    share_fb = action_share(others[2], others[3])
    sign_sum, weight_sum = pair_sums(key_ref, 1, one_cols, *scratch, fetch)
    others = one_regrets(others, one_values(sign_sum, weight_sum, share_ac, share_fb))

    pre_cont, pre_fold = pre_step(pre_cont, pre_fold, jnp.where(first_core, other_sum, own_sum))
    one_now = one_range * action_share(pre_cont, pre_fold)
    pre_sum = pre_sum + 3.0 * one_now
    regrets = (root_check_ref[...], root_bet_ref[...], fc_fold_ref[...], fc_call_ref[...])
    share_root = action_share(regrets[0], regrets[1])
    share_fc = action_share(regrets[2], regrets[3])
    share_ac = action_share(others[0], others[1])
    share_fb = action_share(others[2], others[3])
    one_cols = one_columns(one_now * live, share_root, share_fc)
    two_cols = two_columns(two_all, share_ac, share_fb)
    for k, row in enumerate((*one_rows(one_cols), *two_rows(two_cols))):
        turns[k] = turns[k] + 3.0 * row
    sign_sum, weight_sum = pair_sums(key_ref, 2, {**two_cols, **one_cols}, *scratch)
    values = two_values(sign_sum, weight_sum, share_root, share_fc)
    spread(cont_ref, flop_value(share_ref[...], values[5]))
    regrets = two_regrets(regrets, values)
    others = one_regrets(others, one_values(sign_sum, weight_sum, share_ac, share_fb))
    two_cols = two_columns(
        two_all, action_share(others[0], others[1]), action_share(others[2], others[3])
    )
    for k, row in enumerate(two_rows(two_cols)):
        turns[3 + k] = turns[3 + k] + 4.0 * row
    out_root_ref[...] = action_share(regrets[0], regrets[1])
    out_fc_ref[...] = action_share(regrets[2], regrets[3])
    for k in range(6):
        out_turn_ref[k] = turns[k]
    out_pre_ref[0:1, :] = pre_cont
    out_pre_ref[1:2, :] = pre_fold
    out_pre_ref[2:3, :] = pre_sum


def pair_scratch():
    return [
        pltpu.VMEM((16, H), jnp.float32),
        pltpu.VMEM((16, H), jnp.bfloat16),
        pltpu.VMEM((2, 16, PADDED), jnp.float32),
        pltpu.VMEM((2, H, BLOCK), jnp.int32),
        pltpu.VMEM((H, PADDED), jnp.bfloat16),
        pltpu.SemaphoreType.DMA,
    ]


def in_vmem(count):
    return [pl.BlockSpec(memory_space=pltpu.VMEM)] * count


def in_hbm():
    return pl.BlockSpec(memory_space=pltpu.HBM)


def rows_of(*shapes):
    return [jax.ShapeDtypeStruct(shape, jnp.float32) for shape in shapes]


def last_kernel(
    live_ref, one_ref, sums_in_ref, share_root_ref, share_fc_ref, turn_ref, pre_ref,
    out_ref, pre_out_ref,
):
    total_weight = ITERS * (ITERS + 1) / 2.0
    pre_cont, pre_fold = pre_step(pre_ref[0:1, :], pre_ref[1:2, :], add_parts(sums_in_ref))
    one_now = one_ref[...] * action_share(pre_cont, pre_fold)
    columns = one_columns(one_now * live_ref[...], share_root_ref[...], share_fc_ref[...])
    for k, row in enumerate(one_rows(columns)):
        out_ref[k] = (turn_ref[k] + 4.0 * row) / total_weight
    for k in range(3, 6):
        out_ref[k] = turn_ref[k] / total_weight
    pre_out_ref[...] = (pre_ref[2:3, :] + 4.0 * one_now) / total_weight


def solve(arrived, range_one, range_two, cards, compat):
    one_row = range_one.reshape(1, H)
    two_row = range_two.reshape(1, H)
    pair = (2, H)
    first_count = lax.axis_size(FIRST_SUM)
    key_now, live, share, cont, *state = pl.pallas_call(
        first_kernel,
        out_shape=[
            jax.ShapeDtypeStruct((ITERS - 1, 2, PADDED), jnp.int32),
            *rows_of(pair, (2, 1), (first_count, 1, H), *([pair] * 10), (6, 2, H)),
        ],
        in_specs=[*in_vmem(4), in_hbm()],
        scratch_shapes=pair_scratch(),
        name="first",
        compiler_params=pltpu.CompilerParams(vmem_limit_bytes=20 << 20),
    )(arrived, cards, one_row, two_row, compat)
    own_sum = jnp.sum(whole_parts(cont), axis=0)
    other_sum = lax.ppermute(own_sum, "grp_1", [(0, 1), (1, 0)])
    core = lax.axis_index("grp_1").astype(jnp.int32).reshape(1, 1)
    cont, share_root, share_fc, turns, pre = pl.pallas_call(
        second_kernel,
        out_shape=rows_of((first_count, 1, H), pair, pair, (6, 2, H), (3, H)),
        in_specs=[
            *in_vmem(5), in_hbm(), pl.BlockSpec(memory_space=pltpu.SMEM), *in_vmem(13)
        ],
        scratch_shapes=pair_scratch(),
        name="second",
        compiler_params=pltpu.CompilerParams(vmem_limit_bytes=20 << 20),
    )(key_now, live, one_row, two_row, share, compat, core, own_sum, other_sum, *state)
    parts = whole_parts(cont)
    turns, pre = pl.pallas_call(
        last_kernel,
        out_shape=rows_of((6, 2, H), (1, H)),
        name="last",
        compiler_params=pltpu.CompilerParams(vmem_limit_bytes=8 << 20),
    )(live, one_row, parts, share_root, share_fc, turns, pre)
    return jnp.swapaxes(turns, 0, 1), pre.reshape(H)


def exchanged(copies, axis):
    return lax.all_to_all(copies, axis, split_axis=0, concat_axis=0, tiled=True)


def whole_parts(copies):
    part = jnp.sum(exchanged(copies, FIRST_SUM), axis=0)
    return sent_to_all(part, SECOND_SUM)


ROWS = 80
FIRST_ROWS = (0, 0, FLOP_GRP // 2, FLOP_GRP)


def pack_kernel(first_hand_ref, strength_ref, board_ref, weight_ref, cards_ref, out_ref):
    groups, rows, width = out_ref.shape
    hand_block, _, capacity = strength_ref.shape
    used = ITERS - 1
    hand = first_hand_ref[0, 0] + lax.broadcasted_iota(jnp.int32, (hand_block, capacity), 0)
    flop_live = (board_ref[...] == 1) & (hand < HANDS)
    keys = [jnp.where(flop_live, strength_ref[:, counter, :] + 1, 0) for counter in range(used)]
    weights = weight_ref[...]
    cards = [cards_ref[counter] for counter in range(used)]
    count = jnp.zeros((1, width), jnp.int32) + jnp.sum((weights > 0).astype(jnp.int32))
    extra = used * hand_block
    for group, first in enumerate(FIRST_ROWS):
        for counter in range(used):
            out_ref[group, hand_block * counter : hand_block * (counter + 1), :] = keys[counter][
                :, first : first + width
            ]
        out_ref[group, extra : extra + 1, :] = weights[:, first : first + width]
        for counter in range(used):
            row = extra + 1 + 2 * counter
            out_ref[group, row : row + 2, :] = cards[counter][:, first : first + width]
        blank = extra + 1 + 2 * used
        out_ref[group, blank : blank + 1, :] = count
        out_ref[group, blank + 1 :, :] = jnp.zeros((rows - blank - 1, width), jnp.int32)


def packed(first_hand, strength, board_mask, flop_weight, runout, groups):
    capacity = strength.shape[0]
    return pl.pallas_call(
        pack_kernel,
        out_shape=jax.ShapeDtypeStruct((groups, ROWS, FLOP_GRP), jnp.int32),
        in_specs=[
            pl.BlockSpec(memory_space=pltpu.SMEM),
            *([pl.BlockSpec(memory_space=pltpu.VMEM)] * 4),
        ],
        name="pack",
    )(
        first_hand.astype(jnp.int32).reshape(1, 1),
        jnp.transpose(strength, (2, 1, 0)),
        board_mask.T,
        flop_weight.reshape(1, capacity),
        jnp.transpose(runout, (1, 2, 0)),
    )


def route_kernel(group_ref, slots_ref, out_ref):
    groups, rows, width = slots_ref.shape
    pairs = out_ref.shape[0]
    count_row = (ITERS - 1) * (H // pairs + 2) + 1
    group = group_ref[0, 0]
    first = jnp.where(group == 3, FIRST_ROWS[3], jnp.where(group == 2, FIRST_ROWS[2], 0))
    row = first + lax.broadcasted_iota(jnp.int32, (1, width), 1)
    counts = [slots_ref[g, count_row : count_row + 1, :] for g in range(groups)]
    totals = [[jnp.zeros((pairs, LINE), jnp.float32) for part in range(4)] for odd in range(2)]
    pair = lax.broadcasted_iota(jnp.int32, (pairs, width), 0)
    blank = jnp.zeros((LINE - rows, width), jnp.int32)
    for g in range(groups):
        place = -2 * pairs * group + jnp.zeros((1, width), jnp.int32)
        for other in range(groups):
            place = place + jnp.minimum(counts[other], row + int(other < g))
        place = jnp.where(row < counts[g], place, -1)
        values = jnp.concatenate([slots_ref[g], blank])
        picks = [
            (place == 2 * pair + odd).astype(jnp.float32).astype(jnp.bfloat16) for odd in range(2)
        ]
        for part in range(4):
            digits = (values >> (8 * part)) & (PART - 1)
            digits = digits.astype(jnp.float32).astype(jnp.bfloat16)
            for odd in range(2):
                found = lax.dot_general(
                    picks[odd], digits, (((1,), (1,)), ((), ())), preferred_element_type=jnp.float32
                )
                totals[odd][part] = totals[odd][part] + found
    for odd in range(2):
        whole = jnp.zeros((pairs, LINE), jnp.int32)
        for part in range(4):
            whole = whole + (totals[odd][part].astype(jnp.int32) << (8 * part))
        out_ref[:, 0, LINE * odd : LINE * (odd + 1)] = whole


def route(slots, group_id, pairs):
    return pl.pallas_call(
        route_kernel,
        out_shape=jax.ShapeDtypeStruct((pairs, 1, 2 * LINE), jnp.int32),
        in_specs=[pl.BlockSpec(memory_space=pltpu.SMEM), pl.BlockSpec(memory_space=pltpu.VMEM)],
        name="route",
        compiler_params=pltpu.CompilerParams(vmem_limit_bytes=12 << 20),
    )(group_id.astype(jnp.int32).reshape(1, 1), slots)


def on_device(range_one, range_two, flop_weight, board_mask, runout, strength):
    groups = lax.axis_size(GRP)
    shards = lax.axis_size(INF)
    shard_id = lax.axis_index(INF)
    hand_block = strength.shape[2]
    first_hand = shard_id * hand_block
    cards = jnp.asarray(np.stack(hand_cards(PADDED, HANDS)))
    slots = exchanged(
        packed(first_hand, strength, board_mask, flop_weight, runout, groups), GRP
    )
    slots, compat = lax.optimization_barrier((slots, compat_matrix(cards)))
    routed = route(slots, lax.axis_index(GRP), shards)
    routed, compat = lax.optimization_barrier((routed, compat))
    arrived = exchanged(routed, INF)
    compat = pltpu.with_memory_space_constraint(compat, pltpu.HBM)
    turn_reach, pre_reach = solve(arrived, range_one, range_two, cards, compat)
    return turn_reach, lax.dynamic_slice(
        pre_reach, (first_hand,), (hand_block,), allow_negative_indices=False
    )


def solution(mesh):
    split = Mesh(mesh.devices.reshape(2, 2, 4, 8, 2), ("grp_0", "grp_1", "inf_0", "inf_1", "inf_2"))
    return jax.shard_map(
        on_device,
        mesh=split,
        in_specs=(P(), P(), P(GRP), P(GRP, INF), P(GRP, None, None), P(GRP, None, INF)),
        out_specs=(P(GRP_INF, None, None), P(INF)),
        check_vma=False,
    )
```

```python
from functools import partial

import jax
import jax.numpy as jnp
import numpy as np
from jax import lax
from jax.experimental import pallas as pl
from jax.experimental.pallas import tpu as pltpu
from jax.sharding import Mesh
from jax.sharding import PartitionSpec as P

HANDS = 1326
H = 1408
ITERS = 4
FLOP_GRP = 128
GRP = ("grp_0", "grp_1")
INF = ("inf_0", "inf_1", "inf_2")
GRP_INF = ("grp_0", "grp_1", "inf_0", "inf_1", "inf_2")


EPSILON = 0.01
FOLD_VALUE = -0.1


def sent_to_all(x, axis):
    copies = jnp.broadcast_to(x, (lax.axis_size(axis), *x.shape))
    return lax.all_to_all(copies, axis, split_axis=0, concat_axis=0, tiled=True)


def hand_cards(slot_total, real_total):
    low_list = []
    high_list = []
    for first_card in range(52):
        for second_card in range(first_card + 1, 52):
            low_list.append(first_card)
            high_list.append(second_card)
    low_table = np.full(slot_total, 52, np.int32)
    high_table = np.full(slot_total, 53, np.int32)
    used_count = min(slot_total, real_total)
    low_table[:used_count] = np.array(low_list[:used_count], np.int32)
    high_table[:used_count] = np.array(high_list[:used_count], np.int32)
    return (low_table, high_table)


def action_share(first_regret, second_regret):
    return (first_regret + EPSILON) / (first_regret + second_regret + 2.0 * EPSILON)


SCALE = 1.0 / HANDS
FLOP_TOTAL = 12.0 * FLOP_GRP * 4
LINE = 128
PART = 256
BLOCK = 128
UPPER = 6
WIDE = 1408
DEEP = 128
PADDED = 1408
FIRST_SUM = ("grp_1", "inf_0", "inf_2")
SECOND_SUM = ("grp_0", "inf_1")


def compat_kernel(first_block, cards_ref, out_ref, rows_ref, sems):
    low_ref = cards_ref.at[0:1]
    high_ref = cards_ref.at[1:2]

    def sent(step):
        first = pl.multiple_of(step * BLOCK, BLOCK)
        return pltpu.make_async_copy(
            rows_ref.at[step], out_ref.at[pl.ds(first, BLOCK)], sems.at[step]
        )

    def rows(step, carry):
        first = pl.multiple_of((first_block + step) * BLOCK, BLOCK)
        low_col = jnp.broadcast_to(low_ref[:, pl.ds(first, BLOCK)], (BLOCK, BLOCK)).T
        high_col = jnp.broadcast_to(high_ref[:, pl.ds(first, BLOCK)], (BLOCK, BLOCK)).T
        for start in range(0, PADDED, BLOCK):
            low_here = low_ref[:, start : start + BLOCK]
            high_here = high_ref[:, start : start + BLOCK]
            apart = (low_col != low_here) & (low_col != high_here)
            apart = apart & (high_col != low_here) & (high_col != high_here)
            rows_ref[step, :, start : start + BLOCK] = jnp.where(apart, 1.0, 0.0).astype(
                jnp.bfloat16
            )
        sent(step).start()
        return carry

    lax.fori_loop(0, rows_ref.shape[0], rows, 0)
    for step in range(rows_ref.shape[0]):
        sent(step).wait()


def compat_rows(cards, first_block, blocks):
    return pl.pallas_call(
        partial(compat_kernel, first_block),
        out_shape=pltpu.HBM((blocks * BLOCK, PADDED), jnp.bfloat16),
        out_specs=pl.BlockSpec(memory_space=pltpu.HBM),
        scratch_shapes=[
            pltpu.VMEM((blocks, BLOCK, PADDED), jnp.bfloat16),
            pltpu.SemaphoreType.DMA((blocks,)),
        ],
        name="compat",
        compiler_params=pltpu.CompilerParams(vmem_limit_bytes=12 << 20),
    )(cards)


def compat_copies(upper_ref, lower_ref, compat_ref, sems):
    middle = upper_ref.shape[0]
    return (
        pltpu.make_async_copy(upper_ref, compat_ref.at[pl.ds(0, middle)], sems.at[0]),
        pltpu.make_async_copy(lower_ref, compat_ref.at[pl.ds(middle, H - middle)], sems.at[1]),
    )


def pair_sums(key_ref, counter, columns, compat_ref, lhs_ref, low_ref, sums_ref, col_ref, fetch=()):
    alive = (key_ref[counter, :, :H] >= 0).astype(jnp.float32)
    lhs_ref[...] = jnp.zeros((16, H), jnp.float32)
    for k, column in columns.items():
        lhs_ref[2 * k : 2 * k + 2, :] = column * alive
    low_ref[...] = lhs_ref[...].astype(jnp.bfloat16)

    def key_column(step, carry):
        first = pl.multiple_of(step * BLOCK, BLOCK)
        for flop in range(2):
            keys = key_ref[counter, flop : flop + 1, pl.ds(first, BLOCK)]
            col_ref[flop, pl.ds(first, BLOCK), :] = jnp.broadcast_to(keys, (BLOCK, BLOCK)).T
        return carry

    lax.fori_loop(0, H // BLOCK, key_column, 0)
    for part in fetch:
        part.wait()

    def mine(step, carry):
        start = pl.multiple_of(step * WIDE, WIDE)
        weight_total = jnp.zeros((16, WIDE), jnp.float32)
        totals = [jnp.zeros((16, WIDE), jnp.float32) for flop in range(2)]
        rows = [key_ref[counter, flop : flop + 1, pl.ds(start, WIDE)] for flop in range(2)]
        for first in range(0, H, DEEP):
            depth = min(DEEP, H - first)
            lhs = low_ref[:, first : first + depth]
            most = compat_ref[first : first + depth, pl.ds(start, WIDE)]
            weight_total = weight_total + jnp.dot(lhs, most, preferred_element_type=jnp.float32)
            for flop in range(2):
                parts = []
                key_col = col_ref[flop, first : first + depth, :]
                for lane in range(0, WIDE, BLOCK):
                    gap = rows[flop][:, lane : lane + BLOCK] - key_col
                    parts.append(gap.astype(jnp.float32).astype(jnp.bfloat16))
                sign = jnp.concatenate(parts, axis=1) if len(parts) > 1 else parts[0]
                one = jnp.bfloat16(1)
                sign = jnp.minimum(jnp.maximum(sign, -one), one) * most
                totals[flop] = totals[flop] + jnp.dot(
                    lhs, sign, preferred_element_type=jnp.float32
                )
        row_flop = lax.broadcasted_iota(jnp.int32, (16, WIDE), 0) & 1
        sums_ref[0, :, pl.ds(start, WIDE)] = jnp.where(row_flop == 0, totals[0], totals[1])
        sums_ref[1, :, pl.ds(start, WIDE)] = weight_total
        return carry

    lax.fori_loop(0, PADDED // WIDE, mine, 0)
    sign_sum = {k: sums_ref[0, 2 * k : 2 * k + 2, :H] * alive for k in columns}
    weight_sum = {k: sums_ref[1, 2 * k : 2 * k + 2, :H] * alive for k in columns}
    return sign_sum, weight_sum


def two_values(sign_sum, weight_sum, share_root, share_fc):
    v_cc = 0.5 * SCALE * sign_sum[1]
    v_cbf = -0.5 * SCALE * (weight_sum[0] - weight_sum[1])
    v_cbc = 1.5 * SCALE * (sign_sum[0] - sign_sum[1])
    v_bf = 0.5 * SCALE * weight_sum[2]
    v_bc = 1.5 * SCALE * (sign_sum[0] - sign_sum[2])
    u_fc = share_fc * v_cbf + (1.0 - share_fc) * v_cbc
    v_check = v_cc + u_fc
    v_bet = v_bf + v_bc
    u_root = share_root * v_check + (1.0 - share_root) * v_bet
    return v_cbf, v_cbc, u_fc, v_check, v_bet, u_root


def one_values(sign_sum, weight_sum, share_ac, share_fb):
    w_cc = 0.5 * SCALE * sign_sum[4]
    w_cbf = 0.5 * SCALE * weight_sum[5]
    w_cbc = 1.5 * SCALE * (sign_sum[4] - sign_sum[5])
    w_bf = -0.5 * SCALE * (weight_sum[3] - weight_sum[4])
    w_bc = 1.5 * SCALE * (sign_sum[3] - sign_sum[4])
    x_bet = w_cbf + w_cbc
    u_ac = share_ac * w_cc + (1.0 - share_ac) * x_bet
    u_fb = share_fb * w_bf + (1.0 - share_fb) * w_bc
    return w_cc, x_bet, u_ac, w_bf, w_bc, u_fb


def two_regrets(regrets, values):
    root_check, root_bet, fc_fold, fc_call = regrets
    v_cbf, v_cbc, u_fc, v_check, v_bet, u_root = values
    return (
        jnp.maximum(root_check + v_check - u_root, 0.0),
        jnp.maximum(root_bet + v_bet - u_root, 0.0),
        jnp.maximum(fc_fold + v_cbf - u_fc, 0.0),
        jnp.maximum(fc_call + v_cbc - u_fc, 0.0),
    )


def one_regrets(regrets, values):
    ac_check, ac_bet, fb_fold, fb_call = regrets
    w_cc, x_bet, u_ac, w_bf, w_bc, u_fb = values
    return (
        jnp.maximum(ac_check + w_cc - u_ac, 0.0),
        jnp.maximum(ac_bet + x_bet - u_ac, 0.0),
        jnp.maximum(fb_fold + w_bf - u_fb, 0.0),
        jnp.maximum(fb_call + w_bc - u_fb, 0.0),
    )


def pre_step(pre_cont, pre_fold, cont_value):
    share_pre = action_share(pre_cont, pre_fold)
    u_pre = share_pre * cont_value + (1.0 - share_pre) * FOLD_VALUE
    return (
        jnp.maximum(pre_cont + cont_value - u_pre, 0.0),
        jnp.maximum(pre_fold + FOLD_VALUE - u_pre, 0.0),
    )


def one_columns(one_all, share_root, share_fc):
    one_check = one_all * share_root
    return {3: one_all, 4: one_check, 5: one_check * share_fc}


def two_columns(two_all, share_ac, share_fb):
    return {0: two_all, 1: two_all * share_ac, 2: two_all * share_fb}


def one_rows(columns):
    return columns[4], columns[3] - columns[4], columns[4] - columns[5]


def two_rows(columns):
    return columns[1], columns[0] - columns[2], columns[0] - columns[1]


def flop_value(share, u_root):
    part = share * u_root
    return part[0:1, :] + part[1:2, :]


def add_parts(parts_ref):
    total = parts_ref[0]
    for k in range(1, parts_ref.shape[0]):
        total = total + parts_ref[k]
    return total


def spread(copies_ref, value, part=0, parts=1):
    count = copies_ref.shape[0] // parts
    for k in range(count * part, count * (part + 1)):
        copies_ref[k] = value


def read_flops(arrived_ref, cards_ref, key_ref, live_ref, share_ref):
    used = key_ref.shape[0]
    shards = arrived_ref.shape[0]
    hand_block = H // shards
    for shard in range(shards):
        line = arrived_ref[shard] - 1
        for flop in range(2):
            for counter in range(used):
                first = LINE * flop + hand_block * counter
                key_ref[
                    counter, flop : flop + 1, hand_block * shard : hand_block * (shard + 1)
                ] = line[:, first : first + hand_block]
    live_ref[...] = (key_ref[0, :, :H] >= 0).astype(jnp.float32)
    low = cards_ref[0:1, :]
    high = cards_ref[1:2, :]
    for flop in range(2):
        first = LINE * flop + hand_block * used
        extra = arrived_ref[0, :, first : first + 1 + 2 * used]
        share_ref[flop : flop + 1, :] = extra[:, 0:1].astype(jnp.float32) / FLOP_TOTAL
        for counter in range(used):
            turn = extra[:, 1 + 2 * counter : 2 + 2 * counter]
            river = extra[:, 2 + 2 * counter : 3 + 2 * counter]
            blocked = (low == turn) | (low == river) | (high == turn) | (high == river)
            blocked = blocked | (lax.broadcasted_iota(jnp.int32, (1, PADDED), 1) >= H)
            row = key_ref[counter, flop : flop + 1, :]
            key_ref[counter, flop : flop + 1, :] = jnp.where(blocked, -1, row)


def first_kernel(
    arrived_ref, cards_ref, one_ref, two_ref, upper_ref, lower_ref,
    key_ref, live_ref, share_ref, cont_ref,
    root_check_ref, root_bet_ref, fc_fold_ref, fc_call_ref,
    ac_check_ref, ac_bet_ref, fb_fold_ref, fb_call_ref, share_root_ref, share_fc_ref, turn_ref,
    lhs_ref, low_part_ref, sums_ref, col_ref, compat_ref, compat_sem,
):
    fetch = compat_copies(upper_ref, lower_ref, compat_ref, compat_sem)
    for part in fetch:
        part.start()
    scratch = (compat_ref, lhs_ref, low_part_ref, sums_ref, col_ref)
    read_flops(arrived_ref, cards_ref, key_ref, live_ref, share_ref)
    live = live_ref[...]
    share = share_ref[...]
    zero = jnp.zeros((2, H), jnp.float32)
    zero_row = jnp.zeros((1, H), jnp.float32)
    two_all = two_ref[...] * live
    start = action_share(zero, zero)
    one_all = one_ref[...] * action_share(zero_row, zero_row) * live
    one_cols = one_columns(one_all, start, start)
    two_cols = two_columns(two_all, start, start)
    sign_sum, weight_sum = pair_sums(key_ref, 0, {**two_cols, **one_cols}, *scratch, fetch)
    values = two_values(sign_sum, weight_sum, start, start)
    spread(cont_ref, flop_value(share, values[5]), 0, 2)
    regrets = two_regrets((zero, zero, zero, zero), values)
    others = one_regrets((zero, zero, zero, zero), one_values(sign_sum, weight_sum, start, start))
    turns = [*one_rows(one_cols), *two_rows(two_cols)]

    share_root = action_share(regrets[0], regrets[1])
    share_fc = action_share(regrets[2], regrets[3])
    two_cols = two_columns(
        two_all, action_share(others[0], others[1]), action_share(others[2], others[3])
    )
    sign_sum, weight_sum = pair_sums(key_ref, 1, two_cols, *scratch)
    values = two_values(sign_sum, weight_sum, share_root, share_fc)
    spread(cont_ref, flop_value(share, values[5]), 1, 2)
    regrets = two_regrets(regrets, values)
    for k, row in enumerate(two_rows(two_cols)):
        turns[3 + k] = turns[3 + k] + 2.0 * row
    root_check_ref[...], root_bet_ref[...], fc_fold_ref[...], fc_call_ref[...] = regrets
    ac_check_ref[...], ac_bet_ref[...], fb_fold_ref[...], fb_call_ref[...] = others
    share_root_ref[...] = share_root
    share_fc_ref[...] = share_fc
    for k in range(6):
        turn_ref[k] = turns[k]


def second_kernel(
    key_ref, live_ref, one_ref, two_ref, share_ref, upper_ref, lower_ref,
    core_ref, own_sum_ref, other_sum_ref,
    root_check_ref, root_bet_ref, fc_fold_ref, fc_call_ref,
    ac_check_ref, ac_bet_ref, fb_fold_ref, fb_call_ref, share_root_ref, share_fc_ref, turn_ref,
    cont_ref, out_root_ref, out_fc_ref, out_turn_ref, out_pre_ref,
    lhs_ref, low_ref, sums_ref, col_ref, compat_ref, compat_sem,
):
    fetch = compat_copies(upper_ref, lower_ref, compat_ref, compat_sem)
    for part in fetch:
        part.start()
    scratch = (compat_ref, lhs_ref, low_ref, sums_ref, col_ref)
    first_core = core_ref[0, 0] == 0
    own_sum = own_sum_ref[...]
    other_sum = other_sum_ref[...]
    live = live_ref[...]
    zero_row = jnp.zeros((1, H), jnp.float32)
    two_all = two_ref[...] * live
    one_range = one_ref[...]
    turns = [turn_ref[k] for k in range(6)]
    pre_sum = one_range * action_share(zero_row, zero_row)
    pre_cont, pre_fold = pre_step(zero_row, zero_row, jnp.where(first_core, own_sum, other_sum))
    one_now = one_range * action_share(pre_cont, pre_fold)
    pre_sum = pre_sum + 2.0 * one_now
    one_cols = one_columns(one_now * live, share_root_ref[...], share_fc_ref[...])
    for k, row in enumerate(one_rows(one_cols)):
        turns[k] = turns[k] + 2.0 * row
    others = (ac_check_ref[...], ac_bet_ref[...], fb_fold_ref[...], fb_call_ref[...])
    share_ac = action_share(others[0], others[1])
    share_fb = action_share(others[2], others[3])
    sign_sum, weight_sum = pair_sums(key_ref, 1, one_cols, *scratch, fetch)
    others = one_regrets(others, one_values(sign_sum, weight_sum, share_ac, share_fb))

    pre_cont, pre_fold = pre_step(pre_cont, pre_fold, jnp.where(first_core, other_sum, own_sum))
    one_now = one_range * action_share(pre_cont, pre_fold)
    pre_sum = pre_sum + 3.0 * one_now
    regrets = (root_check_ref[...], root_bet_ref[...], fc_fold_ref[...], fc_call_ref[...])
    share_root = action_share(regrets[0], regrets[1])
    share_fc = action_share(regrets[2], regrets[3])
    share_ac = action_share(others[0], others[1])
    share_fb = action_share(others[2], others[3])
    one_cols = one_columns(one_now * live, share_root, share_fc)
    two_cols = two_columns(two_all, share_ac, share_fb)
    for k, row in enumerate((*one_rows(one_cols), *two_rows(two_cols))):
        turns[k] = turns[k] + 3.0 * row
    sign_sum, weight_sum = pair_sums(key_ref, 2, {**two_cols, **one_cols}, *scratch)
    values = two_values(sign_sum, weight_sum, share_root, share_fc)
    spread(cont_ref, flop_value(share_ref[...], values[5]))
    regrets = two_regrets(regrets, values)
    others = one_regrets(others, one_values(sign_sum, weight_sum, share_ac, share_fb))
    two_cols = two_columns(
        two_all, action_share(others[0], others[1]), action_share(others[2], others[3])
    )
    for k, row in enumerate(two_rows(two_cols)):
        turns[3 + k] = turns[3 + k] + 4.0 * row
    out_root_ref[...] = action_share(regrets[0], regrets[1])
    out_fc_ref[...] = action_share(regrets[2], regrets[3])
    for k in range(6):
        out_turn_ref[k] = turns[k]
    out_pre_ref[0:1, :] = pre_cont
    out_pre_ref[1:2, :] = pre_fold
    out_pre_ref[2:3, :] = pre_sum


def pair_scratch():
    return [
        pltpu.VMEM((16, H), jnp.float32),
        pltpu.VMEM((16, H), jnp.bfloat16),
        pltpu.VMEM((2, 16, PADDED), jnp.float32),
        pltpu.VMEM((2, H, BLOCK), jnp.int32),
        pltpu.VMEM((H, PADDED), jnp.bfloat16),
        pltpu.SemaphoreType.DMA((2,)),
    ]


def in_vmem(count):
    return [pl.BlockSpec(memory_space=pltpu.VMEM)] * count


def in_hbm():
    return pl.BlockSpec(memory_space=pltpu.HBM)


def rows_of(*shapes):
    return [jax.ShapeDtypeStruct(shape, jnp.float32) for shape in shapes]


def last_kernel(
    live_ref, one_ref, sums_in_ref, share_root_ref, share_fc_ref, turn_ref, pre_ref,
    out_ref, pre_out_ref,
):
    total_weight = ITERS * (ITERS + 1) / 2.0
    pre_cont, pre_fold = pre_step(pre_ref[0:1, :], pre_ref[1:2, :], add_parts(sums_in_ref))
    one_now = one_ref[...] * action_share(pre_cont, pre_fold)
    columns = one_columns(one_now * live_ref[...], share_root_ref[...], share_fc_ref[...])
    for k, row in enumerate(one_rows(columns)):
        out_ref[k] = (turn_ref[k] + 4.0 * row) / total_weight
    for k in range(3, 6):
        out_ref[k] = turn_ref[k] / total_weight
    pre_out_ref[...] = (pre_ref[2:3, :] + 4.0 * one_now) / total_weight


def solve(arrived, range_one, range_two, cards, compat):
    one_row = range_one.reshape(1, H)
    two_row = range_two.reshape(1, H)
    pair = (2, H)
    first_count = lax.axis_size(FIRST_SUM)
    key_now, live, share, cont, *state = pl.pallas_call(
        first_kernel,
        out_shape=[
            jax.ShapeDtypeStruct((ITERS - 1, 2, PADDED), jnp.int32),
            *rows_of(pair, (2, 1), (first_count, 1, H), *([pair] * 10), (6, 2, H)),
        ],
        in_specs=[*in_vmem(4), in_hbm(), in_hbm()],
        scratch_shapes=pair_scratch(),
        name="first",
        compiler_params=pltpu.CompilerParams(vmem_limit_bytes=20 << 20),
    )(arrived, cards, one_row, two_row, *compat)
    own_sum = jnp.sum(whole_parts(cont), axis=0)
    other_sum = lax.ppermute(own_sum, "grp_1", [(0, 1), (1, 0)])
    core = lax.axis_index("grp_1").astype(jnp.int32).reshape(1, 1)
    cont, share_root, share_fc, turns, pre = pl.pallas_call(
        second_kernel,
        out_shape=rows_of((first_count, 1, H), pair, pair, (6, 2, H), (3, H)),
        in_specs=[
            *in_vmem(5), in_hbm(), in_hbm(), pl.BlockSpec(memory_space=pltpu.SMEM), *in_vmem(13)
        ],
        scratch_shapes=pair_scratch(),
        name="second",
        compiler_params=pltpu.CompilerParams(vmem_limit_bytes=20 << 20),
    )(key_now, live, one_row, two_row, share, *compat, core, own_sum, other_sum, *state)
    parts = whole_parts(cont)
    turns, pre = pl.pallas_call(
        last_kernel,
        out_shape=rows_of((6, 2, H), (1, H)),
        name="last",
        compiler_params=pltpu.CompilerParams(vmem_limit_bytes=8 << 20),
    )(live, one_row, parts, share_root, share_fc, turns, pre)
    return jnp.swapaxes(turns, 0, 1), pre.reshape(H)


def exchanged(copies, axis):
    return lax.all_to_all(copies, axis, split_axis=0, concat_axis=0, tiled=True)


def whole_parts(copies):
    part = jnp.sum(exchanged(copies, FIRST_SUM), axis=0)
    return sent_to_all(part, SECOND_SUM)


ROWS = 80
FIRST_ROWS = (0, 0, FLOP_GRP // 2, FLOP_GRP)


def pack_kernel(first_hand_ref, strength_ref, board_ref, weight_ref, cards_ref, out_ref):
    groups, rows, width = out_ref.shape
    hand_block, _, capacity = strength_ref.shape
    used = ITERS - 1
    hand = first_hand_ref[0, 0] + lax.broadcasted_iota(jnp.int32, (hand_block, capacity), 0)
    flop_live = (board_ref[...] == 1) & (hand < HANDS)
    keys = [jnp.where(flop_live, strength_ref[:, counter, :] + 1, 0) for counter in range(used)]
    weights = weight_ref[...]
    cards = [cards_ref[counter] for counter in range(used)]
    count = jnp.zeros((1, width), jnp.int32) + jnp.sum((weights > 0).astype(jnp.int32))
    extra = used * hand_block
    for group, first in enumerate(FIRST_ROWS):
        for counter in range(used):
            out_ref[group, hand_block * counter : hand_block * (counter + 1), :] = keys[counter][
                :, first : first + width
            ]
        out_ref[group, extra : extra + 1, :] = weights[:, first : first + width]
        for counter in range(used):
            row = extra + 1 + 2 * counter
            out_ref[group, row : row + 2, :] = cards[counter][:, first : first + width]
        blank = extra + 1 + 2 * used
        out_ref[group, blank : blank + 1, :] = count
        out_ref[group, blank + 1 :, :] = jnp.zeros((rows - blank - 1, width), jnp.int32)


def packed(first_hand, strength, board_mask, flop_weight, runout, groups):
    capacity = strength.shape[0]
    return pl.pallas_call(
        pack_kernel,
        out_shape=jax.ShapeDtypeStruct((groups, ROWS, FLOP_GRP), jnp.int32),
        in_specs=[
            pl.BlockSpec(memory_space=pltpu.SMEM),
            *([pl.BlockSpec(memory_space=pltpu.VMEM)] * 4),
        ],
        name="pack",
    )(
        first_hand.astype(jnp.int32).reshape(1, 1),
        jnp.transpose(strength, (2, 1, 0)),
        board_mask.T,
        flop_weight.reshape(1, capacity),
        jnp.transpose(runout, (1, 2, 0)),
    )


def route_kernel(group_ref, slots_ref, out_ref):
    groups, rows, width = slots_ref.shape
    pairs = out_ref.shape[0]
    count_row = (ITERS - 1) * (H // pairs + 2) + 1
    group = group_ref[0, 0]
    first = jnp.where(group == 3, FIRST_ROWS[3], jnp.where(group == 2, FIRST_ROWS[2], 0))
    row = first + lax.broadcasted_iota(jnp.int32, (1, width), 1)
    counts = [slots_ref[g, count_row : count_row + 1, :] for g in range(groups)]
    totals = [[jnp.zeros((pairs, LINE), jnp.float32) for part in range(4)] for odd in range(2)]
    pair = lax.broadcasted_iota(jnp.int32, (pairs, width), 0)
    blank = jnp.zeros((LINE - rows, width), jnp.int32)
    for g in range(groups):
        place = -2 * pairs * group + jnp.zeros((1, width), jnp.int32)
        for other in range(groups):
            place = place + jnp.minimum(counts[other], row + int(other < g))
        place = jnp.where(row < counts[g], place, -1)
        values = jnp.concatenate([slots_ref[g], blank])
        picks = [
            (place == 2 * pair + odd).astype(jnp.float32).astype(jnp.bfloat16) for odd in range(2)
        ]
        for part in range(4):
            digits = (values >> (8 * part)) & (PART - 1)
            digits = digits.astype(jnp.float32).astype(jnp.bfloat16)
            for odd in range(2):
                found = lax.dot_general(
                    picks[odd], digits, (((1,), (1,)), ((), ())), preferred_element_type=jnp.float32
                )
                totals[odd][part] = totals[odd][part] + found
    for odd in range(2):
        whole = jnp.zeros((pairs, LINE), jnp.int32)
        for part in range(4):
            whole = whole + (totals[odd][part].astype(jnp.int32) << (8 * part))
        out_ref[:, 0, LINE * odd : LINE * (odd + 1)] = whole


def route(slots, group_id, pairs):
    return pl.pallas_call(
        route_kernel,
        out_shape=jax.ShapeDtypeStruct((pairs, 1, 2 * LINE), jnp.int32),
        in_specs=[pl.BlockSpec(memory_space=pltpu.SMEM), pl.BlockSpec(memory_space=pltpu.VMEM)],
        name="route",
        compiler_params=pltpu.CompilerParams(vmem_limit_bytes=12 << 20),
    )(group_id.astype(jnp.int32).reshape(1, 1), slots)


def on_device(range_one, range_two, flop_weight, board_mask, runout, strength):
    groups = lax.axis_size(GRP)
    shards = lax.axis_size(INF)
    shard_id = lax.axis_index(INF)
    hand_block = strength.shape[2]
    first_hand = shard_id * hand_block
    cards = jnp.asarray(np.stack(hand_cards(PADDED, HANDS)))
    slots = exchanged(
        packed(first_hand, strength, board_mask, flop_weight, runout, groups), GRP
    )
    slots, upper = lax.optimization_barrier((slots, compat_rows(cards, 0, UPPER)))
    arrived = exchanged(route(slots, lax.axis_index(GRP), shards), INF)
    lower = compat_rows(cards, UPPER, H // BLOCK - UPPER)
    compat = [pltpu.with_memory_space_constraint(part, pltpu.HBM) for part in (upper, lower)]
    turn_reach, pre_reach = solve(arrived, range_one, range_two, cards, compat)
    return turn_reach, lax.dynamic_slice(
        pre_reach, (first_hand,), (hand_block,), allow_negative_indices=False
    )


def solution(mesh):
    split = Mesh(mesh.devices.reshape(2, 2, 4, 8, 2), ("grp_0", "grp_1", "inf_0", "inf_1", "inf_2"))
    return jax.shard_map(
        on_device,
        mesh=split,
        in_specs=(P(), P(), P(GRP), P(GRP, INF), P(GRP, None, None), P(GRP, None, INF)),
        out_specs=(P(GRP_INF, None, None), P(INF)),
        check_vma=False,
    )
```

```python
from functools import partial

import jax
import jax.numpy as jnp
import numpy as np
from jax import lax
from jax.experimental import pallas as pl
from jax.experimental.pallas import tpu as pltpu
from jax.sharding import Mesh
from jax.sharding import PartitionSpec as P

HANDS = 1326
H = 1408
ITERS = 4
FLOP_GRP = 128
GRP = ("grp_0", "grp_1")
INF = ("inf_0", "inf_1", "inf_2")
GRP_INF = ("grp_0", "grp_1", "inf_0", "inf_1", "inf_2")


EPSILON = 0.01
FOLD_VALUE = -0.1


def sent_to_all(x, axis):
    copies = jnp.broadcast_to(x, (lax.axis_size(axis), *x.shape))
    return lax.all_to_all(copies, axis, split_axis=0, concat_axis=0, tiled=True)


def hand_cards(slot_total, real_total):
    low_list = []
    high_list = []
    for first_card in range(52):
        for second_card in range(first_card + 1, 52):
            low_list.append(first_card)
            high_list.append(second_card)
    low_table = np.full(slot_total, 52, np.int32)
    high_table = np.full(slot_total, 53, np.int32)
    used_count = min(slot_total, real_total)
    low_table[:used_count] = np.array(low_list[:used_count], np.int32)
    high_table[:used_count] = np.array(high_list[:used_count], np.int32)
    return (low_table, high_table)


def action_share(first_regret, second_regret):
    return (first_regret + EPSILON) / (first_regret + second_regret + 2.0 * EPSILON)


SCALE = 1.0 / HANDS
FLOP_TOTAL = 12.0 * FLOP_GRP * 4
LINE = 128
PART = 256
BLOCK = 128
UPPER = 5
WIDE = 1408
DEEP = 128
PADDED = 1408
FIRST_SUM = ("grp_1", "inf_0", "inf_2")
SECOND_SUM = ("grp_0", "inf_1")


def compat_kernel(first_block, cards_ref, out_ref, rows_ref, sems):
    low_ref = cards_ref.at[0:1]
    high_ref = cards_ref.at[1:2]

    def sent(step):
        first = pl.multiple_of(step * BLOCK, BLOCK)
        return pltpu.make_async_copy(
            rows_ref.at[step], out_ref.at[pl.ds(first, BLOCK)], sems.at[step]
        )

    def rows(step, carry):
        first = pl.multiple_of((first_block + step) * BLOCK, BLOCK)
        low_col = jnp.broadcast_to(low_ref[:, pl.ds(first, BLOCK)], (BLOCK, BLOCK)).T
        high_col = jnp.broadcast_to(high_ref[:, pl.ds(first, BLOCK)], (BLOCK, BLOCK)).T
        for start in range(0, PADDED, BLOCK):
            low_here = low_ref[:, start : start + BLOCK]
            high_here = high_ref[:, start : start + BLOCK]
            apart = (low_col != low_here) & (low_col != high_here)
            apart = apart & (high_col != low_here) & (high_col != high_here)
            rows_ref[step, :, start : start + BLOCK] = jnp.where(apart, 1.0, 0.0).astype(
                jnp.bfloat16
            )
        sent(step).start()
        return carry

    lax.fori_loop(0, rows_ref.shape[0], rows, 0)
    for step in range(rows_ref.shape[0]):
        sent(step).wait()


def compat_rows(cards, first_block, blocks):
    return pl.pallas_call(
        partial(compat_kernel, first_block),
        out_shape=pltpu.HBM((blocks * BLOCK, PADDED), jnp.bfloat16),
        out_specs=pl.BlockSpec(memory_space=pltpu.HBM),
        scratch_shapes=[
            pltpu.VMEM((blocks, BLOCK, PADDED), jnp.bfloat16),
            pltpu.SemaphoreType.DMA((blocks,)),
        ],
        name="compat",
        compiler_params=pltpu.CompilerParams(vmem_limit_bytes=12 << 20),
    )(cards)


def compat_copies(upper_ref, lower_ref, compat_ref, sems):
    middle = upper_ref.shape[0]
    return (
        pltpu.make_async_copy(upper_ref, compat_ref.at[pl.ds(0, middle)], sems.at[0]),
        pltpu.make_async_copy(lower_ref, compat_ref.at[pl.ds(middle, H - middle)], sems.at[1]),
    )


def pair_sums(key_ref, counter, columns, compat_ref, lhs_ref, low_ref, sums_ref, col_ref, fetch=()):
    alive = (key_ref[counter, :, :H] >= 0).astype(jnp.float32)
    lhs_ref[...] = jnp.zeros((16, H), jnp.float32)
    for k, column in columns.items():
        lhs_ref[2 * k : 2 * k + 2, :] = column * alive
    low_ref[...] = lhs_ref[...].astype(jnp.bfloat16)

    def key_column(step, carry):
        first = pl.multiple_of(step * BLOCK, BLOCK)
        for flop in range(2):
            keys = key_ref[counter, flop : flop + 1, pl.ds(first, BLOCK)]
            col_ref[flop, pl.ds(first, BLOCK), :] = jnp.broadcast_to(keys, (BLOCK, BLOCK)).T
        return carry

    lax.fori_loop(0, H // BLOCK, key_column, 0)
    for part in fetch:
        part.wait()

    def mine(step, carry):
        start = pl.multiple_of(step * WIDE, WIDE)
        weight_total = jnp.zeros((16, WIDE), jnp.float32)
        totals = [jnp.zeros((16, WIDE), jnp.float32) for flop in range(2)]
        rows = [key_ref[counter, flop : flop + 1, pl.ds(start, WIDE)] for flop in range(2)]
        for first in range(0, H, DEEP):
            depth = min(DEEP, H - first)
            lhs = low_ref[:, first : first + depth]
            most = compat_ref[first : first + depth, pl.ds(start, WIDE)]
            weight_total = weight_total + jnp.dot(lhs, most, preferred_element_type=jnp.float32)
            for flop in range(2):
                parts = []
                key_col = col_ref[flop, first : first + depth, :]
                for lane in range(0, WIDE, BLOCK):
                    gap = rows[flop][:, lane : lane + BLOCK] - key_col
                    parts.append(gap.astype(jnp.float32).astype(jnp.bfloat16))
                sign = jnp.concatenate(parts, axis=1) if len(parts) > 1 else parts[0]
                one = jnp.bfloat16(1)
                sign = jnp.minimum(jnp.maximum(sign, -one), one) * most
                totals[flop] = totals[flop] + jnp.dot(
                    lhs, sign, preferred_element_type=jnp.float32
                )
        row_flop = lax.broadcasted_iota(jnp.int32, (16, WIDE), 0) & 1
        sums_ref[0, :, pl.ds(start, WIDE)] = jnp.where(row_flop == 0, totals[0], totals[1])
        sums_ref[1, :, pl.ds(start, WIDE)] = weight_total
        return carry

    lax.fori_loop(0, PADDED // WIDE, mine, 0)
    sign_sum = {k: sums_ref[0, 2 * k : 2 * k + 2, :H] * alive for k in columns}
    weight_sum = {k: sums_ref[1, 2 * k : 2 * k + 2, :H] * alive for k in columns}
    return sign_sum, weight_sum


def two_values(sign_sum, weight_sum, share_root, share_fc):
    v_cc = 0.5 * SCALE * sign_sum[1]
    v_cbf = -0.5 * SCALE * (weight_sum[0] - weight_sum[1])
    v_cbc = 1.5 * SCALE * (sign_sum[0] - sign_sum[1])
    v_bf = 0.5 * SCALE * weight_sum[2]
    v_bc = 1.5 * SCALE * (sign_sum[0] - sign_sum[2])
    u_fc = share_fc * v_cbf + (1.0 - share_fc) * v_cbc
    v_check = v_cc + u_fc
    v_bet = v_bf + v_bc
    u_root = share_root * v_check + (1.0 - share_root) * v_bet
    return v_cbf, v_cbc, u_fc, v_check, v_bet, u_root


def one_values(sign_sum, weight_sum, share_ac, share_fb):
    w_cc = 0.5 * SCALE * sign_sum[4]
    w_cbf = 0.5 * SCALE * weight_sum[5]
    w_cbc = 1.5 * SCALE * (sign_sum[4] - sign_sum[5])
    w_bf = -0.5 * SCALE * (weight_sum[3] - weight_sum[4])
    w_bc = 1.5 * SCALE * (sign_sum[3] - sign_sum[4])
    x_bet = w_cbf + w_cbc
    u_ac = share_ac * w_cc + (1.0 - share_ac) * x_bet
    u_fb = share_fb * w_bf + (1.0 - share_fb) * w_bc
    return w_cc, x_bet, u_ac, w_bf, w_bc, u_fb


def two_regrets(regrets, values):
    root_check, root_bet, fc_fold, fc_call = regrets
    v_cbf, v_cbc, u_fc, v_check, v_bet, u_root = values
    return (
        jnp.maximum(root_check + v_check - u_root, 0.0),
        jnp.maximum(root_bet + v_bet - u_root, 0.0),
        jnp.maximum(fc_fold + v_cbf - u_fc, 0.0),
        jnp.maximum(fc_call + v_cbc - u_fc, 0.0),
    )


def one_regrets(regrets, values):
    ac_check, ac_bet, fb_fold, fb_call = regrets
    w_cc, x_bet, u_ac, w_bf, w_bc, u_fb = values
    return (
        jnp.maximum(ac_check + w_cc - u_ac, 0.0),
        jnp.maximum(ac_bet + x_bet - u_ac, 0.0),
        jnp.maximum(fb_fold + w_bf - u_fb, 0.0),
        jnp.maximum(fb_call + w_bc - u_fb, 0.0),
    )


def pre_step(pre_cont, pre_fold, cont_value):
    share_pre = action_share(pre_cont, pre_fold)
    u_pre = share_pre * cont_value + (1.0 - share_pre) * FOLD_VALUE
    return (
        jnp.maximum(pre_cont + cont_value - u_pre, 0.0),
        jnp.maximum(pre_fold + FOLD_VALUE - u_pre, 0.0),
    )


def one_columns(one_all, share_root, share_fc):
    one_check = one_all * share_root
    return {3: one_all, 4: one_check, 5: one_check * share_fc}


def two_columns(two_all, share_ac, share_fb):
    return {0: two_all, 1: two_all * share_ac, 2: two_all * share_fb}


def one_rows(columns):
    return columns[4], columns[3] - columns[4], columns[4] - columns[5]


def two_rows(columns):
    return columns[1], columns[0] - columns[2], columns[0] - columns[1]


def flop_value(share, u_root):
    part = share * u_root
    return part[0:1, :] + part[1:2, :]


def add_parts(parts_ref):
    total = parts_ref[0]
    for k in range(1, parts_ref.shape[0]):
        total = total + parts_ref[k]
    return total


def spread(copies_ref, value, part=0, parts=1):
    count = copies_ref.shape[0] // parts
    for k in range(count * part, count * (part + 1)):
        copies_ref[k] = value


def read_flops(arrived_ref, cards_ref, key_ref, live_ref, share_ref):
    used = key_ref.shape[0]
    shards = arrived_ref.shape[0]
    hand_block = H // shards
    for shard in range(shards):
        line = arrived_ref[shard] - 1
        for flop in range(2):
            for counter in range(used):
                first = LINE * flop + hand_block * counter
                key_ref[
                    counter, flop : flop + 1, hand_block * shard : hand_block * (shard + 1)
                ] = line[:, first : first + hand_block]
    live_ref[...] = (key_ref[0, :, :H] >= 0).astype(jnp.float32)
    low = cards_ref[0:1, :]
    high = cards_ref[1:2, :]
    for flop in range(2):
        first = LINE * flop + hand_block * used
        extra = arrived_ref[0, :, first : first + 1 + 2 * used]
        share_ref[flop : flop + 1, :] = extra[:, 0:1].astype(jnp.float32) / FLOP_TOTAL
        for counter in range(used):
            turn = extra[:, 1 + 2 * counter : 2 + 2 * counter]
            river = extra[:, 2 + 2 * counter : 3 + 2 * counter]
            blocked = (low == turn) | (low == river) | (high == turn) | (high == river)
            blocked = blocked | (lax.broadcasted_iota(jnp.int32, (1, PADDED), 1) >= H)
            row = key_ref[counter, flop : flop + 1, :]
            key_ref[counter, flop : flop + 1, :] = jnp.where(blocked, -1, row)


def first_kernel(
    arrived_ref, cards_ref, one_ref, two_ref, upper_ref, lower_ref,
    key_ref, live_ref, share_ref, cont_ref,
    root_check_ref, root_bet_ref, fc_fold_ref, fc_call_ref,
    ac_check_ref, ac_bet_ref, fb_fold_ref, fb_call_ref, share_root_ref, share_fc_ref, turn_ref,
    lhs_ref, low_part_ref, sums_ref, col_ref, compat_ref, compat_sem,
):
    fetch = compat_copies(upper_ref, lower_ref, compat_ref, compat_sem)
    for part in fetch:
        part.start()
    scratch = (compat_ref, lhs_ref, low_part_ref, sums_ref, col_ref)
    read_flops(arrived_ref, cards_ref, key_ref, live_ref, share_ref)
    live = live_ref[...]
    share = share_ref[...]
    zero = jnp.zeros((2, H), jnp.float32)
    zero_row = jnp.zeros((1, H), jnp.float32)
    two_all = two_ref[...] * live
    start = action_share(zero, zero)
    one_all = one_ref[...] * action_share(zero_row, zero_row) * live
    one_cols = one_columns(one_all, start, start)
    two_cols = two_columns(two_all, start, start)
    sign_sum, weight_sum = pair_sums(key_ref, 0, {**two_cols, **one_cols}, *scratch, fetch)
    values = two_values(sign_sum, weight_sum, start, start)
    spread(cont_ref, flop_value(share, values[5]), 0, 2)
    regrets = two_regrets((zero, zero, zero, zero), values)
    others = one_regrets((zero, zero, zero, zero), one_values(sign_sum, weight_sum, start, start))
    turns = [*one_rows(one_cols), *two_rows(two_cols)]

    share_root = action_share(regrets[0], regrets[1])
    share_fc = action_share(regrets[2], regrets[3])
    two_cols = two_columns(
        two_all, action_share(others[0], others[1]), action_share(others[2], others[3])
    )
    sign_sum, weight_sum = pair_sums(key_ref, 1, two_cols, *scratch)
    values = two_values(sign_sum, weight_sum, share_root, share_fc)
    spread(cont_ref, flop_value(share, values[5]), 1, 2)
    regrets = two_regrets(regrets, values)
    for k, row in enumerate(two_rows(two_cols)):
        turns[3 + k] = turns[3 + k] + 2.0 * row
    root_check_ref[...], root_bet_ref[...], fc_fold_ref[...], fc_call_ref[...] = regrets
    ac_check_ref[...], ac_bet_ref[...], fb_fold_ref[...], fb_call_ref[...] = others
    share_root_ref[...] = share_root
    share_fc_ref[...] = share_fc
    for k in range(6):
        turn_ref[k] = turns[k]


def second_kernel(
    key_ref, live_ref, one_ref, two_ref, share_ref, upper_ref, lower_ref,
    core_ref, own_sum_ref, other_sum_ref,
    root_check_ref, root_bet_ref, fc_fold_ref, fc_call_ref,
    ac_check_ref, ac_bet_ref, fb_fold_ref, fb_call_ref, share_root_ref, share_fc_ref, turn_ref,
    cont_ref, out_root_ref, out_fc_ref, out_turn_ref, out_pre_ref,
    lhs_ref, low_ref, sums_ref, col_ref, compat_ref, compat_sem,
):
    fetch = compat_copies(upper_ref, lower_ref, compat_ref, compat_sem)
    for part in fetch:
        part.start()
    scratch = (compat_ref, lhs_ref, low_ref, sums_ref, col_ref)
    first_core = core_ref[0, 0] == 0
    own_sum = own_sum_ref[...]
    other_sum = other_sum_ref[...]
    live = live_ref[...]
    zero_row = jnp.zeros((1, H), jnp.float32)
    two_all = two_ref[...] * live
    one_range = one_ref[...]
    turns = [turn_ref[k] for k in range(6)]
    pre_sum = one_range * action_share(zero_row, zero_row)
    pre_cont, pre_fold = pre_step(zero_row, zero_row, jnp.where(first_core, own_sum, other_sum))
    one_now = one_range * action_share(pre_cont, pre_fold)
    pre_sum = pre_sum + 2.0 * one_now
    one_cols = one_columns(one_now * live, share_root_ref[...], share_fc_ref[...])
    for k, row in enumerate(one_rows(one_cols)):
        turns[k] = turns[k] + 2.0 * row
    others = (ac_check_ref[...], ac_bet_ref[...], fb_fold_ref[...], fb_call_ref[...])
    share_ac = action_share(others[0], others[1])
    share_fb = action_share(others[2], others[3])
    sign_sum, weight_sum = pair_sums(key_ref, 1, one_cols, *scratch, fetch)
    others = one_regrets(others, one_values(sign_sum, weight_sum, share_ac, share_fb))

    pre_cont, pre_fold = pre_step(pre_cont, pre_fold, jnp.where(first_core, other_sum, own_sum))
    one_now = one_range * action_share(pre_cont, pre_fold)
    pre_sum = pre_sum + 3.0 * one_now
    regrets = (root_check_ref[...], root_bet_ref[...], fc_fold_ref[...], fc_call_ref[...])
    share_root = action_share(regrets[0], regrets[1])
    share_fc = action_share(regrets[2], regrets[3])
    share_ac = action_share(others[0], others[1])
    share_fb = action_share(others[2], others[3])
    one_cols = one_columns(one_now * live, share_root, share_fc)
    two_cols = two_columns(two_all, share_ac, share_fb)
    for k, row in enumerate((*one_rows(one_cols), *two_rows(two_cols))):
        turns[k] = turns[k] + 3.0 * row
    sign_sum, weight_sum = pair_sums(key_ref, 2, {**two_cols, **one_cols}, *scratch)
    values = two_values(sign_sum, weight_sum, share_root, share_fc)
    spread(cont_ref, flop_value(share_ref[...], values[5]))
    regrets = two_regrets(regrets, values)
    others = one_regrets(others, one_values(sign_sum, weight_sum, share_ac, share_fb))
    two_cols = two_columns(
        two_all, action_share(others[0], others[1]), action_share(others[2], others[3])
    )
    for k, row in enumerate(two_rows(two_cols)):
        turns[3 + k] = turns[3 + k] + 4.0 * row
    out_root_ref[...] = action_share(regrets[0], regrets[1])
    out_fc_ref[...] = action_share(regrets[2], regrets[3])
    for k in range(6):
        out_turn_ref[k] = turns[k]
    out_pre_ref[0:1, :] = pre_cont
    out_pre_ref[1:2, :] = pre_fold
    out_pre_ref[2:3, :] = pre_sum


def pair_scratch():
    return [
        pltpu.VMEM((16, H), jnp.float32),
        pltpu.VMEM((16, H), jnp.bfloat16),
        pltpu.VMEM((2, 16, PADDED), jnp.float32),
        pltpu.VMEM((2, H, BLOCK), jnp.int32),
        pltpu.VMEM((H, PADDED), jnp.bfloat16),
        pltpu.SemaphoreType.DMA((2,)),
    ]


def in_vmem(count):
    return [pl.BlockSpec(memory_space=pltpu.VMEM)] * count


def in_hbm():
    return pl.BlockSpec(memory_space=pltpu.HBM)


def rows_of(*shapes):
    return [jax.ShapeDtypeStruct(shape, jnp.float32) for shape in shapes]


def last_kernel(
    live_ref, one_ref, sums_in_ref, share_root_ref, share_fc_ref, turn_ref, pre_ref,
    out_ref, pre_out_ref,
):
    total_weight = ITERS * (ITERS + 1) / 2.0
    pre_cont, pre_fold = pre_step(pre_ref[0:1, :], pre_ref[1:2, :], add_parts(sums_in_ref))
    one_now = one_ref[...] * action_share(pre_cont, pre_fold)
    columns = one_columns(one_now * live_ref[...], share_root_ref[...], share_fc_ref[...])
    for k, row in enumerate(one_rows(columns)):
        out_ref[k] = (turn_ref[k] + 4.0 * row) / total_weight
    for k in range(3, 6):
        out_ref[k] = turn_ref[k] / total_weight
    pre_out_ref[...] = (pre_ref[2:3, :] + 4.0 * one_now) / total_weight


def solve(arrived, range_one, range_two, cards, compat):
    one_row = range_one.reshape(1, H)
    two_row = range_two.reshape(1, H)
    pair = (2, H)
    first_count = lax.axis_size(FIRST_SUM)
    key_now, live, share, cont, *state = pl.pallas_call(
        first_kernel,
        out_shape=[
            jax.ShapeDtypeStruct((ITERS - 1, 2, PADDED), jnp.int32),
            *rows_of(pair, (2, 1), (first_count, 1, H), *([pair] * 10), (6, 2, H)),
        ],
        in_specs=[*in_vmem(4), in_hbm(), in_hbm()],
        scratch_shapes=pair_scratch(),
        name="first",
        compiler_params=pltpu.CompilerParams(vmem_limit_bytes=20 << 20),
    )(arrived, cards, one_row, two_row, *compat)
    own_sum = jnp.sum(whole_parts(cont), axis=0)
    other_sum = lax.ppermute(own_sum, "grp_1", [(0, 1), (1, 0)])
    core = lax.axis_index("grp_1").astype(jnp.int32).reshape(1, 1)
    cont, share_root, share_fc, turns, pre = pl.pallas_call(
        second_kernel,
        out_shape=rows_of((first_count, 1, H), pair, pair, (6, 2, H), (3, H)),
        in_specs=[
            *in_vmem(5), in_hbm(), in_hbm(), pl.BlockSpec(memory_space=pltpu.SMEM), *in_vmem(13)
        ],
        scratch_shapes=pair_scratch(),
        name="second",
        compiler_params=pltpu.CompilerParams(vmem_limit_bytes=20 << 20),
    )(key_now, live, one_row, two_row, share, *compat, core, own_sum, other_sum, *state)
    parts = whole_parts(cont)
    turns, pre = pl.pallas_call(
        last_kernel,
        out_shape=rows_of((6, 2, H), (1, H)),
        name="last",
        compiler_params=pltpu.CompilerParams(vmem_limit_bytes=8 << 20),
    )(live, one_row, parts, share_root, share_fc, turns, pre)
    return jnp.swapaxes(turns, 0, 1), pre.reshape(H)


def exchanged(copies, axis):
    return lax.all_to_all(copies, axis, split_axis=0, concat_axis=0, tiled=True)


def whole_parts(copies):
    part = jnp.sum(exchanged(copies, FIRST_SUM), axis=0)
    return sent_to_all(part, SECOND_SUM)


ROWS = 80
FIRST_ROWS = (0, 0, FLOP_GRP // 2, FLOP_GRP)


def pack_kernel(first_hand_ref, strength_ref, board_ref, weight_ref, cards_ref, out_ref):
    groups, rows, width = out_ref.shape
    hand_block, _, capacity = strength_ref.shape
    used = ITERS - 1
    hand = first_hand_ref[0, 0] + lax.broadcasted_iota(jnp.int32, (hand_block, capacity), 0)
    flop_live = (board_ref[...] == 1) & (hand < HANDS)
    keys = [jnp.where(flop_live, strength_ref[:, counter, :] + 1, 0) for counter in range(used)]
    weights = weight_ref[...]
    cards = [cards_ref[counter] for counter in range(used)]
    count = jnp.zeros((1, width), jnp.int32) + jnp.sum((weights > 0).astype(jnp.int32))
    extra = used * hand_block
    for group, first in enumerate(FIRST_ROWS):
        for counter in range(used):
            out_ref[group, hand_block * counter : hand_block * (counter + 1), :] = keys[counter][
                :, first : first + width
            ]
        out_ref[group, extra : extra + 1, :] = weights[:, first : first + width]
        for counter in range(used):
            row = extra + 1 + 2 * counter
            out_ref[group, row : row + 2, :] = cards[counter][:, first : first + width]
        blank = extra + 1 + 2 * used
        out_ref[group, blank : blank + 1, :] = count
        out_ref[group, blank + 1 :, :] = jnp.zeros((rows - blank - 1, width), jnp.int32)


def packed(first_hand, strength, board_mask, flop_weight, runout, groups):
    capacity = strength.shape[0]
    return pl.pallas_call(
        pack_kernel,
        out_shape=jax.ShapeDtypeStruct((groups, ROWS, FLOP_GRP), jnp.int32),
        in_specs=[
            pl.BlockSpec(memory_space=pltpu.SMEM),
            *([pl.BlockSpec(memory_space=pltpu.VMEM)] * 4),
        ],
        name="pack",
    )(
        first_hand.astype(jnp.int32).reshape(1, 1),
        jnp.transpose(strength, (2, 1, 0)),
        board_mask.T,
        flop_weight.reshape(1, capacity),
        jnp.transpose(runout, (1, 2, 0)),
    )


def route_kernel(group_ref, slots_ref, out_ref):
    groups, rows, width = slots_ref.shape
    pairs = out_ref.shape[0]
    count_row = (ITERS - 1) * (H // pairs + 2) + 1
    group = group_ref[0, 0]
    first = jnp.where(group == 3, FIRST_ROWS[3], jnp.where(group == 2, FIRST_ROWS[2], 0))
    row = first + lax.broadcasted_iota(jnp.int32, (1, width), 1)
    counts = [slots_ref[g, count_row : count_row + 1, :] for g in range(groups)]
    totals = [[jnp.zeros((pairs, LINE), jnp.float32) for part in range(4)] for odd in range(2)]
    pair = lax.broadcasted_iota(jnp.int32, (pairs, width), 0)
    blank = jnp.zeros((LINE - rows, width), jnp.int32)
    for g in range(groups):
        place = -2 * pairs * group + jnp.zeros((1, width), jnp.int32)
        for other in range(groups):
            place = place + jnp.minimum(counts[other], row + int(other < g))
        place = jnp.where(row < counts[g], place, -1)
        values = jnp.concatenate([slots_ref[g], blank])
        picks = [
            (place == 2 * pair + odd).astype(jnp.float32).astype(jnp.bfloat16) for odd in range(2)
        ]
        for part in range(4):
            digits = (values >> (8 * part)) & (PART - 1)
            digits = digits.astype(jnp.float32).astype(jnp.bfloat16)
            for odd in range(2):
                found = lax.dot_general(
                    picks[odd], digits, (((1,), (1,)), ((), ())), preferred_element_type=jnp.float32
                )
                totals[odd][part] = totals[odd][part] + found
    for odd in range(2):
        whole = jnp.zeros((pairs, LINE), jnp.int32)
        for part in range(4):
            whole = whole + (totals[odd][part].astype(jnp.int32) << (8 * part))
        out_ref[:, 0, LINE * odd : LINE * (odd + 1)] = whole


def route(slots, group_id, pairs):
    return pl.pallas_call(
        route_kernel,
        out_shape=jax.ShapeDtypeStruct((pairs, 1, 2 * LINE), jnp.int32),
        in_specs=[pl.BlockSpec(memory_space=pltpu.SMEM), pl.BlockSpec(memory_space=pltpu.VMEM)],
        name="route",
        compiler_params=pltpu.CompilerParams(vmem_limit_bytes=12 << 20),
    )(group_id.astype(jnp.int32).reshape(1, 1), slots)


def on_device(range_one, range_two, flop_weight, board_mask, runout, strength):
    groups = lax.axis_size(GRP)
    shards = lax.axis_size(INF)
    shard_id = lax.axis_index(INF)
    hand_block = strength.shape[2]
    first_hand = shard_id * hand_block
    cards = jnp.asarray(np.stack(hand_cards(PADDED, HANDS)))
    slots = exchanged(
        packed(first_hand, strength, board_mask, flop_weight, runout, groups), GRP
    )
    slots, upper = lax.optimization_barrier((slots, compat_rows(cards, 0, UPPER)))
    arrived = exchanged(route(slots, lax.axis_index(GRP), shards), INF)
    lower = compat_rows(cards, UPPER, H // BLOCK - UPPER)
    compat = [pltpu.with_memory_space_constraint(part, pltpu.HBM) for part in (upper, lower)]
    turn_reach, pre_reach = solve(arrived, range_one, range_two, cards, compat)
    return turn_reach, lax.dynamic_slice(
        pre_reach, (first_hand,), (hand_block,), allow_negative_indices=False
    )


def solution(mesh):
    split = Mesh(mesh.devices.reshape(2, 2, 4, 8, 2), ("grp_0", "grp_1", "inf_0", "inf_1", "inf_2"))
    return jax.shard_map(
        on_device,
        mesh=split,
        in_specs=(P(), P(), P(GRP), P(GRP, INF), P(GRP, None, None), P(GRP, None, INF)),
        out_specs=(P(GRP_INF, None, None), P(INF)),
        check_vma=False,
    )
```
